8 devices in a mesh: fit: 1 (over z), comp: 2 (over y), data: 4 (over x, core).
Axes of the slice: x: 2, y: 2, z: 1, core: 2. Of those that a mesh axis runs over, the one named last changes fastest.
Arguments:
- points: bfloat16 [4096, 256], P(('fit', 'data'))
- mu_init: float32 [16384, 256], P(('fit', 'comp'))
- logpi_init: float32 [16384], P(('fit', 'comp'))
- inv_temp: float32 [3], replicated
Outputs:
- output 1: float32 [16384, 256], P(('fit', 'comp'))
- output 2: float32 [16384], P(('fit', 'comp'))
- output 3: float32 [4096], P(('fit', 'data'))
All inputs are finite; a program needn't handle non-finite values.
Results may differ from the reference program's by a relative error of at most 0.00129327.
Values are sent between devices in bfloat16 or wider.
A program may use at most 1 GiB of HBM per device.

```python
import math
import jax
import jax.numpy as jnp
from jax import lax

NPTS = 4096
DIM = 256
CLUSTERS = 16384
SWEEPS = 3
LANDMARKS = 1024
WINDOW = 32
ROW_BLOCK = math.gcd(NPTS, 512)
EPS_COUNT = 1e-6
ALPHA = 1e-3


def curve_at(curve_nodes, numer):
    scaled = numer * LANDMARKS
    left_idx = scaled // NPTS
    frac_part = ((scaled % NPTS).astype(jnp.float32) / NPTS)[:, None]
    return curve_nodes[left_idx] * (1.0 - frac_part) + curve_nodes[left_idx + 1] * frac_part


def setup_inputs(seed: int = 0, part: int = 0) -> dict:
    part_key = jax.random.fold_in(jax.random.key(seed), part)
    key_list = jax.random.split(part_key, 6)
    step_scale = (WINDOW * math.sqrt(2.0 * DIM)) ** -0.5
    start_node = 0.5 * jax.random.normal(key_list[0], (1, DIM), jnp.float32)
    step_vecs = step_scale * jax.random.normal(key_list[1], (LANDMARKS, DIM), jnp.float32)
    curve_nodes = jnp.concatenate([start_node, start_node + jnp.cumsum(step_vecs, axis=0)], axis=0)
    row_pos = jnp.arange(NPTS, dtype=jnp.int32)
    points = curve_at(curve_nodes, row_pos) + 0.5 * jax.random.normal(key_list[2], (NPTS, DIM), jnp.float32)
    comp_pos = jax.random.randint(key_list[3], (CLUSTERS,), 0, NPTS, dtype=jnp.int32)
    mu_init = curve_at(curve_nodes, comp_pos) + 0.5 * jax.random.normal(key_list[4], (CLUSTERS, DIM), jnp.float32)
    raw_w = jax.random.normal(key_list[5], (CLUSTERS,), jnp.float32)
    logpi_init = raw_w - jax.nn.logsumexp(raw_w)
    beta_key = jax.random.key(seed + 101)
    jitter = jax.random.uniform(beta_key, (SWEEPS,), jnp.float32, -0.25, 0.25)
    beta_ramp = 0.6 * 1.5 ** jnp.arange(SWEEPS, dtype=jnp.float32)
    inv_temp = math.sqrt(2.0 / DIM) * beta_ramp * jnp.exp(jitter)
    return {"points": points.astype(jnp.bfloat16), "mu_init": mu_init, "logpi_init": logpi_init, "inv_temp": inv_temp}


def reference(points, mu_init, logpi_init, inv_temp):
    point_blocks = points.reshape(NPTS // ROW_BLOCK, ROW_BLOCK, DIM)
    norm_const = NPTS + CLUSTERS * ALPHA

    def one_sweep(carry_state, beta_t):
        mean_rows, log_w = carry_state
        mean_low = mean_rows.astype(jnp.bfloat16)
        mean_sq = jnp.sum(mean_rows * mean_rows, axis=1)

        def one_block(acc_state, x_blk):
            stat_sum, counts = acc_state
            row_sq = jnp.sum(jnp.square(x_blk.astype(jnp.float32)), axis=1)
            cross_dot = jnp.dot(x_blk, mean_low.T, preferred_element_type=jnp.float32)
            logits = log_w[None, :] - beta_t * (row_sq[:, None] - 2.0 * cross_dot + mean_sq[None, :])
            row_max = jnp.max(logits, axis=1)
            row_lse = row_max + jnp.log(jnp.sum(jnp.exp(logits - row_max[:, None]), axis=1))
            resp_blk = jnp.exp(logits - row_lse[:, None])
            counts = counts + jnp.sum(resp_blk, axis=0)
            stat_sum = stat_sum + jnp.dot(resp_blk.astype(jnp.bfloat16).T, x_blk, preferred_element_type=jnp.float32)
            return (stat_sum, counts), row_lse

        acc_init = (jnp.zeros((CLUSTERS, DIM), jnp.float32), jnp.zeros((CLUSTERS,), jnp.float32))
        (stat_sum, counts), lse_blocks = lax.scan(one_block, acc_init, point_blocks)
        new_means = stat_sum / (counts + EPS_COUNT)[:, None]
        new_w = jnp.log((counts + ALPHA) / norm_const)
        return (new_means, new_w), lse_blocks.reshape(NPTS)

    (mean_rows, log_w), lse_all = lax.scan(one_sweep, (mu_init, logpi_init), inv_temp)
    return mean_rows, log_w, lse_all[-1]
```

```python
import jax
import jax.numpy as jnp
from jax import lax
from jax.sharding import PartitionSpec as P

EPS_COUNT = 1e-6
ALPHA = 1e-3


def solution(mesh):
    comp_size = mesh.shape["comp"]
    data_size = mesh.shape["data"]

    def local_fit(points, mu_init, logpi_init, inv_temp):
        total_rows = points.shape[0] * data_size
        total_comp = mu_init.shape[0] * comp_size
        norm_const = total_rows + total_comp * ALPHA
        pts = lax.all_gather(points, "data", axis=0, tiled=True)
        own = mu_init.shape[0] // data_size
        start = lax.axis_index("data") * own
        mean_rows = lax.dynamic_slice_in_dim(mu_init, start, own, 0)
        log_w = lax.dynamic_slice_in_dim(logpi_init, start, own, 0)
        row_sq = jnp.sum(jnp.square(pts.astype(jnp.float32)), axis=1)
        for sweep_idx in range(inv_temp.shape[0]):
            beta_t = inv_temp[sweep_idx]
            mean_sq = jnp.sum(mean_rows * mean_rows, axis=1)
            cross = lax.dot_general(mean_rows.astype(jnp.bfloat16), pts, (((1,), (1,)), ((), ())), preferred_element_type=jnp.float32)
            logits = log_w[:, None] - beta_t * (row_sq[None, :] - 2.0 * cross + mean_sq[:, None])
            m_loc = jnp.max(logits, axis=0)
            expd = jnp.exp(logits - m_loc[None, :])
            s_loc = jnp.sum(expd, axis=0)
            stats = lax.all_gather(jnp.stack([m_loc, s_loc]), ("comp", "data"), axis=0)
            row_max = jnp.max(stats[:, 0], axis=0)
            row_sum = jnp.sum(stats[:, 1] * jnp.exp(stats[:, 0] - row_max[None, :]), axis=0)
            row_lse = row_max + jnp.log(row_sum)
            resp = expd * jnp.exp(m_loc - row_lse)[None, :]
            counts = jnp.sum(resp, axis=1)
            stat_sum = lax.dot_general(resp.astype(jnp.bfloat16), pts, (((1,), (0,)), ((), ())), preferred_element_type=jnp.float32)
            mean_rows = stat_sum / (counts + EPS_COUNT)[:, None]
            log_w = jnp.log((counts + ALPHA) / norm_const)
        means = lax.all_gather(mean_rows, "data", axis=0, tiled=True)
        weights = lax.all_gather(log_w, "data", axis=0, tiled=True)
        n_pts = points.shape[0]
        lse = lax.dynamic_slice_in_dim(row_lse, lax.axis_index("data") * n_pts, n_pts, 0)
        return means, weights, lse

    row_spec = P(("fit", "data"), None)
    comp_spec = P(("fit", "comp"), None)
    weight_spec = P(("fit", "comp"))
    lse_spec = P(("fit", "data"))
    return jax.shard_map(local_fit, mesh=mesh, in_specs=(row_spec, comp_spec, weight_spec, P(None)), out_specs=(comp_spec, weight_spec, lse_spec), check_vma=False)
```

```python
import functools
import math

import jax
import jax.numpy as jnp
from jax import lax
from jax.experimental import pallas as pl
from jax.experimental.pallas import tpu as pltpu
from jax.sharding import PartitionSpec as P

EPS_COUNT = 1e-6
ALPHA = 1e-3
LOG2E = math.log2(math.e)
LN2 = math.log(2.0)
KB = 512
IB = 256
KT = 128
MESH = pl.DeviceIdType.MESH
F32 = jnp.float32
BF16 = jnp.bfloat16
NT = (((1,), (1,)), ((), ()))


def fit_kernel(cfg, temp_ref, pts_ref, mu_ref, logpi_ref, means_ref, logw_ref, lse_out_ref,
               x_ref, p_ref, mub_ref, muf_ref, c_ref, crow_ref, cfrow_ref, s_ref, n_ref, fin_ref,
               wrow_ref, m_ref, sum_ref, lse_ref, g_ref, lseo_ref,
               loc_sem, pts_send, pts_recv, st_send, st_recv, mu_send, mu_recv,
               out_loc, out_send, out_recv, w_loc, w_send, w_recv):
    sweeps, own, nq, dim, norm_const = cfg
    n_kb = own // KB
    n_kt = own // KT
    half = nq // 2
    fit = lax.axis_index("fit")
    comp = lax.axis_index("comp")
    data = lax.axis_index("data")
    xpos = data // 2

    def data_xor(d):
        if d == 0:
            return data
        if d == 1:
            return data + 1 - 2 * (data % 2)
        if d == 2:
            return (data + 2) % 4
        return (data + 1 - 2 * (data % 2) + 2) % 4

    def peer(r):
        return (fit, (comp + r // 4) % 2, data_xor(r % 4))

    sib, par = data_xor(1), data_xor(2)
    me = comp * 4 + data

    barrier = pltpu.get_barrier_semaphore()
    for r in range(1, 8):
        pl.semaphore_signal(barrier, inc=1, device_id=peer(r), device_id_type=MESH)

    ld_pts = pltpu.make_async_copy(pts_ref, x_ref.at[pl.ds(pl.multiple_of(data * nq, nq), nq)], loc_sem.at[0])
    ld_mu = pltpu.make_async_copy(mu_ref.at[pl.ds(pl.multiple_of(data * own, own), own)], s_ref, loc_sem.at[1])
    ld_pi = pltpu.make_async_copy(logpi_ref.at[data], crow_ref, loc_sem.at[2])
    ld_pts.start()
    ld_mu.start()
    ld_pi.start()
    pl.semaphore_wait(barrier, 7)

    def pts_copy(kind, ch):
        owner = data if kind < 2 else par
        rows = pl.ds(pl.multiple_of(owner * nq + ch * half, half), half)
        src = pts_ref.at[pl.ds(ch * half, half)] if kind < 2 else x_ref.at[rows]
        dev = peer(2) if kind == 1 else peer(1)
        return pltpu.make_async_remote_copy(
            src_ref=src, dst_ref=x_ref.at[rows], send_sem=pts_send.at[kind, ch], recv_sem=pts_recv.at[kind, ch],
            device_id=dev, device_id_type=MESH)

    for ch in range(2):
        pts_copy(1, ch).start()
    for ch in range(2):
        pts_copy(0, ch).start()

    def to_col(row):
        return jnp.transpose(jnp.broadcast_to(row, (128, row.shape[1])))

    def to_row(col):
        return jnp.transpose(col)[0:1, :]

    ld_pi.wait()
    ld_mu.wait()
    beta0 = temp_ref[0]

    def init_body(kb, _):
        rows = pl.ds(pl.multiple_of(kb * KB, KB), KB)
        mu = s_ref[rows, :]
        mub_ref[rows, :] = mu.astype(BF16)
        msq = jnp.sum(mu * mu, axis=1, keepdims=True)
        lp = to_col(crow_ref[:, rows])
        c_ref[rows, :] = LOG2E * (lp - beta0 * msq)
        return 0

    lax.fori_loop(0, n_kb, init_body, 0)

    def e_quarter(q, tb):
        for it in range(nq // IB):
            i0 = q * nq + it * IB
            xt = x_ref[pl.ds(pl.multiple_of(i0, IB), IB), :]
            for kb in range(n_kb):
                a = lax.dot_general(mub_ref[pl.ds(kb * KB, KB), :], xt, NT, preferred_element_type=F32)
                for u in range(KB // KT):
                    rows = pl.ds(kb * KB + u * KT, KT)
                    tile = kb * (KB // KT) + u
                    cc = c_ref[rows, :]
                    for lc in range(IB // 128):
                        cols = pl.ds(pl.multiple_of(i0 + lc * 128, 128), 128)
                        l = a[u * KT:(u + 1) * KT, lc * 128:(lc + 1) * 128] * tb + cc
                        l3 = l.reshape(KT // 8, 8, 128)
                        m = jnp.max(l3, axis=0)
                        p3 = jnp.exp2(l3 - m[None])
                        p_ref[rows, cols] = p3.reshape(KT, 128)
                        m_ref[tile, :, cols] = m
                        sum_ref[tile, :, pl.ds(it * IB + lc * 128, 128)] = jnp.sum(p3, axis=0)

    def st_copy(t, q, r):
        return pltpu.make_async_remote_copy(
            src_ref=g_ref.at[t, q, me], dst_ref=g_ref.at[t, q, me], send_sem=st_send.at[t, q, r],
            recv_sem=st_recv.at[t, q, r], device_id=peer(r), device_id_type=MESH)

    def st_send_all(t, q):
        cols = pl.ds(pl.multiple_of(q * nq, nq), nq)
        top = jnp.max(functools.reduce(jnp.maximum, [m_ref[k, :, cols] for k in range(n_kt)]), axis=0, keepdims=True)
        tot = functools.reduce(lambda u, v: u + v,
                               [sum_ref[k] * jnp.exp2(m_ref[k, :, cols] - top) for k in range(n_kt)])
        tot = jnp.sum(tot, axis=0, keepdims=True)
        g_ref[t, q, me] = top + LOG2E * jnp.log(tot)
        for r in range(1, 8):
            st_copy(t, q, r).start()

    def e_step(t, q, tb):
        e_quarter(q, tb)
        st_send_all(t, q)

    def st_combine(t, q):
        for r in range(1, 8):
            st_copy(t, q, r).wait_recv()
        cols = pl.ds(pl.multiple_of(q * nq, nq), nq)
        vals = [g_ref[t, q, s] for s in range(8)]
        top = functools.reduce(jnp.maximum, vals)
        tot = functools.reduce(lambda u, v: u + v, [jnp.exp2(v - top) for v in vals])
        lse = top + LOG2E * jnp.log(tot)
        lse_ref[:, cols] = lse
        for k in range(n_kt):
            m_ref[k, :, cols] = jnp.exp2(m_ref[k, :, cols] - lse)

    def m_block(kb, quarters):
        k0 = kb * KB
        ns = [jnp.zeros((KT, 128), F32)] * (KB // KT)
        acc = jnp.zeros((KB, dim), F32)
        for q in quarters:
            for ic in range(nq // IB):
                i0 = q * nq + ic * IB
                parts = []
                for u in range(KB // KT):
                    rows = pl.ds(pl.multiple_of(k0 + u * KT, KT), KT)
                    cols = pl.ds(i0, IB)
                    sc = m_ref[kb * (KB // KT) + u, :, cols]
                    r = (p_ref[rows, cols].reshape(KT // 8, 8, IB) * sc[None]).reshape(KT, IB)
                    ns[u] = ns[u] + (r[:, :128] + r[:, 128:])
                    parts.append(r.astype(BF16))
                rb = jnp.concatenate(parts, axis=0)
                acc = acc + jnp.dot(rb, x_ref[pl.ds(i0, IB), :], preferred_element_type=F32)
        return jnp.concatenate(ns, axis=0), acc

    def m_first(kb, _):
        rows = pl.ds(pl.multiple_of(kb * KB, KB), KB)
        n_acc, acc = m_block(kb, (0, 2))
        n_ref[rows, :] = n_acc
        s_ref[rows, :] = acc
        return 0

    def finish(n_acc, acc):
        n = jnp.sum(n_acc, axis=1, keepdims=True)
        mu = acc * (1.0 / (n + EPS_COUNT))
        return n, mu

    def mu_copy(kb):
        rows = pl.ds(pl.multiple_of(kb * KB, KB), KB)
        return pltpu.make_async_remote_copy(
            src_ref=mub_ref.at[rows], dst_ref=muf_ref.at[rows], send_sem=mu_send.at[kb], recv_sem=mu_recv.at[kb],
            device_id=peer(2), device_id_type=MESH)

    def c_copy():
        return pltpu.make_async_remote_copy(
            src_ref=crow_ref, dst_ref=cfrow_ref, send_sem=mu_send.at[n_kb], recv_sem=mu_recv.at[n_kb],
            device_id=peer(2), device_id_type=MESH)

    def m_second(kb, beta_next, share):
        rows = pl.ds(pl.multiple_of(kb * KB, KB), KB)
        n_acc, acc = m_block(kb, (1, 3))
        n, mu = finish(n_ref[rows, :] + n_acc, s_ref[rows, :] + acc)
        mub_ref[rows, :] = mu.astype(BF16)
        msq = jnp.sum(mu * mu, axis=1, keepdims=True)
        lp = jnp.log((jnp.broadcast_to(n, (KB, 128)) + ALPHA) / norm_const)
        c = LOG2E * (lp - beta_next * msq)
        c_ref[rows, :] = c
        if share:
            crow_ref[:, rows] = to_row(c)
            mu_copy(kb).start()

    def out_copies(slot, kb):
        owner = data if slot == 0 else par
        dst = means_ref.at[pl.ds(pl.multiple_of(owner * own + kb * KB, KB), KB)]
        src = fin_ref.at[slot, pl.ds(pl.multiple_of(kb * KB, KB), KB)]
        here = pltpu.make_async_copy(src, dst, out_loc.at[slot, kb])
        there = pltpu.make_async_remote_copy(
            src_ref=src, dst_ref=dst, send_sem=out_send.at[slot, kb], recv_sem=out_recv.at[slot, kb],
            device_id=peer(1), device_id_type=MESH)
        return here, there

    def w_copies(slot):
        owner = data if slot == 0 else par
        here = pltpu.make_async_copy(wrow_ref.at[slot], logw_ref.at[owner], w_loc.at[slot])
        there = pltpu.make_async_remote_copy(
            src_ref=wrow_ref.at[slot], dst_ref=logw_ref.at[owner], send_sem=w_send.at[slot], recv_sem=w_recv.at[slot],
            device_id=peer(1), device_id_type=MESH)
        return here, there

    def emit(slot, kb, n_acc, acc):
        rows = pl.ds(pl.multiple_of(kb * KB, KB), KB)
        n, mu = finish(n_acc, acc)
        fin_ref[slot, rows, :] = mu
        nrow = to_row(jnp.broadcast_to(n, (KB, 128)))
        wrow_ref[slot, :, rows] = jnp.log((nrow + ALPHA) / norm_const)
        for cp in out_copies(slot, kb):
            cp.start()

    for t in range(sweeps):
        beta = temp_ref[t]
        tb = (2.0 * LOG2E) * beta
        last = t == sweeps - 1
        if t == 0:
            ld_pts.wait()
            for ch in range(2):
                pts_copy(0, ch).wait_recv()
            lax.fori_loop(0, 2, lambda s, _: (e_step(0, xpos * 2 + s, tb), 0)[1], 0)
            for ch in range(2):
                pts_copy(1, ch).wait_recv()
                pts_copy(2, ch).start()
            for ch in range(2):
                pts_copy(2, ch).wait_recv()
            lax.fori_loop(0, 2, lambda s, _: (e_step(0, (1 - xpos) * 2 + s, tb), 0)[1], 0)
        else:
            lax.fori_loop(0, 4, lambda s, _: (e_step(t, (s % 2) * 2 + s // 2, tb), 0)[1], 0)
        st_combine(t, 0)
        st_combine(t, 2)
        lax.fori_loop(0, n_kb, m_first, 0)
        st_combine(t, 1)
        st_combine(t, 3)
        if not last:
            beta_next = temp_ref[t + 1]
            share = t == sweeps - 2
            lax.fori_loop(0, n_kb, lambda kb, _: (m_second(kb, beta_next, share), 0)[1], 0)
            if share:
                c_copy().start()
        else:
            def m_last(kb, _):
                rows = pl.ds(pl.multiple_of(kb * KB, KB), KB)
                n_acc, acc = m_block(kb, (1, 3))
                emit(0, kb, n_ref[rows, :] + n_acc, s_ref[rows, :] + acc)
                return 0

            lax.fori_loop(0, n_kb, m_last, 0)
            for cp in w_copies(0):
                cp.start()
            c_copy().wait_recv()

            def far_block(kb, _):
                mu_copy(kb).wait_recv()
                rows = pl.ds(pl.multiple_of(kb * KB, KB), KB)
                c = to_col(cfrow_ref[:, rows])
                c_ref[rows, :] = c
                n_ref[rows, :] = jnp.zeros((KB, 128), F32)
                s_ref[rows, :] = jnp.zeros((KB, dim), F32)

                def far_quarter(q, _):
                    cc = c_ref[rows, :]
                    c2 = jnp.concatenate([cc, cc], axis=1)
                    n_acc = n_ref[rows, :]
                    acc = s_ref[rows, :]
                    for ic in range(nq // IB):
                        cols = pl.ds(pl.multiple_of(q * nq + ic * IB, IB), IB)
                        xt = x_ref[cols, :]
                        a = lax.dot_general(muf_ref[rows, :], xt, NT, preferred_element_type=F32)
                        r = jnp.exp2((a * tb + c2) - lse_ref[:, cols])
                        n_acc = n_acc + (r[:, :128] + r[:, 128:])
                        acc = acc + jnp.dot(r.astype(BF16), xt, preferred_element_type=F32)
                    n_ref[rows, :] = n_acc
                    s_ref[rows, :] = acc
                    return 0

                lax.fori_loop(0, 4, far_quarter, 0)
                emit(1, kb, n_ref[rows, :], s_ref[rows, :])
                return 0

            lax.fori_loop(0, n_kb, far_block, 0)
            for cp in w_copies(1):
                cp.start()
            mine = pl.ds(pl.multiple_of(data * nq, nq), nq)
            xo = x_ref[mine, :].astype(F32)
            sq = xo * xo
            hi = sq.astype(BF16)
            lo = (sq - hi.astype(F32)).astype(BF16)
            ones = jnp.ones((8, dim), BF16)
            row_sq = (lax.dot_general(ones, hi, NT, preferred_element_type=F32)
                      + lax.dot_general(ones, lo, NT, preferred_element_type=F32))
            lseo_ref[...] = LN2 * lse_ref[:, mine] - beta * row_sq[0:1, :]
            lse_cp = pltpu.make_async_copy(lseo_ref, lse_out_ref, loc_sem.at[3])
            lse_cp.start()
            lse_cp.wait()

    for kind in range(3):
        for ch in range(2):
            pts_copy(kind, ch).wait_send()
    for t in range(sweeps):
        for q in range(4):
            for r in range(1, 8):
                st_copy(t, q, r).wait_send()
    for kb in range(n_kb):
        mu_copy(kb).wait_send()
    c_copy().wait_send()
    for slot in range(2):
        for kb in range(n_kb):
            here, there = out_copies(slot, kb)
            here.wait()
            there.wait_send()
        here, there = w_copies(slot)
        here.wait()
        there.wait_send()
    for slot in range(2):
        sib_slot_recv(slot, means_ref, logw_ref, out_copies, w_copies, n_kb)


def sib_slot_recv(slot, means_ref, logw_ref, out_copies, w_copies, n_kb):
    for kb in range(n_kb):
        out_copies(slot, kb)[1].wait_recv()
    w_copies(slot)[1].wait_recv()


def solution(mesh):
    comp_size = mesh.shape["comp"]
    data_size = mesh.shape["data"]

    def local_fit(points, mu_init, logpi_init, inv_temp):
        nq, dim = points.shape
        rows = mu_init.shape[0]
        own = rows // data_size
        sweeps = inv_temp.shape[0]
        n_pts = nq * data_size
        n_kb = own // KB
        norm_const = n_pts + rows * comp_size * ALPHA
        cfg = (sweeps, own, nq, dim, norm_const)
        any_spec = pl.BlockSpec(memory_space=pl.ANY)
        dma = pltpu.SemaphoreType.DMA
        means, logw, lse = pl.pallas_call(
            functools.partial(fit_kernel, cfg),
            out_shape=(jax.ShapeDtypeStruct((rows, dim), F32),
                       jax.ShapeDtypeStruct((data_size, 1, own), F32),
                       jax.ShapeDtypeStruct((1, nq), F32)),
            in_specs=[pl.BlockSpec(memory_space=pltpu.SMEM), any_spec, any_spec, any_spec],
            out_specs=(any_spec, any_spec, any_spec),
            scratch_shapes=[
                pltpu.VMEM((n_pts, dim), BF16),
                pltpu.VMEM((own, n_pts), F32),
                pltpu.VMEM((own, dim), BF16),
                pltpu.VMEM((own, dim), BF16),
                pltpu.VMEM((own, 128), F32),
                pltpu.VMEM((1, own), F32),
                pltpu.VMEM((1, own), F32),
                pltpu.VMEM((own, dim), F32),
                pltpu.VMEM((own, 128), F32),
                pltpu.VMEM((2, own, dim), F32),
                pltpu.VMEM((2, 1, own), F32),
                pltpu.VMEM((own // KT, 8, n_pts), F32),
                pltpu.VMEM((own // KT, 8, nq), F32),
                pltpu.VMEM((1, n_pts), F32),
                pltpu.VMEM((sweeps, data_size, 8, 1, nq), F32),
                pltpu.VMEM((1, nq), F32),
                dma((4,)),
                dma((3, 2)), dma((3, 2)),
                dma((sweeps, 4, 8)), dma((sweeps, 4, 8)),
                dma((n_kb + 1,)), dma((n_kb + 1,)),
                dma((2, n_kb)), dma((2, n_kb)), dma((2, n_kb)),
                dma((2,)), dma((2,)), dma((2,)),
            ],
            compiler_params=pltpu.CompilerParams(
                collective_id=0, has_side_effects=True, vmem_limit_bytes=62 * 1024 * 1024),
        )(inv_temp, points, mu_init, logpi_init.reshape(data_size, 1, own))
        return means, logw.reshape(rows), lse.reshape(nq)

    row_spec = P(("fit", "data"), None)
    comp_spec = P(("fit", "comp"), None)
    weight_spec = P(("fit", "comp"))
    lse_spec = P(("fit", "data"))
    return jax.shard_map(local_fit, mesh=mesh, in_specs=(row_spec, comp_spec, weight_spec, P(None)), out_specs=(comp_spec, weight_spec, lse_spec), check_vma=False)
```

```python
import functools
import math

import jax
import jax.numpy as jnp
from jax import lax
from jax.experimental import pallas as pl
from jax.experimental.pallas import tpu as pltpu
from jax.sharding import PartitionSpec as P

EPS_COUNT = 1e-6
ALPHA = 1e-3
LOG2E = math.log2(math.e)
LN2 = math.log(2.0)
KB = 512
IB = 256
KT = 64
MB = 1024
EARLY = 3
FB = 256
MESH = pl.DeviceIdType.MESH
F32 = jnp.float32
BF16 = jnp.bfloat16
NT = (((1,), (1,)), ((), ()))


def fit_kernel(cfg, temp_ref, pts_ref, mu_ref, logpi_ref, means_ref, logw_ref, lse_out_ref,
               x_ref, p_ref, mub_ref, muf_ref, c_ref, crow_ref, cfrow_ref, s_ref, n_ref,
               m_ref, sum_ref, lse_ref, g_ref,
               loc_sem, pts_send, pts_recv, st_send, st_recv, mu_send, mu_recv,
               out_send, out_recv, w_send, w_recv):
    sweeps, own, nq, dim, norm_const = cfg
    n_kb = own // KB
    n_kt = own // KT
    n_mb = own // MB
    n_fb = own // FB
    n_ch = nq // IB
    fit = lax.axis_index("fit")
    comp = lax.axis_index("comp")
    data = lax.axis_index("data")
    xpos = data // 2

    def data_xor(d):
        if d == 0:
            return data
        if d == 1:
            return data + 1 - 2 * (data % 2)
        if d == 2:
            return (data + 2) % 4
        return (data + 1 - 2 * (data % 2) + 2) % 4

    def peer(r):
        return (fit, (comp + r // 4) % 2, data_xor(r % 4))

    sib, par = data_xor(1), data_xor(2)
    me = comp * 4 + data

    barrier = pltpu.get_barrier_semaphore()
    for r in range(1, 8):
        pl.semaphore_signal(barrier, inc=1, device_id=peer(r), device_id_type=MESH)

    ld_pts = pltpu.make_async_copy(pts_ref, x_ref.at[pl.ds(pl.multiple_of(data * nq, nq), nq)], loc_sem.at[0])
    ld_mu = pltpu.make_async_copy(mu_ref.at[pl.ds(pl.multiple_of(data * own, own), own)], s_ref, loc_sem.at[1])
    ld_pi = pltpu.make_async_copy(logpi_ref.at[data], crow_ref, loc_sem.at[2])
    ld_pts.start()
    ld_mu.start()
    ld_pi.start()
    pl.semaphore_wait(barrier, 7)

    def pts_copy(kind, ch):
        owner = data if kind < 2 else par
        rows = pl.ds(pl.multiple_of(owner * nq + ch * IB, IB), IB)
        src = pts_ref.at[pl.ds(ch * IB, IB)] if kind < 2 else x_ref.at[rows]
        dev = peer(2) if kind == 1 else peer(1)
        return pltpu.make_async_remote_copy(
            src_ref=src, dst_ref=x_ref.at[rows], send_sem=pts_send.at[kind, ch], recv_sem=pts_recv.at[kind, ch],
            device_id=dev, device_id_type=MESH)

    for ch in range(n_ch):
        pts_copy(1, ch).start()
    for ch in range(n_ch):
        pts_copy(0, ch).start()

    def to_col(row):
        return jnp.transpose(jnp.broadcast_to(row, (128, row.shape[1])))

    def to_row(col):
        return jnp.transpose(col)[0:1, :]

    ld_pi.wait()
    ld_mu.wait()
    beta0 = temp_ref[0]

    def init_body(kb, _):
        rows = pl.ds(pl.multiple_of(kb * KB, KB), KB)
        mu = s_ref[rows, :]
        mub_ref[rows, :] = mu.astype(BF16)
        msq = jnp.sum(mu * mu, axis=1, keepdims=True)
        lp = to_col(crow_ref[:, rows])
        c_ref[rows, :] = LOG2E * (lp - beta0 * msq)
        return 0

    lax.fori_loop(0, n_kb, init_body, 0)

    def e_tile(i0, tb):
        cols = pl.ds(pl.multiple_of(i0, IB), IB)
        xt = x_ref[cols, :]
        for kb in range(n_kb):
            a = lax.dot_general(mub_ref[pl.ds(kb * KB, KB), :], xt, NT, preferred_element_type=F32)
            for u in range(KB // KT):
                rows = pl.ds(kb * KB + u * KT, KT)
                tile = kb * (KB // KT) + u
                cc = c_ref[rows, :]
                l = a[u * KT:(u + 1) * KT, :] * tb + jnp.concatenate([cc, cc], axis=1)
                l3 = l.reshape(KT // 8, 8, IB)
                m = jnp.max(l3, axis=0)
                p3 = jnp.exp2(l3 - m[None])
                p_ref[rows, cols] = p3.reshape(KT, IB)
                m_ref[tile, :, cols] = m
                sum_ref[tile, :, cols] = jnp.sum(p3, axis=0)

    def e_quarter(q, tb):
        for it in range(n_ch):
            e_tile(q * nq + it * IB, tb)

    def st_copy(t, q, r):
        return pltpu.make_async_remote_copy(
            src_ref=g_ref.at[t, q, me], dst_ref=g_ref.at[t, q, me], send_sem=st_send.at[t, q, r],
            recv_sem=st_recv.at[t, q, r], device_id=peer(r), device_id_type=MESH)

    def st_send_all(t, q):
        cols = pl.ds(pl.multiple_of(q * nq, nq), nq)
        top = jnp.max(jnp.max(m_ref[:, :, cols], axis=0), axis=0, keepdims=True)
        part = [pl.ds(k, 8) for k in range(0, n_kt, 8)]
        tot = functools.reduce(lambda u, v: u + v,
                               [jnp.sum(sum_ref[k, :, cols] * jnp.exp2(m_ref[k, :, cols] - top), axis=0) for k in part])
        tot = jnp.sum(tot, axis=0, keepdims=True)
        g_ref[t, q, me] = top + LOG2E * jnp.log(tot)
        for r in range(1, 8):
            st_copy(t, q, r).start()

    def e_step(t, q, tb):
        e_quarter(q, tb)
        st_send_all(t, q)

    def st_combine(t, q):
        for r in range(1, 8):
            st_copy(t, q, r).wait_recv()
        cols = pl.ds(pl.multiple_of(q * nq, nq), nq)
        vals = g_ref[t, q]
        top = jnp.max(vals, axis=0)
        tot = jnp.sum(jnp.exp2(vals - top[None]), axis=0)
        lse = top + LOG2E * jnp.log(tot)
        lse_ref[:, cols] = lse
        m_ref[:, :, cols] = jnp.exp2(m_ref[:, :, cols] - lse)

    def m_block(kb, quarters):
        rows = pl.ds(pl.multiple_of(kb * MB, MB), MB)
        n_acc = jnp.zeros((MB, 128), F32)
        acc = jnp.zeros((MB, dim), F32)
        for q in quarters:
            for ic in range(n_ch):
                cols = pl.ds(q * nq + ic * IB, IB)
                sc = m_ref[pl.ds(kb * (MB // KT), MB // KT), :, cols]
                r = (p_ref[rows, cols].reshape(MB // KT, KT // 8, 8, IB) * sc[:, None]).reshape(MB, IB)
                n_acc = n_acc + (r[:, :128] + r[:, 128:])
                acc = acc + jnp.dot(r.astype(BF16), x_ref[cols, :], preferred_element_type=F32)
        return n_acc, acc

    def m_first(kb, _):
        rows = pl.ds(pl.multiple_of(kb * MB, MB), MB)
        n_acc, acc = m_block(kb, (0, 2))
        n_ref[rows, :] = n_acc
        s_ref[rows, :] = acc
        return 0

    def finish(n_acc, acc):
        n = jnp.sum(n_acc, axis=1, keepdims=True)
        mu = acc * (1.0 / (n + EPS_COUNT))
        return n, mu

    def mu_copy(j):
        rows = pl.ds(pl.multiple_of(j * FB, FB), FB)
        return pltpu.make_async_remote_copy(
            src_ref=mub_ref.at[rows], dst_ref=muf_ref.at[rows], send_sem=mu_send.at[j], recv_sem=mu_recv.at[j],
            device_id=peer(2), device_id_type=MESH)

    def c_copy():
        return pltpu.make_async_remote_copy(
            src_ref=crow_ref, dst_ref=cfrow_ref, send_sem=mu_send.at[n_fb], recv_sem=mu_recv.at[n_fb],
            device_id=peer(2), device_id_type=MESH)

    def m_second(kb, beta_next, share):
        rows = pl.ds(pl.multiple_of(kb * MB, MB), MB)
        n_acc, acc = m_block(kb, (1, 3))
        n, mu = finish(n_ref[rows, :] + n_acc, s_ref[rows, :] + acc)
        mub_ref[rows, :] = mu.astype(BF16)
        msq = jnp.sum(mu * mu, axis=1, keepdims=True)
        lp = jnp.log((jnp.broadcast_to(n, (MB, 128)) + ALPHA) / norm_const)
        c = LOG2E * (lp - beta_next * msq)
        c_ref[rows, :] = c
        if share:
            crow_ref[:, rows] = to_row(c)

    def out_copy(slot, kb):
        size = (MB, FB)[slot]
        owner = data if slot == 0 else par
        rows = pl.ds(pl.multiple_of(owner * own + kb * size, size), size)
        return pltpu.make_async_remote_copy(
            src_ref=means_ref.at[rows], dst_ref=means_ref.at[rows], send_sem=out_send.at[slot, kb],
            recv_sem=out_recv.at[slot, kb], device_id=peer(1), device_id_type=MESH)

    def w_copy(slot):
        owner = data if slot == 0 else par
        return pltpu.make_async_remote_copy(
            src_ref=logw_ref.at[owner], dst_ref=logw_ref.at[owner], send_sem=w_send.at[slot], recv_sem=w_recv.at[slot],
            device_id=peer(1), device_id_type=MESH)

    def emit(slot, kb, n_acc, acc):
        size = (MB, FB)[slot]
        owner = data if slot == 0 else par
        n, mu = finish(n_acc, acc)
        means_ref[pl.ds(pl.multiple_of(owner * own + kb * size, size), size), :] = mu
        nrow = to_row(jnp.broadcast_to(n, (size, 128)))
        logw_ref[owner, :, pl.ds(pl.multiple_of(kb * size, size), size)] = jnp.log((nrow + ALPHA) / norm_const)
        out_copy(slot, kb).start()

    for t in range(sweeps):
        beta = temp_ref[t]
        tb = (2.0 * LOG2E) * beta
        last = t == sweeps - 1
        if t == 0:
            ld_pts.wait()
            for ch in range(n_ch):
                pts_copy(0, ch).wait_recv()
            lax.fori_loop(0, 2, lambda s, _: (e_step(0, xpos * 2 + s, tb), 0)[1], 0)

            def far_points(ch, _):
                pts_copy(1, ch).wait_recv()
                pts_copy(2, ch).start()
                e_tile(par * nq + ch * IB, tb)
                pts_copy(2, ch).wait_recv()
                e_tile(data_xor(3) * nq + ch * IB, tb)
                return 0

            lax.fori_loop(0, n_ch, far_points, 0)
            st_send_all(0, par)
            st_send_all(0, data_xor(3))
        else:
            lax.fori_loop(0, 4, lambda s, _: (e_step(t, (s % 2) * 2 + s // 2, tb), 0)[1], 0)
            if last:
                for j in range(EARLY, n_fb):
                    mu_copy(j).start()
        st_combine(t, 0)
        st_combine(t, 2)
        lax.fori_loop(0, n_mb, m_first, 0)
        st_combine(t, 1)
        st_combine(t, 3)
        if not last:
            beta_next = temp_ref[t + 1]
            share = t == sweeps - 2
            lax.fori_loop(0, n_mb, lambda kb, _: (m_second(kb, beta_next, share), 0)[1], 0)
            if share:
                c_copy().start()
                for j in range(EARLY):
                    mu_copy(j).start()
        else:
            def m_last(kb, _):
                rows = pl.ds(pl.multiple_of(kb * MB, MB), MB)
                n_acc, acc = m_block(kb, (1, 3))
                emit(0, kb, n_ref[rows, :] + n_acc, s_ref[rows, :] + acc)
                return 0

            lax.fori_loop(0, n_mb, m_last, 0)
            w_copy(0).start()
            c_copy().wait_recv()

            def far_block(kb, _):
                mu_copy(kb).wait_recv()
                rows = pl.ds(pl.multiple_of(kb * FB, FB), FB)
                c = to_col(cfrow_ref[:, rows])
                c2 = jnp.concatenate([c, c], axis=1)
                n_acc = jnp.zeros((FB, 128), F32)
                acc = jnp.zeros((FB, dim), F32)
                for ic in range(4 * n_ch):
                    cols = pl.ds(ic * IB, IB)
                    xt = x_ref[cols, :]
                    a = lax.dot_general(muf_ref[rows, :], xt, NT, preferred_element_type=F32)
                    r = jnp.exp2((a * tb + c2) - lse_ref[:, cols])
                    n_acc = n_acc + (r[:, :128] + r[:, 128:])
                    acc = acc + jnp.dot(r.astype(BF16), xt, preferred_element_type=F32)
                emit(1, kb, n_acc, acc)
                return 0

            lax.fori_loop(0, n_fb, far_block, 0)
            w_copy(1).start()
            mine = pl.ds(pl.multiple_of(data * nq, nq), nq)
            xo = x_ref[mine, :].astype(F32)
            sq = xo * xo
            hi = sq.astype(BF16)
            lo = (sq - hi.astype(F32)).astype(BF16)
            ones = jnp.ones((8, dim), BF16)
            row_sq = (lax.dot_general(ones, hi, NT, preferred_element_type=F32)
                      + lax.dot_general(ones, lo, NT, preferred_element_type=F32))
            lse_out_ref[...] = LN2 * lse_ref[:, mine] - beta * row_sq[0:1, :]

    for kind in range(3):
        for ch in range(n_ch):
            pts_copy(kind, ch).wait_send()
    for t in range(sweeps):
        for q in range(4):
            for r in range(1, 8):
                st_copy(t, q, r).wait_send()
    for j in range(n_fb):
        mu_copy(j).wait_send()
    c_copy().wait_send()
    for slot in range(2):
        w_copy(slot).wait_send()
        for kb in range((n_mb, n_fb)[slot]):
            out_copy(slot, kb).wait_send()

    def sibling(dev_slot):
        owner = (sib, data_xor(3))[dev_slot]
        size = (MB, FB)[dev_slot]
        for kb in range((n_mb, n_fb)[dev_slot]):
            rows = pl.ds(pl.multiple_of(owner * own + kb * size, size), size)
            pltpu.make_async_remote_copy(
                src_ref=means_ref.at[rows], dst_ref=means_ref.at[rows], send_sem=out_send.at[dev_slot, kb],
                recv_sem=out_recv.at[dev_slot, kb], device_id=peer(1), device_id_type=MESH).wait_recv()
        pltpu.make_async_remote_copy(
            src_ref=logw_ref.at[owner], dst_ref=logw_ref.at[owner], send_sem=w_send.at[dev_slot],
            recv_sem=w_recv.at[dev_slot], device_id=peer(1), device_id_type=MESH).wait_recv()

    sibling(0)
    sibling(1)


def solution(mesh):
    comp_size = mesh.shape["comp"]
    data_size = mesh.shape["data"]

    def local_fit(points, mu_init, logpi_init, inv_temp):
        nq, dim = points.shape
        rows = mu_init.shape[0]
        own = rows // data_size
        sweeps = inv_temp.shape[0]
        n_pts = nq * data_size
        n_kb = own // KB
        norm_const = n_pts + rows * comp_size * ALPHA
        cfg = (sweeps, own, nq, dim, norm_const)
        any_spec = pl.BlockSpec(memory_space=pl.ANY)
        vmem_spec = pl.BlockSpec(memory_space=pltpu.VMEM)
        dma = pltpu.SemaphoreType.DMA
        n_fb = own // FB
        means, logw, lse = pl.pallas_call(
            functools.partial(fit_kernel, cfg),
            out_shape=(pltpu.VMEM((rows, dim), F32),
                       pltpu.VMEM((data_size, 1, own), F32),
                       pltpu.VMEM((1, nq), F32)),
            in_specs=[pl.BlockSpec(memory_space=pltpu.SMEM), any_spec, any_spec, any_spec],
            out_specs=(vmem_spec, vmem_spec, vmem_spec),
            scratch_shapes=[
                pltpu.VMEM((n_pts, dim), BF16),
                pltpu.VMEM((own, n_pts), F32),
                pltpu.VMEM((own, dim), BF16),
                pltpu.VMEM((own, dim), BF16),
                pltpu.VMEM((own, 128), F32),
                pltpu.VMEM((1, own), F32),
                pltpu.VMEM((1, own), F32),
                pltpu.VMEM((own, dim), F32),
                pltpu.VMEM((own, 128), F32),
                pltpu.VMEM((own // KT, 8, n_pts), F32),
                pltpu.VMEM((own // KT, 8, n_pts), F32),
                pltpu.VMEM((1, n_pts), F32),
                pltpu.VMEM((sweeps, data_size, 8, 1, nq), F32),
                dma((3,)),
                dma((3, nq // IB)), dma((3, nq // IB)),
                dma((sweeps, 4, 8)), dma((sweeps, 4, 8)),
                dma((n_fb + 1,)), dma((n_fb + 1,)),
                dma((2, n_fb)), dma((2, n_fb)),
                dma((2,)), dma((2,)),
            ],
            compiler_params=pltpu.CompilerParams(
                collective_id=0, has_side_effects=True, vmem_limit_bytes=54 * 1024 * 1024),
        )(inv_temp, points, mu_init, logpi_init.reshape(data_size, 1, own))
        return means, logw.reshape(rows), lse.reshape(nq)

    row_spec = P(("fit", "data"), None)
    comp_spec = P(("fit", "comp"), None)
    weight_spec = P(("fit", "comp"))
    lse_spec = P(("fit", "data"))
    return jax.shard_map(local_fit, mesh=mesh, in_specs=(row_spec, comp_spec, weight_spec, P(None)), out_specs=(comp_spec, weight_spec, lse_spec), check_vma=False)
```

```python
import functools
import math

import jax
import jax.numpy as jnp
from jax import lax
from jax.experimental import pallas as pl
from jax.experimental.pallas import tpu as pltpu
from jax.sharding import PartitionSpec as P

EPS_COUNT = 1e-6
ALPHA = 1e-3
PIECES = 8
LOG2E = math.log2(math.e)
LN2 = math.log(2.0)
KB = 512
IB = 256
KT = 64
MB = 1024
EARLY = 3
FB = 256
MESH = pl.DeviceIdType.MESH
F32 = jnp.float32
BF16 = jnp.bfloat16
NT = (((1,), (1,)), ((), ()))


def fit_kernel(cfg, temp_ref, pts_ref, mu_ref, logpi_ref, means_ref, logw_ref, lse_out_ref,
               x_ref, p_ref, mub_ref, muf_ref, c_ref, crow_ref, cfrow_ref, s_ref, n_ref,
               m_ref, sum_ref, lse_ref, g_ref,
               loc_sem, q_sem, sib_send, pts_send, pts_recv, st_send, st_recv, mu_send, mu_recv,
               out_send, out_recv, w_send, w_recv):
    sweeps, own, nq, dim, norm_const = cfg
    n_kb = own // KB
    n_kt = own // KT
    n_mb = own // MB
    n_fb = own // FB
    n_ch = nq // IB
    fit = lax.axis_index("fit")
    comp = lax.axis_index("comp")
    data = lax.axis_index("data")
    xpos = data // 2

    def data_xor(d):
        if d == 0:
            return data
        if d == 1:
            return data + 1 - 2 * (data % 2)
        if d == 2:
            return (data + 2) % 4
        return (data + 1 - 2 * (data % 2) + 2) % 4

    def peer(r):
        return (fit, (comp + r // 4) % 2, data_xor(r % 4))

    sib, par = data_xor(1), data_xor(2)
    me = comp * 4 + data

    barrier = pltpu.get_barrier_semaphore()
    for r in range(1, 8):
        pl.semaphore_signal(barrier, inc=1, device_id=peer(r), device_id_type=MESH)

    def blk(i, size):
        return pl.ds(pl.multiple_of(i * size, size), size)

    ld_pts = pltpu.make_async_copy(pts_ref, x_ref.at[blk(data, nq)], q_sem.at[0])
    ld_mu = [pltpu.make_async_copy(mu_ref.at[blk(o, own)], means_ref.at[blk(o, own)], loc_sem.at[i])
             for i, o in enumerate((data, par))]
    ld_pi = [pltpu.make_async_copy(logpi_ref.at[o], dst, loc_sem.at[2 + i])
             for i, (o, dst) in enumerate(((data, crow_ref), (par, cfrow_ref)))]
    ld_pts.start()
    for cp in ld_mu + ld_pi:
        cp.start()
    pl.semaphore_wait(barrier, 7)

    def sib_copy():
        return pltpu.make_async_remote_copy(
            src_ref=pts_ref, dst_ref=x_ref.at[blk(data, nq)], send_sem=sib_send, recv_sem=q_sem.at[1],
            device_id=peer(1), device_id_type=MESH)

    def pts_copy(kind, ch):
        owner = (data, par)[kind]
        rows = blk(owner * n_ch + ch, IB)
        return pltpu.make_async_remote_copy(
            src_ref=pts_ref.at[pl.ds(ch * IB, IB)] if kind == 0 else x_ref.at[rows], dst_ref=x_ref.at[rows],
            send_sem=pts_send.at[kind, ch], recv_sem=pts_recv.at[kind, ch],
            device_id=peer(2 - kind), device_id_type=MESH)

    def pass_on(ch):
        pts_copy(0, ch).wait_recv()
        pts_copy(1, ch).start()

    for ch in range(n_ch):
        pts_copy(0, ch).start()
    sib_copy().start()

    def to_col(row):
        return jnp.transpose(jnp.broadcast_to(row, (128, row.shape[1])))

    def to_row(col):
        return jnp.transpose(col)[0:1, :]

    beta0 = temp_ref[0]
    for i, (o, low, row, col) in enumerate(((data, mub_ref, crow_ref, c_ref), (par, muf_ref, cfrow_ref, n_ref))):
        ld_mu[i].wait()
        ld_pi[i].wait()

        def init_body(kb, _, o=o, low=low, row=row, col=col):
            rows = blk(kb, KB)
            mu = means_ref[blk(o * n_kb + kb, KB), :]
            low[rows, :] = mu.astype(BF16)
            msq = jnp.sum(mu * mu, axis=1, keepdims=True)
            col[rows, :] = LOG2E * (to_col(row[:, rows]) - beta0 * msq)
            return 0

        lax.fori_loop(0, n_kb, init_body, 0)

    def e_tile(i0, tb, low, col, s0, keep):
        cols = pl.ds(pl.multiple_of(i0, IB), IB)
        scols = pl.ds(pl.multiple_of(s0, IB), IB)
        xt = x_ref[cols, :]
        for kb in range(n_kb):
            a = lax.dot_general(low[pl.ds(kb * KB, KB), :], xt, NT, preferred_element_type=F32)
            for u in range(KB // KT):
                rows = pl.ds(kb * KB + u * KT, KT)
                tile = kb * (KB // KT) + u
                cc = col[rows, :]
                l = a[u * KT:(u + 1) * KT, :] * tb + jnp.concatenate([cc, cc], axis=1)
                l3 = l.reshape(KT // 8, 8, IB)
                m = jnp.max(l3, axis=0)
                p3 = jnp.exp2(l3 - m[None])
                if keep:
                    p_ref[rows, cols] = p3.reshape(KT, IB)
                m_ref[tile, :, scols] = m
                sum_ref[tile, :, scols] = jnp.sum(p3, axis=0)

    def e_quarter(q, tb, low=mub_ref, col=c_ref, sq=None, keep=True):
        for it in range(n_ch):
            e_tile(q * nq + it * IB, tb, low, col, (q if sq is None else sq) * nq + it * IB, keep)

    def st_copy(t, q, r):
        return pltpu.make_async_remote_copy(
            src_ref=g_ref.at[t, q, me], dst_ref=g_ref.at[t, q, me], send_sem=st_send.at[t, q, r],
            recv_sem=st_recv.at[t, q, r], device_id=peer(r), device_id_type=MESH)

    def st_send_all(t, q, stats):
        cols = [blk(c, nq) for c in stats]
        top = functools.reduce(jnp.maximum, [jnp.max(m_ref[:, :, c], axis=0) for c in cols])
        top = jnp.max(top, axis=0, keepdims=True)
        tot = functools.reduce(lambda u, v: u + v,
                               [jnp.sum(sum_ref[pl.ds(k, 8), :, c] * jnp.exp2(m_ref[pl.ds(k, 8), :, c] - top), axis=0)
                                for c in cols for k in range(0, n_kt, 8)])
        tot = jnp.sum(tot, axis=0, keepdims=True)
        g_ref[t, q, me] = top + LOG2E * jnp.log(tot)
        for r in range(1, 8):
            st_copy(t, q, r).start()

    def e_step(t, q, tb):
        e_quarter(q, tb)
        st_send_all(t, q, (q,))

    def combine(q, vals):
        top = functools.reduce(jnp.maximum, [jnp.max(v, axis=0) for v in vals])
        tot = functools.reduce(lambda u, v: u + v, [jnp.sum(jnp.exp2(v - top[None]), axis=0) for v in vals])
        lse = top + LOG2E * jnp.log(tot)
        lse_ref[:, blk(q, nq)] = lse
        return lse

    def scale(q, lse):
        cols = blk(q, nq)
        m_ref[:, :, cols] = jnp.exp2(m_ref[:, :, cols] - lse)

    def st_combine(t, q):
        for r in range(1, 8):
            st_copy(t, q, r).wait_recv()
        scale(q, combine(q, [g_ref[t, q]]))

    def st_combine_four(q, x, rs):
        for r in rs:
            st_copy(0, q, r).wait_recv()
        return combine(q, [g_ref[0, q, pl.ds(4 * c + 2 * x, 2)] for c in range(2)])

    def m_block(kb, quarters):
        rows = pl.ds(pl.multiple_of(kb * MB, MB), MB)
        n_acc = jnp.zeros((MB, 128), F32)
        acc = jnp.zeros((MB, dim), F32)
        for q in quarters:
            for ic in range(n_ch):
                cols = blk(q * n_ch + ic, IB)
                sc = m_ref[pl.ds(kb * (MB // KT), MB // KT), :, cols]
                r = (p_ref[rows, cols].reshape(MB // KT, KT // 8, 8, IB) * sc[:, None]).reshape(MB, IB)
                n_acc = n_acc + (r[:, :128] + r[:, 128:])
                acc = acc + jnp.dot(r.astype(BF16), x_ref[cols, :], preferred_element_type=F32)
        return n_acc, acc

    def m_first(kb, quarters):
        rows = blk(kb, MB)
        n_acc, acc = m_block(kb, quarters)
        n_ref[rows, :] = n_acc
        s_ref[rows, :] = acc
        return 0

    def flash(low, rows, c, tb, chunks, size):
        c2 = jnp.concatenate([c, c], axis=1)
        n_acc = jnp.zeros((size, 128), F32)
        acc = jnp.zeros((size, dim), F32)
        for ch in chunks:
            cols = blk(ch, IB)
            xt = x_ref[cols, :]
            a = lax.dot_general(low[rows, :], xt, NT, preferred_element_type=F32)
            r = jnp.exp2((a * tb + c2) - lse_ref[:, cols])
            n_acc = n_acc + (r[:, :128] + r[:, 128:])
            acc = acc + jnp.dot(r.astype(BF16), xt, preferred_element_type=F32)
        return n_acc, acc

    def finish(n_acc, acc):
        n = jnp.sum(n_acc, axis=1, keepdims=True)
        mu = acc * (1.0 / (n + EPS_COUNT))
        return n, mu

    def mu_copy(j):
        rows = pl.ds(pl.multiple_of(j * FB, FB), FB)
        return pltpu.make_async_remote_copy(
            src_ref=mub_ref.at[rows], dst_ref=muf_ref.at[rows], send_sem=mu_send.at[j], recv_sem=mu_recv.at[j],
            device_id=peer(2), device_id_type=MESH)

    def c_copy():
        return pltpu.make_async_remote_copy(
            src_ref=crow_ref, dst_ref=cfrow_ref, send_sem=mu_send.at[n_fb], recv_sem=mu_recv.at[n_fb],
            device_id=peer(2), device_id_type=MESH)

    def renew(rows, size, n_acc, acc, beta_next, share):
        n, mu = finish(n_ref[rows, :] + n_acc, s_ref[rows, :] + acc)
        mub_ref[rows, :] = mu.astype(BF16)
        msq = jnp.sum(mu * mu, axis=1, keepdims=True)
        lp = jnp.log((jnp.broadcast_to(n, (size, 128)) + ALPHA) / norm_const)
        c = LOG2E * (lp - beta_next * msq)
        c_ref[rows, :] = c
        if share:
            crow_ref[:, rows] = to_row(c)
        return 0

    def out_copy(slot, kb):
        size = (MB, FB)[slot]
        owner = data if slot == 0 else par
        rows = pl.ds(pl.multiple_of(owner * own + kb * size, size), size)
        return pltpu.make_async_remote_copy(
            src_ref=means_ref.at[rows], dst_ref=means_ref.at[rows], send_sem=out_send.at[slot, kb],
            recv_sem=out_recv.at[slot, kb], device_id=peer(1), device_id_type=MESH)

    def w_copy(slot):
        owner = data if slot == 0 else par
        return pltpu.make_async_remote_copy(
            src_ref=logw_ref.at[owner], dst_ref=logw_ref.at[owner], send_sem=w_send.at[slot], recv_sem=w_recv.at[slot],
            device_id=peer(1), device_id_type=MESH)

    def emit(slot, kb, n_acc, acc):
        size = (MB, FB)[slot]
        owner = data if slot == 0 else par
        n, mu = finish(n_acc, acc)
        means_ref[pl.ds(pl.multiple_of(owner * own + kb * size, size), size), :] = mu
        nrow = to_row(jnp.broadcast_to(n, (size, 128)))
        logw_ref[owner, :, pl.ds(pl.multiple_of(kb * size, size), size)] = jnp.log((nrow + ALPHA) / norm_const)
        out_copy(slot, kb).start()

    for t in range(sweeps):
        beta = temp_ref[t]
        tb = (2.0 * LOG2E) * beta
        last = t == sweeps - 1
        if t == 0:
            def own_points(s, _):
                q = data + s * (sib - data)
                pltpu.make_async_copy(pts_ref, x_ref.at[blk(q, nq)], q_sem.at[s]).wait()
                far = (q + 2) % 4
                e_quarter(q, tb)
                e_quarter(q, tb, muf_ref, n_ref, far, False)
                st_send_all(0, q, (q, far))
                return 0

            lax.fori_loop(0, 2, own_points, 0)
            pass_on(0)
            pass_on(1)
            near = (xpos * 2, xpos * 2 + 1)
            away = ((1 - xpos) * 2, (1 - xpos) * 2 + 1)
            for q in near:
                scale(q, st_combine_four(q, xpos, (1, 4, 5)))
            lax.fori_loop(0, n_mb, lambda kb, _: m_first(kb, near), 0)
            pass_on(2)
            pass_on(3)
            for q in away:
                st_combine_four(q, 1 - xpos, (2, 3, 6, 7))
            for ch in range(n_ch):
                pts_copy(1, ch).wait_recv()
            beta_next = temp_ref[1]
            chunks = [q * n_ch + ic for q in away for ic in range(n_ch)]

            def away_block(kb, _):
                rows = blk(kb, KB)
                n_acc, acc = flash(mub_ref, rows, c_ref[rows, :], tb, chunks, KB)
                return renew(rows, KB, n_acc, acc, beta_next, False)

            lax.fori_loop(0, n_kb, away_block, 0)
            continue
        lax.fori_loop(0, 4, lambda s, _: (e_step(t, (s % 2) * 2 + s // 2, tb), 0)[1], 0)
        if last:
            for j in range(EARLY, n_fb):
                mu_copy(j).start()
        st_combine(t, 0)
        st_combine(t, 2)
        lax.fori_loop(0, n_mb, lambda kb, _: m_first(kb, (0, 2)), 0)
        st_combine(t, 1)
        st_combine(t, 3)
        if not last:
            beta_next = temp_ref[t + 1]
            share = t == sweeps - 2
            lax.fori_loop(0, n_mb, lambda kb, _: renew(blk(kb, MB), MB, *m_block(kb, (1, 3)), beta_next, share), 0)
            if share:
                c_copy().start()
                for j in range(EARLY):
                    mu_copy(j).start()
        else:
            def m_last(kb, _):
                rows = pl.ds(pl.multiple_of(kb * MB, MB), MB)
                n_acc, acc = m_block(kb, (1, 3))
                emit(0, kb, n_ref[rows, :] + n_acc, s_ref[rows, :] + acc)
                return 0

            lax.fori_loop(0, n_mb, m_last, 0)
            w_copy(0).start()
            c_copy().wait_recv()

            def far_block(kb, _):
                mu_copy(kb).wait_recv()
                rows = pl.ds(pl.multiple_of(kb * FB, FB), FB)
                n_acc, acc = flash(muf_ref, rows, to_col(cfrow_ref[:, rows]), tb, range(4 * n_ch), FB)
                emit(1, kb, n_acc, acc)
                return 0

            lax.fori_loop(0, n_fb, far_block, 0)
            w_copy(1).start()
            mine = pl.ds(pl.multiple_of(data * nq, nq), nq)
            xo = x_ref[mine, :].astype(F32)
            sq = xo * xo
            hi = sq.astype(BF16)
            lo = (sq - hi.astype(F32)).astype(BF16)
            ones = jnp.ones((8, dim), BF16)
            row_sq = (lax.dot_general(ones, hi, NT, preferred_element_type=F32)
                      + lax.dot_general(ones, lo, NT, preferred_element_type=F32))
            lse_out_ref[...] = LN2 * lse_ref[:, mine] - beta * row_sq[0:1, :]

    sib_copy().wait_send()
    for kind in range(2):
        for ch in range(n_ch):
            pts_copy(kind, ch).wait_send()
    for t in range(sweeps):
        for q in (near if t == 0 else range(4)):
            for r in range(1, 8):
                st_copy(t, q, r).wait_send()
    for j in range(n_fb):
        mu_copy(j).wait_send()
    c_copy().wait_send()
    for slot in range(2):
        w_copy(slot).wait_send()
        for kb in range((n_mb, n_fb)[slot]):
            out_copy(slot, kb).wait_send()

    def sibling(dev_slot):
        owner = (sib, data_xor(3))[dev_slot]
        size = (MB, FB)[dev_slot]
        for kb in range((n_mb, n_fb)[dev_slot]):
            rows = pl.ds(pl.multiple_of(owner * own + kb * size, size), size)
            pltpu.make_async_remote_copy(
                src_ref=means_ref.at[rows], dst_ref=means_ref.at[rows], send_sem=out_send.at[dev_slot, kb],
                recv_sem=out_recv.at[dev_slot, kb], device_id=peer(1), device_id_type=MESH).wait_recv()
        pltpu.make_async_remote_copy(
            src_ref=logw_ref.at[owner], dst_ref=logw_ref.at[owner], send_sem=w_send.at[dev_slot],
            recv_sem=w_recv.at[dev_slot], device_id=peer(1), device_id_type=MESH).wait_recv()

    sibling(0)
    sibling(1)


def flush_kernel(means_ref, logw_ref, lse_ref, means_out, logw_out, lse_out, sem):
    rows = means_ref.shape[0] // PIECES
    copies = [pltpu.make_async_copy(means_ref.at[pl.ds(i * rows, rows)], means_out.at[pl.ds(i * rows, rows)], sem.at[i])
              for i in range(PIECES)]
    copies.append(pltpu.make_async_copy(logw_ref, logw_out, sem.at[PIECES]))
    copies.append(pltpu.make_async_copy(lse_ref, lse_out, sem.at[PIECES + 1]))
    for cp in copies:
        cp.start()
    for cp in copies:
        cp.wait()


def solution(mesh):
    comp_size = mesh.shape["comp"]
    data_size = mesh.shape["data"]

    def local_fit(points, mu_init, logpi_init, inv_temp):
        nq, dim = points.shape
        rows = mu_init.shape[0]
        own = rows // data_size
        sweeps = inv_temp.shape[0]
        n_pts = nq * data_size
        n_kb = own // KB
        norm_const = n_pts + rows * comp_size * ALPHA
        cfg = (sweeps, own, nq, dim, norm_const)
        any_spec = pl.BlockSpec(memory_space=pl.ANY)
        vmem_spec = pl.BlockSpec(memory_space=pltpu.VMEM)
        dma = pltpu.SemaphoreType.DMA
        n_fb = own // FB
        means, logw, lse = pl.pallas_call(
            functools.partial(fit_kernel, cfg),
            out_shape=(pltpu.VMEM((rows, dim), F32),
                       pltpu.VMEM((data_size, 1, own), F32),
                       pltpu.VMEM((1, nq), F32)),
            in_specs=[pl.BlockSpec(memory_space=pltpu.SMEM), any_spec, any_spec, any_spec],
            out_specs=(vmem_spec, vmem_spec, vmem_spec),
            scratch_shapes=[
                pltpu.VMEM((n_pts, dim), BF16),
                pltpu.VMEM((own, n_pts), F32),
                pltpu.VMEM((own, dim), BF16),
                pltpu.VMEM((own, dim), BF16),
                pltpu.VMEM((own, 128), F32),
                pltpu.VMEM((1, own), F32),
                pltpu.VMEM((1, own), F32),
                pltpu.VMEM((own, dim), F32),
                pltpu.VMEM((own, 128), F32),
                pltpu.VMEM((own // KT, 8, n_pts), F32),
                pltpu.VMEM((own // KT, 8, n_pts), F32),
                pltpu.VMEM((1, n_pts), F32),
                pltpu.VMEM((sweeps, data_size, 8, 1, nq), F32),
                dma((4,)), dma((2,)), dma,
                dma((2, nq // IB)), dma((2, nq // IB)),
                dma((sweeps, 4, 8)), dma((sweeps, 4, 8)),
                dma((n_fb + 1,)), dma((n_fb + 1,)),
                dma((2, n_fb)), dma((2, n_fb)),
                dma((2,)), dma((2,)),
            ],
            compiler_params=pltpu.CompilerParams(
                collective_id=0, has_side_effects=True, vmem_limit_bytes=54 * 1024 * 1024),
        )(inv_temp, points, mu_init, logpi_init.reshape(data_size, 1, own))
        results = [pltpu.with_memory_space_constraint(v, pltpu.VMEM) for v in (means, logw, lse)]
        means, logw, lse = pl.pallas_call(
            flush_kernel,
            out_shape=tuple(jax.ShapeDtypeStruct(v.shape, F32) for v in results),
            in_specs=[vmem_spec] * 3,
            out_specs=(any_spec,) * 3,
            scratch_shapes=[dma((PIECES + 2,))],
            compiler_params=pltpu.CompilerParams(vmem_limit_bytes=16 * 1024 * 1024),
        )(*results)
        return means, logw.reshape(rows), lse.reshape(nq)

    row_spec = P(("fit", "data"), None)
    comp_spec = P(("fit", "comp"), None)
    weight_spec = P(("fit", "comp"))
    lse_spec = P(("fit", "data"))
    return jax.shard_map(local_fit, mesh=mesh, in_specs=(row_spec, comp_spec, weight_spec, P(None)), out_specs=(comp_spec, weight_spec, lse_spec), check_vma=False)
```

```python
import functools
import math

import jax
import jax.numpy as jnp
from jax import lax
from jax.experimental import pallas as pl
from jax.experimental.pallas import tpu as pltpu
from jax.sharding import PartitionSpec as P

EPS_COUNT = 1e-6
ALPHA = 1e-3
PIECES = 8
LOG2E = math.log2(math.e)
LN2 = math.log(2.0)
KB = 512
IB = 256
KT = 64
MB = 1024
EARLY = 3
FB = 256
MESH = pl.DeviceIdType.MESH
F32 = jnp.float32
BF16 = jnp.bfloat16
NT = (((1,), (1,)), ((), ()))


def fit_kernel(cfg, temp_ref, pts_ref, mu_ref, logpi_ref, means_ref, logw_ref, lse_out_ref,
               x_ref, p_ref, mub_ref, muf_ref, c_ref, crow_ref, cfrow_ref, s_ref, n_ref,
               m_ref, sum_ref, lse_ref, g_ref,
               loc_sem, q_sem, sib_send, pts_send, pts_recv, st_send, st_recv, mu_send, mu_recv,
               out_send, out_recv, w_send, w_recv):
    sweeps, own, nq, dim, norm_const = cfg
    n_kb = own // KB
    n_kt = own // KT
    n_mb = own // MB
    n_fb = own // FB
    n_ch = nq // IB
    fit = lax.axis_index("fit")
    comp = lax.axis_index("comp")
    data = lax.axis_index("data")
    xpos = data // 2

    def data_xor(d):
        if d == 0:
            return data
        if d == 1:
            return data + 1 - 2 * (data % 2)
        if d == 2:
            return (data + 2) % 4
        return (data + 1 - 2 * (data % 2) + 2) % 4

    def peer(r):
        return (fit, (comp + r // 4) % 2, data_xor(r % 4))

    sib, par = data_xor(1), data_xor(2)
    me = comp * 4 + data

    barrier = pltpu.get_barrier_semaphore()
    for r in range(1, 8):
        pl.semaphore_signal(barrier, inc=1, device_id=peer(r), device_id_type=MESH)

    def blk(i, size):
        return pl.ds(pl.multiple_of(i * size, size), size)

    ld_pts = pltpu.make_async_copy(pts_ref, x_ref.at[blk(data, nq)], q_sem.at[0])
    ld_mu = [pltpu.make_async_copy(mu_ref.at[blk(o, own)], means_ref.at[blk(o, own)], loc_sem.at[i])
             for i, o in enumerate((data, par))]
    ld_pi = [pltpu.make_async_copy(logpi_ref.at[o], dst, loc_sem.at[2 + i])
             for i, (o, dst) in enumerate(((data, crow_ref), (par, cfrow_ref)))]
    ld_pts.start()
    for cp in ld_mu + ld_pi:
        cp.start()
    pl.semaphore_wait(barrier, 7)

    def sib_copy():
        return pltpu.make_async_remote_copy(
            src_ref=pts_ref, dst_ref=x_ref.at[blk(data, nq)], send_sem=sib_send, recv_sem=q_sem.at[1],
            device_id=peer(1), device_id_type=MESH)

    def pts_copy(kind, ch):
        owner = (data, par)[kind]
        rows = blk(owner * n_ch + ch, IB)
        return pltpu.make_async_remote_copy(
            src_ref=pts_ref.at[pl.ds(ch * IB, IB)] if kind == 0 else x_ref.at[rows], dst_ref=x_ref.at[rows],
            send_sem=pts_send.at[kind, ch], recv_sem=pts_recv.at[kind, ch],
            device_id=peer(2 - kind), device_id_type=MESH)

    def pass_on(ch):
        pts_copy(0, ch).wait_recv()
        pts_copy(1, ch).start()

    sib_copy().start()
    for ch in range(n_ch):
        pts_copy(0, ch).start()

    def to_col(row):
        return jnp.transpose(jnp.broadcast_to(row, (128, row.shape[1])))

    def to_row(col):
        return jnp.transpose(col)[0:1, :]

    beta0 = temp_ref[0]
    for i, (o, low, row, col) in enumerate(((data, mub_ref, crow_ref, c_ref), (par, muf_ref, cfrow_ref, n_ref))):
        ld_mu[i].wait()
        ld_pi[i].wait()

        def init_body(kb, _, o=o, low=low, row=row, col=col):
            rows = blk(kb, KB)
            mu = means_ref[blk(o * n_kb + kb, KB), :]
            low[rows, :] = mu.astype(BF16)
            msq = jnp.sum(mu * mu, axis=1, keepdims=True)
            col[rows, :] = LOG2E * (to_col(row[:, rows]) - beta0 * msq)
            return 0

        lax.fori_loop(0, n_kb, init_body, 0)

    def e_tile(i0, tb, low, col, s0, keep):
        cols = pl.ds(pl.multiple_of(i0, IB), IB)
        scols = pl.ds(pl.multiple_of(s0, IB), IB)
        xt = x_ref[cols, :]
        for kb in range(n_kb):
            a = lax.dot_general(low[pl.ds(kb * KB, KB), :], xt, NT, preferred_element_type=F32)
            for u in range(KB // KT):
                rows = pl.ds(kb * KB + u * KT, KT)
                tile = kb * (KB // KT) + u
                cc = col[rows, :]
                l = a[u * KT:(u + 1) * KT, :] * tb + jnp.concatenate([cc, cc], axis=1)
                l3 = l.reshape(KT // 8, 8, IB)
                m = jnp.max(l3, axis=0)
                p3 = jnp.exp2(l3 - m[None])
                if keep:
                    p_ref[rows, cols] = p3.reshape(KT, IB)
                m_ref[tile, :, scols] = m
                sum_ref[tile, :, scols] = jnp.sum(p3, axis=0)

    def e_quarter(q, tb, low=mub_ref, col=c_ref, sq=None, keep=True):
        for it in range(n_ch):
            e_tile(q * nq + it * IB, tb, low, col, (q if sq is None else sq) * nq + it * IB, keep)

    def st_copy(t, q, r):
        return pltpu.make_async_remote_copy(
            src_ref=g_ref.at[t, q, me], dst_ref=g_ref.at[t, q, me], send_sem=st_send.at[t, q, r],
            recv_sem=st_recv.at[t, q, r], device_id=peer(r), device_id_type=MESH)

    def st_send_all(t, q, stats):
        cols = [blk(c, nq) for c in stats]
        top = functools.reduce(jnp.maximum, [jnp.max(m_ref[:, :, c], axis=0) for c in cols])
        top = jnp.max(top, axis=0, keepdims=True)
        tot = functools.reduce(lambda u, v: u + v,
                               [jnp.sum(sum_ref[pl.ds(k, 8), :, c] * jnp.exp2(m_ref[pl.ds(k, 8), :, c] - top), axis=0)
                                for c in cols for k in range(0, n_kt, 8)])
        tot = jnp.sum(tot, axis=0, keepdims=True)
        g_ref[t, q, me] = top + LOG2E * jnp.log(tot)
        for r in ((5, 4, 1, 6, 7, 2, 3) if t == 0 else (6, 7, 2, 3, 5, 4, 1)):
            st_copy(t, q, r).start()

    def e_step(t, q, tb):
        e_quarter(q, tb)
        st_send_all(t, q, (q,))

    def combine(q, vals):
        top = functools.reduce(jnp.maximum, [jnp.max(v, axis=0) for v in vals])
        tot = functools.reduce(lambda u, v: u + v, [jnp.sum(jnp.exp2(v - top[None]), axis=0) for v in vals])
        lse = top + LOG2E * jnp.log(tot)
        lse_ref[:, blk(q, nq)] = lse
        return lse

    def scale(q, lse):
        cols = blk(q, nq)
        m_ref[:, :, cols] = jnp.exp2(m_ref[:, :, cols] - lse)

    def st_combine(t, q):
        for r in range(1, 8):
            st_copy(t, q, r).wait_recv()
        scale(q, combine(q, [g_ref[t, q]]))

    def st_combine_four(q, x, rs):
        for r in rs:
            st_copy(0, q, r).wait_recv()
        return combine(q, [g_ref[0, q, pl.ds(4 * c + 2 * x, 2)] for c in range(2)])

    def m_block(kb, quarters):
        rows = pl.ds(pl.multiple_of(kb * MB, MB), MB)
        n_acc = jnp.zeros((MB, 128), F32)
        acc = jnp.zeros((MB, dim), F32)
        for q in quarters:
            for ic in range(n_ch):
                cols = blk(q * n_ch + ic, IB)
                sc = m_ref[pl.ds(kb * (MB // KT), MB // KT), :, cols]
                r = (p_ref[rows, cols].reshape(MB // KT, KT // 8, 8, IB) * sc[:, None]).reshape(MB, IB)
                n_acc = n_acc + (r[:, :128] + r[:, 128:])
                acc = acc + jnp.dot(r.astype(BF16), x_ref[cols, :], preferred_element_type=F32)
        return n_acc, acc

    def m_first(kb, quarters):
        rows = blk(kb, MB)
        n_acc, acc = m_block(kb, quarters)
        n_ref[rows, :] = n_acc
        s_ref[rows, :] = acc
        return 0

    def flash(low, rows, c, tb, chunks, size):
        c2 = jnp.concatenate([c, c], axis=1)
        n_acc = jnp.zeros((size, 128), F32)
        acc = jnp.zeros((size, dim), F32)
        for ch in chunks:
            cols = blk(ch, IB)
            xt = x_ref[cols, :]
            a = lax.dot_general(low[rows, :], xt, NT, preferred_element_type=F32)
            r = jnp.exp2((a * tb + c2) - lse_ref[:, cols])
            n_acc = n_acc + (r[:, :128] + r[:, 128:])
            acc = acc + jnp.dot(r.astype(BF16), xt, preferred_element_type=F32)
        return n_acc, acc

    def finish(n_acc, acc):
        n = jnp.sum(n_acc, axis=1, keepdims=True)
        mu = acc * (1.0 / (n + EPS_COUNT))
        return n, mu

    def mu_copy(j):
        rows = pl.ds(pl.multiple_of(j * FB, FB), FB)
        return pltpu.make_async_remote_copy(
            src_ref=mub_ref.at[rows], dst_ref=muf_ref.at[rows], send_sem=mu_send.at[j], recv_sem=mu_recv.at[j],
            device_id=peer(2), device_id_type=MESH)

    def c_copy():
        return pltpu.make_async_remote_copy(
            src_ref=crow_ref, dst_ref=cfrow_ref, send_sem=mu_send.at[n_fb], recv_sem=mu_recv.at[n_fb],
            device_id=peer(2), device_id_type=MESH)

    def renew(rows, size, n_acc, acc, beta_next, share):
        n, mu = finish(n_ref[rows, :] + n_acc, s_ref[rows, :] + acc)
        mub_ref[rows, :] = mu.astype(BF16)
        msq = jnp.sum(mu * mu, axis=1, keepdims=True)
        lp = jnp.log((jnp.broadcast_to(n, (size, 128)) + ALPHA) / norm_const)
        c = LOG2E * (lp - beta_next * msq)
        c_ref[rows, :] = c
        if share:
            crow_ref[:, rows] = to_row(c)
        return 0

    def out_copy(slot, kb):
        size = (MB, FB)[slot]
        owner = data if slot == 0 else par
        rows = pl.ds(pl.multiple_of(owner * own + kb * size, size), size)
        return pltpu.make_async_remote_copy(
            src_ref=means_ref.at[rows], dst_ref=means_ref.at[rows], send_sem=out_send.at[slot, kb],
            recv_sem=out_recv.at[slot, kb], device_id=peer(1), device_id_type=MESH)

    def w_copy(slot):
        owner = data if slot == 0 else par
        return pltpu.make_async_remote_copy(
            src_ref=logw_ref.at[owner], dst_ref=logw_ref.at[owner], send_sem=w_send.at[slot], recv_sem=w_recv.at[slot],
            device_id=peer(1), device_id_type=MESH)

    def emit(slot, kb, n_acc, acc):
        size = (MB, FB)[slot]
        owner = data if slot == 0 else par
        n, mu = finish(n_acc, acc)
        means_ref[pl.ds(pl.multiple_of(owner * own + kb * size, size), size), :] = mu
        nrow = to_row(jnp.broadcast_to(n, (size, 128)))
        logw_ref[owner, :, pl.ds(pl.multiple_of(kb * size, size), size)] = jnp.log((nrow + ALPHA) / norm_const)
        out_copy(slot, kb).start()

    for t in range(sweeps):
        beta = temp_ref[t]
        tb = (2.0 * LOG2E) * beta
        last = t == sweeps - 1
        if t == 0:
            def own_points(s, _):
                q = data + s * (sib - data)
                pltpu.make_async_copy(pts_ref, x_ref.at[blk(q, nq)], q_sem.at[s]).wait()
                far = (q + 2) % 4
                e_quarter(q, tb)
                e_quarter(q, tb, muf_ref, n_ref, far, False)
                st_send_all(0, q, (q, far))
                return 0

            lax.fori_loop(0, 2, own_points, 0)
            pass_on(0)
            pass_on(1)
            near = (xpos * 2, xpos * 2 + 1)
            away = ((1 - xpos) * 2, (1 - xpos) * 2 + 1)
            for q in near:
                scale(q, st_combine_four(q, xpos, (1, 4, 5)))
            lax.fori_loop(0, n_mb, lambda kb, _: m_first(kb, near), 0)
            pass_on(2)
            pass_on(3)
            for q in away:
                st_combine_four(q, 1 - xpos, (2, 3, 6, 7))
            for ch in range(n_ch):
                pts_copy(1, ch).wait_recv()
            beta_next = temp_ref[1]
            chunks = [q * n_ch + ic for q in away for ic in range(n_ch)]

            def away_block(kb, _):
                rows = blk(kb, KB)
                n_acc, acc = flash(mub_ref, rows, c_ref[rows, :], tb, chunks, KB)
                return renew(rows, KB, n_acc, acc, beta_next, False)

            lax.fori_loop(0, n_kb, away_block, 0)
            continue
        lax.fori_loop(0, 4, lambda s, _: (e_step(t, (s % 2) * 2 + s // 2, tb), 0)[1], 0)
        if last:
            for j in range(EARLY, n_fb):
                mu_copy(j).start()
        st_combine(t, 0)
        st_combine(t, 2)
        lax.fori_loop(0, n_mb, lambda kb, _: m_first(kb, (0, 2)), 0)
        st_combine(t, 1)
        st_combine(t, 3)
        if not last:
            beta_next = temp_ref[t + 1]
            share = t == sweeps - 2
            lax.fori_loop(0, n_mb, lambda kb, _: renew(blk(kb, MB), MB, *m_block(kb, (1, 3)), beta_next, share), 0)
            if share:
                c_copy().start()
                for j in range(EARLY):
                    mu_copy(j).start()
        else:
            def m_last(kb, _):
                rows = pl.ds(pl.multiple_of(kb * MB, MB), MB)
                n_acc, acc = m_block(kb, (1, 3))
                emit(0, kb, n_ref[rows, :] + n_acc, s_ref[rows, :] + acc)
                return 0

            lax.fori_loop(0, n_mb, m_last, 0)
            w_copy(0).start()
            c_copy().wait_recv()

            def far_block(kb, _):
                mu_copy(kb).wait_recv()
                rows = pl.ds(pl.multiple_of(kb * FB, FB), FB)
                n_acc, acc = flash(muf_ref, rows, to_col(cfrow_ref[:, rows]), tb, range(4 * n_ch), FB)
                emit(1, kb, n_acc, acc)
                return 0

            lax.fori_loop(0, n_fb, far_block, 0)
            w_copy(1).start()
            mine = pl.ds(pl.multiple_of(data * nq, nq), nq)
            xo = x_ref[mine, :].astype(F32)
            sq = xo * xo
            hi = sq.astype(BF16)
            lo = (sq - hi.astype(F32)).astype(BF16)
            ones = jnp.ones((8, dim), BF16)
            row_sq = (lax.dot_general(ones, hi, NT, preferred_element_type=F32)
                      + lax.dot_general(ones, lo, NT, preferred_element_type=F32))
            lse_out_ref[...] = LN2 * lse_ref[:, mine] - beta * row_sq[0:1, :]

    sib_copy().wait_send()
    for kind in range(2):
        for ch in range(n_ch):
            pts_copy(kind, ch).wait_send()
    for t in range(sweeps):
        for q in (near if t == 0 else range(4)):
            for r in range(1, 8):
                st_copy(t, q, r).wait_send()
    for j in range(n_fb):
        mu_copy(j).wait_send()
    c_copy().wait_send()
    for slot in range(2):
        w_copy(slot).wait_send()
        for kb in range((n_mb, n_fb)[slot]):
            out_copy(slot, kb).wait_send()

    def sibling(dev_slot):
        owner = (sib, data_xor(3))[dev_slot]
        size = (MB, FB)[dev_slot]
        for kb in range((n_mb, n_fb)[dev_slot]):
            rows = pl.ds(pl.multiple_of(owner * own + kb * size, size), size)
            pltpu.make_async_remote_copy(
                src_ref=means_ref.at[rows], dst_ref=means_ref.at[rows], send_sem=out_send.at[dev_slot, kb],
                recv_sem=out_recv.at[dev_slot, kb], device_id=peer(1), device_id_type=MESH).wait_recv()
        pltpu.make_async_remote_copy(
            src_ref=logw_ref.at[owner], dst_ref=logw_ref.at[owner], send_sem=w_send.at[dev_slot],
            recv_sem=w_recv.at[dev_slot], device_id=peer(1), device_id_type=MESH).wait_recv()

    sibling(0)
    sibling(1)


def flush_kernel(means_ref, logw_ref, lse_ref, means_out, logw_out, lse_out, sem):
    rows = means_ref.shape[0] // PIECES
    copies = [pltpu.make_async_copy(means_ref.at[pl.ds(i * rows, rows)], means_out.at[pl.ds(i * rows, rows)], sem.at[i])
              for i in range(PIECES)]
    copies.append(pltpu.make_async_copy(logw_ref, logw_out, sem.at[PIECES]))
    copies.append(pltpu.make_async_copy(lse_ref, lse_out, sem.at[PIECES + 1]))
    for cp in copies:
        cp.start()
    for cp in copies:
        cp.wait()


def solution(mesh):
    comp_size = mesh.shape["comp"]
    data_size = mesh.shape["data"]

    def local_fit(points, mu_init, logpi_init, inv_temp):
        nq, dim = points.shape
        rows = mu_init.shape[0]
        own = rows // data_size
        sweeps = inv_temp.shape[0]
        n_pts = nq * data_size
        n_kb = own // KB
        norm_const = n_pts + rows * comp_size * ALPHA
        cfg = (sweeps, own, nq, dim, norm_const)
        any_spec = pl.BlockSpec(memory_space=pl.ANY)
        vmem_spec = pl.BlockSpec(memory_space=pltpu.VMEM)
        dma = pltpu.SemaphoreType.DMA
        n_fb = own // FB
        means, logw, lse = pl.pallas_call(
            functools.partial(fit_kernel, cfg),
            out_shape=(pltpu.VMEM((rows, dim), F32),
                       pltpu.VMEM((data_size, 1, own), F32),
                       pltpu.VMEM((1, nq), F32)),
            in_specs=[pl.BlockSpec(memory_space=pltpu.SMEM), any_spec, any_spec, any_spec],
            out_specs=(vmem_spec, vmem_spec, vmem_spec),
            scratch_shapes=[
                pltpu.VMEM((n_pts, dim), BF16),
                pltpu.VMEM((own, n_pts), F32),
                pltpu.VMEM((own, dim), BF16),
                pltpu.VMEM((own, dim), BF16),
                pltpu.VMEM((own, 128), F32),
                pltpu.VMEM((1, own), F32),
                pltpu.VMEM((1, own), F32),
                pltpu.VMEM((own, dim), F32),
                pltpu.VMEM((own, 128), F32),
                pltpu.VMEM((own // KT, 8, n_pts), F32),
                pltpu.VMEM((own // KT, 8, n_pts), F32),
                pltpu.VMEM((1, n_pts), F32),
                pltpu.VMEM((sweeps, data_size, 8, 1, nq), F32),
                dma((4,)), dma((2,)), dma,
                dma((2, nq // IB)), dma((2, nq // IB)),
                dma((sweeps, 4, 8)), dma((sweeps, 4, 8)),
                dma((n_fb + 1,)), dma((n_fb + 1,)),
                dma((2, n_fb)), dma((2, n_fb)),
                dma((2,)), dma((2,)),
            ],
            compiler_params=pltpu.CompilerParams(
                collective_id=0, has_side_effects=True, vmem_limit_bytes=54 * 1024 * 1024),
        )(inv_temp, points, mu_init, logpi_init.reshape(data_size, 1, own))
        results = [pltpu.with_memory_space_constraint(v, pltpu.VMEM) for v in (means, logw, lse)]
        means, logw, lse = pl.pallas_call(
            flush_kernel,
            out_shape=tuple(jax.ShapeDtypeStruct(v.shape, F32) for v in results),
            in_specs=[vmem_spec] * 3,
            out_specs=(any_spec,) * 3,
            scratch_shapes=[dma((PIECES + 2,))],
            compiler_params=pltpu.CompilerParams(vmem_limit_bytes=16 * 1024 * 1024),
        )(*results)
        return means, logw.reshape(rows), lse.reshape(nq)

    row_spec = P(("fit", "data"), None)
    comp_spec = P(("fit", "comp"), None)
    weight_spec = P(("fit", "comp"))
    lse_spec = P(("fit", "data"))
    return jax.shard_map(local_fit, mesh=mesh, in_specs=(row_spec, comp_spec, weight_spec, P(None)), out_specs=(comp_spec, weight_spec, lse_spec), check_vma=False)
```

```python
import functools
import math

import jax
import jax.numpy as jnp
from jax import lax
from jax.experimental import pallas as pl
from jax.experimental.pallas import tpu as pltpu
from jax.sharding import PartitionSpec as P

EPS_COUNT = 1e-6
ALPHA = 1e-3
PIECES = 8
LOG2E = math.log2(math.e)
LN2 = math.log(2.0)
KB = 1024
IB = 256
KT = 64
MB = 1024
EARLY = 3
SB = 256
FB = 512
MESH = pl.DeviceIdType.MESH
F32 = jnp.float32
BF16 = jnp.bfloat16
NN = (((1,), (0,)), ((), ()))
NT = (((1,), (1,)), ((), ()))


def fit_kernel(cfg, temp_ref, pts_ref, mu_ref, logpi_ref, means_ref, logw_ref, lse_out_ref,
               x_ref, xt_ref, p_ref, mub_ref, muf_ref, c_ref, crow_ref, cfrow_ref, s_ref, n_ref,
               m_ref, sum_ref, lse_ref, g_ref,
               loc_sem, q_sem, sib_send, pts_send, pts_recv, st_send, st_recv, mu_send, mu_recv,
               out_send, out_recv, w_send, w_recv):
    sweeps, own, nq, dim, norm_const = cfg
    n_kb = own // KB
    n_kt = own // KT
    n_mb = own // MB
    n_fb = own // FB
    n_sb = own // SB
    n_ch = nq // IB
    fit = lax.axis_index("fit")
    comp = lax.axis_index("comp")
    data = lax.axis_index("data")
    xpos = data // 2

    def data_xor(d):
        if d == 0:
            return data
        if d == 1:
            return data + 1 - 2 * (data % 2)
        if d == 2:
            return (data + 2) % 4
        return (data + 1 - 2 * (data % 2) + 2) % 4

    def peer(r):
        return (fit, (comp + r // 4) % 2, data_xor(r % 4))

    sib, par = data_xor(1), data_xor(2)
    me = comp * 4 + data

    barrier = pltpu.get_barrier_semaphore()
    for r in range(1, 8):
        pl.semaphore_signal(barrier, inc=1, device_id=peer(r), device_id_type=MESH)

    def blk(i, size):
        return pl.ds(pl.multiple_of(i * size, size), size)

    ld_pts = pltpu.make_async_copy(pts_ref, x_ref.at[blk(data, nq)], q_sem.at[0])
    ld_mu = [pltpu.make_async_copy(mu_ref.at[blk(o, own)], means_ref.at[blk(o, own)], loc_sem.at[i])
             for i, o in enumerate((data, par))]
    ld_pi = [pltpu.make_async_copy(logpi_ref.at[o], dst, loc_sem.at[2 + i])
             for i, (o, dst) in enumerate(((data, crow_ref), (par, cfrow_ref)))]
    ld_pts.start()
    for cp in ld_mu + ld_pi:
        cp.start()
    pl.semaphore_wait(barrier, 7)

    def sib_copy():
        return pltpu.make_async_remote_copy(
            src_ref=pts_ref, dst_ref=x_ref.at[blk(data, nq)], send_sem=sib_send, recv_sem=q_sem.at[1],
            device_id=peer(1), device_id_type=MESH)

    def pts_copy(kind, ch):
        owner = (data, par)[kind]
        rows = blk(owner * n_ch + ch, IB)
        return pltpu.make_async_remote_copy(
            src_ref=pts_ref.at[pl.ds(ch * IB, IB)] if kind == 0 else x_ref.at[rows], dst_ref=x_ref.at[rows],
            send_sem=pts_send.at[kind, ch], recv_sem=pts_recv.at[kind, ch],
            device_id=peer(2 - kind), device_id_type=MESH)

    def pass_on(ch):
        pts_copy(0, ch).wait_recv()
        pts_copy(1, ch).start()

    sib_copy().start()
    for ch in range(n_ch):
        pts_copy(0, ch).start()

    def to_col(row):
        return jnp.transpose(jnp.broadcast_to(row, (128, row.shape[1])))

    def to_row(col):
        return jnp.transpose(col)[0:1, :]

    beta0 = temp_ref[0]
    for i, (o, low, row, col) in enumerate(((data, mub_ref, crow_ref, c_ref), (par, muf_ref, cfrow_ref, n_ref))):
        ld_mu[i].wait()
        ld_pi[i].wait()

        def init_body(kb, _, o=o, low=low, row=row, col=col):
            rows = blk(kb, KB)
            mu = means_ref[blk(o * n_kb + kb, KB), :]
            low[rows, :] = mu.astype(BF16)
            msq = jnp.sum(mu * mu, axis=1, keepdims=True)
            col[rows, :] = LOG2E * (to_col(row[:, rows]) - beta0 * msq)
            return 0

        lax.fori_loop(0, n_kb, init_body, 0)

    def e_tile(i0, tb, low, col, s0, keep, first):
        cols = pl.ds(pl.multiple_of(i0, IB), IB)
        scols = pl.ds(pl.multiple_of(s0, IB), IB)
        if first:
            xt_ref[:, cols] = jnp.transpose(x_ref[cols, :])
        xt = xt_ref[:, cols]
        for kb in range(n_kb):
            a = lax.dot_general(low[pl.ds(kb * KB, KB), :], xt, NN, preferred_element_type=F32)
            for u in range(KB // KT):
                rows = pl.ds(kb * KB + u * KT, KT)
                tile = kb * (KB // KT) + u
                cc = col[rows, :]
                l = a[u * KT:(u + 1) * KT, :] * tb + jnp.concatenate([cc, cc], axis=1)
                l3 = l.reshape(KT // 8, 8, IB)
                m = jnp.max(l3, axis=0)
                p3 = jnp.exp2(l3 - m[None])
                if keep:
                    p_ref[rows, cols] = p3.reshape(KT, IB)
                m_ref[tile, :, scols] = m
                sum_ref[tile, :, scols] = jnp.sum(p3, axis=0)

    def e_quarter(q, tb, low=mub_ref, col=c_ref, sq=None, keep=True, first=False):
        for it in range(n_ch):
            e_tile(q * nq + it * IB, tb, low, col, (q if sq is None else sq) * nq + it * IB, keep, first)

    def st_copy(t, q, r):
        return pltpu.make_async_remote_copy(
            src_ref=g_ref.at[t, q, me], dst_ref=g_ref.at[t, q, me], send_sem=st_send.at[t, q, r],
            recv_sem=st_recv.at[t, q, r], device_id=peer(r), device_id_type=MESH)

    def st_send_all(t, q, stats):
        cols = [blk(c, nq) for c in stats]
        top = functools.reduce(jnp.maximum, [jnp.max(m_ref[:, :, c], axis=0) for c in cols])
        top = jnp.max(top, axis=0, keepdims=True)
        tot = functools.reduce(lambda u, v: u + v,
                               [jnp.sum(sum_ref[pl.ds(k, 8), :, c] * jnp.exp2(m_ref[pl.ds(k, 8), :, c] - top), axis=0)
                                for c in cols for k in range(0, n_kt, 8)])
        tot = jnp.sum(tot, axis=0, keepdims=True)
        g_ref[t, q, me] = top + LOG2E * jnp.log(tot)
        for r in ((5, 4, 1, 6, 7, 2, 3) if t == 0 else (6, 7, 2, 3, 5, 4, 1)):
            st_copy(t, q, r).start()

    def e_step(t, q, tb):
        e_quarter(q, tb)
        st_send_all(t, q, (q,))

    def combine(q, vals):
        top = functools.reduce(jnp.maximum, [jnp.max(v, axis=0) for v in vals])
        tot = functools.reduce(lambda u, v: u + v, [jnp.sum(jnp.exp2(v - top[None]), axis=0) for v in vals])
        lse = top + LOG2E * jnp.log(tot)
        lse_ref[:, blk(q, nq)] = lse
        return lse

    def scale(q, lse):
        cols = blk(q, nq)
        m_ref[:, :, cols] = jnp.exp2(m_ref[:, :, cols] - lse)

    def st_combine(t, q):
        for r in range(1, 8):
            st_copy(t, q, r).wait_recv()
        scale(q, combine(q, [g_ref[t, q]]))

    def st_combine_four(q, x, rs):
        for r in rs:
            st_copy(0, q, r).wait_recv()
        return combine(q, [g_ref[0, q, pl.ds(4 * c + 2 * x, 2)] for c in range(2)])

    def m_block(kb, quarters):
        rows = pl.ds(pl.multiple_of(kb * MB, MB), MB)
        n_acc = jnp.zeros((MB, 128), F32)
        acc = jnp.zeros((MB, dim), F32)
        for q in quarters:
            for ic in range(n_ch):
                cols = blk(q * n_ch + ic, IB)
                sc = m_ref[pl.ds(kb * (MB // KT), MB // KT), :, cols]
                r = (p_ref[rows, cols].reshape(MB // KT, KT // 8, 8, IB) * sc[:, None]).reshape(MB, IB)
                n_acc = n_acc + (r[:, :128] + r[:, 128:])
                acc = acc + jnp.dot(r.astype(BF16), x_ref[cols, :], preferred_element_type=F32)
        return n_acc, acc

    def m_first(kb, quarters):
        rows = blk(kb, MB)
        n_acc, acc = m_block(kb, quarters)
        n_ref[rows, :] = n_acc
        s_ref[rows, :] = acc
        return 0

    def flash(low, rows, c, tb, chunks, size):
        c2 = jnp.concatenate([c, c], axis=1)
        n_acc = jnp.zeros((size, 128), F32)
        acc = jnp.zeros((size, dim), F32)
        for ch in chunks:
            cols = blk(ch, IB)
            a = lax.dot_general(low[rows, :], xt_ref[:, cols], NN, preferred_element_type=F32)
            r = jnp.exp2((a * tb + c2) - lse_ref[:, cols])
            n_acc = n_acc + (r[:, :128] + r[:, 128:])
            acc = acc + jnp.dot(r.astype(BF16), x_ref[cols, :], preferred_element_type=F32)
        return n_acc, acc

    def finish(n_acc, acc):
        n = jnp.sum(n_acc, axis=1, keepdims=True)
        mu = acc * (1.0 / (n + EPS_COUNT))
        return n, mu

    def mu_copy(j):
        rows = pl.ds(pl.multiple_of(j * SB, SB), SB)
        return pltpu.make_async_remote_copy(
            src_ref=mub_ref.at[rows], dst_ref=muf_ref.at[rows], send_sem=mu_send.at[j], recv_sem=mu_recv.at[j],
            device_id=peer(2), device_id_type=MESH)

    def c_copy():
        return pltpu.make_async_remote_copy(
            src_ref=crow_ref, dst_ref=cfrow_ref, send_sem=mu_send.at[n_sb], recv_sem=mu_recv.at[n_sb],
            device_id=peer(2), device_id_type=MESH)

    def renew(rows, size, n_acc, acc, beta_next, share):
        n, mu = finish(n_ref[rows, :] + n_acc, s_ref[rows, :] + acc)
        mub_ref[rows, :] = mu.astype(BF16)
        msq = jnp.sum(mu * mu, axis=1, keepdims=True)
        lp = jnp.log((jnp.broadcast_to(n, (size, 128)) + ALPHA) / norm_const)
        c = LOG2E * (lp - beta_next * msq)
        c_ref[rows, :] = c
        if share:
            crow_ref[:, rows] = to_row(c)
        return 0

    def out_copy(slot, kb):
        size = (MB, FB)[slot]
        owner = data if slot == 0 else par
        rows = pl.ds(pl.multiple_of(owner * own + kb * size, size), size)
        return pltpu.make_async_remote_copy(
            src_ref=means_ref.at[rows], dst_ref=means_ref.at[rows], send_sem=out_send.at[slot, kb],
            recv_sem=out_recv.at[slot, kb], device_id=peer(1), device_id_type=MESH)

    def w_copy(slot):
        owner = data if slot == 0 else par
        return pltpu.make_async_remote_copy(
            src_ref=logw_ref.at[owner], dst_ref=logw_ref.at[owner], send_sem=w_send.at[slot], recv_sem=w_recv.at[slot],
            device_id=peer(1), device_id_type=MESH)

    def emit(slot, kb, n_acc, acc):
        size = (MB, FB)[slot]
        owner = data if slot == 0 else par
        n, mu = finish(n_acc, acc)
        means_ref[pl.ds(pl.multiple_of(owner * own + kb * size, size), size), :] = mu
        nrow = to_row(jnp.broadcast_to(n, (size, 128)))
        logw_ref[owner, :, pl.ds(pl.multiple_of(kb * size, size), size)] = jnp.log((nrow + ALPHA) / norm_const)
        out_copy(slot, kb).start()

    for t in range(sweeps):
        beta = temp_ref[t]
        tb = (2.0 * LOG2E) * beta
        last = t == sweeps - 1
        if t == 0:
            def own_points(s, _):
                q = data + s * (sib - data)
                pltpu.make_async_copy(pts_ref, x_ref.at[blk(q, nq)], q_sem.at[s]).wait()
                far = (q + 2) % 4
                e_quarter(q, tb, first=True)
                e_quarter(q, tb, muf_ref, n_ref, far, False)
                st_send_all(0, q, (q, far))
                return 0

            lax.fori_loop(0, 2, own_points, 0)
            pass_on(0)
            pass_on(1)
            near = (xpos * 2, xpos * 2 + 1)
            away = ((1 - xpos) * 2, (1 - xpos) * 2 + 1)
            for q in near:
                scale(q, st_combine_four(q, xpos, (1, 4, 5)))
            lax.fori_loop(0, n_mb, lambda kb, _: m_first(kb, near), 0)
            pass_on(2)
            pass_on(3)
            for q in away:
                st_combine_four(q, 1 - xpos, (2, 3, 6, 7))
            for ch in range(n_ch):
                pts_copy(1, ch).wait_recv()
            chunks = [q * n_ch + ic for q in away for ic in range(n_ch)]

            beta_next = temp_ref[1]

            def turn(ch, _):
                cols = blk((1 - xpos) * 2 * n_ch + ch, IB)
                xt_ref[:, cols] = jnp.transpose(x_ref[cols, :])
                return 0

            lax.fori_loop(0, 2 * n_ch, turn, 0)

            def away_block(kb, _):
                rows = blk(kb, FB)
                n_acc, acc = flash(mub_ref, rows, c_ref[rows, :], tb, chunks, FB)
                return renew(rows, FB, n_acc, acc, beta_next, False)

            lax.fori_loop(0, n_fb, away_block, 0)
            continue
        lax.fori_loop(0, 4, lambda s, _: (e_step(t, (s % 2) * 2 + s // 2, tb), 0)[1], 0)
        if last:
            for j in range(EARLY, n_sb):
                mu_copy(j).start()
        st_combine(t, 0)
        st_combine(t, 2)
        lax.fori_loop(0, n_mb, lambda kb, _: m_first(kb, (0, 2)), 0)
        st_combine(t, 1)
        st_combine(t, 3)
        if not last:
            beta_next = temp_ref[t + 1]
            share = t == sweeps - 2
            lax.fori_loop(0, n_mb, lambda kb, _: renew(blk(kb, MB), MB, *m_block(kb, (1, 3)), beta_next, share), 0)
            if share:
                c_copy().start()
                for j in range(EARLY):
                    mu_copy(j).start()
        else:
            def m_last(kb, _):
                rows = pl.ds(pl.multiple_of(kb * MB, MB), MB)
                n_acc, acc = m_block(kb, (1, 3))
                emit(0, kb, n_ref[rows, :] + n_acc, s_ref[rows, :] + acc)
                return 0

            lax.fori_loop(0, n_mb, m_last, 0)
            w_copy(0).start()
            c_copy().wait_recv()

            def far_block(kb, _):
                for j in range(FB // SB):
                    mu_copy(kb * (FB // SB) + j).wait_recv()
                rows = pl.ds(pl.multiple_of(kb * FB, FB), FB)
                n_acc, acc = flash(muf_ref, rows, to_col(cfrow_ref[:, rows]), tb, range(4 * n_ch), FB)
                emit(1, kb, n_acc, acc)
                return 0

            lax.fori_loop(0, n_fb, far_block, 0)
            w_copy(1).start()
            mine = pl.ds(pl.multiple_of(data * nq, nq), nq)
            xo = x_ref[mine, :].astype(F32)
            sq = xo * xo
            hi = sq.astype(BF16)
            lo = (sq - hi.astype(F32)).astype(BF16)
            ones = jnp.ones((8, dim), BF16)
            row_sq = (lax.dot_general(ones, hi, NT, preferred_element_type=F32)
                      + lax.dot_general(ones, lo, NT, preferred_element_type=F32))
            lse_out_ref[...] = LN2 * lse_ref[:, mine] - beta * row_sq[0:1, :]

    sib_copy().wait_send()
    for kind in range(2):
        for ch in range(n_ch):
            pts_copy(kind, ch).wait_send()
    for t in range(sweeps):
        for q in (near if t == 0 else range(4)):
            for r in range(1, 8):
                st_copy(t, q, r).wait_send()
    for j in range(n_sb):
        mu_copy(j).wait_send()
    c_copy().wait_send()
    for slot in range(2):
        w_copy(slot).wait_send()
        for kb in range((n_mb, n_fb)[slot]):
            out_copy(slot, kb).wait_send()

    def sibling(dev_slot):
        owner = (sib, data_xor(3))[dev_slot]
        size = (MB, FB)[dev_slot]
        for kb in range((n_mb, n_fb)[dev_slot]):
            rows = pl.ds(pl.multiple_of(owner * own + kb * size, size), size)
            pltpu.make_async_remote_copy(
                src_ref=means_ref.at[rows], dst_ref=means_ref.at[rows], send_sem=out_send.at[dev_slot, kb],
                recv_sem=out_recv.at[dev_slot, kb], device_id=peer(1), device_id_type=MESH).wait_recv()
        pltpu.make_async_remote_copy(
            src_ref=logw_ref.at[owner], dst_ref=logw_ref.at[owner], send_sem=w_send.at[dev_slot],
            recv_sem=w_recv.at[dev_slot], device_id=peer(1), device_id_type=MESH).wait_recv()

    sibling(0)
    sibling(1)


def flush_kernel(means_ref, logw_ref, lse_ref, means_out, logw_out, lse_out, sem):
    rows = means_ref.shape[0] // PIECES
    copies = [pltpu.make_async_copy(means_ref.at[pl.ds(i * rows, rows)], means_out.at[pl.ds(i * rows, rows)], sem.at[i])
              for i in range(PIECES)]
    copies.append(pltpu.make_async_copy(logw_ref, logw_out, sem.at[PIECES]))
    copies.append(pltpu.make_async_copy(lse_ref, lse_out, sem.at[PIECES + 1]))
    for cp in copies:
        cp.start()
    for cp in copies:
        cp.wait()


def solution(mesh):
    comp_size = mesh.shape["comp"]
    data_size = mesh.shape["data"]

    def local_fit(points, mu_init, logpi_init, inv_temp):
        nq, dim = points.shape
        rows = mu_init.shape[0]
        own = rows // data_size
        sweeps = inv_temp.shape[0]
        n_pts = nq * data_size
        n_kb = own // KB
        norm_const = n_pts + rows * comp_size * ALPHA
        cfg = (sweeps, own, nq, dim, norm_const)
        any_spec = pl.BlockSpec(memory_space=pl.ANY)
        vmem_spec = pl.BlockSpec(memory_space=pltpu.VMEM)
        dma = pltpu.SemaphoreType.DMA
        n_fb, n_sb = own // FB, own // SB
        means, logw, lse = pl.pallas_call(
            functools.partial(fit_kernel, cfg),
            out_shape=(pltpu.VMEM((rows, dim), F32),
                       pltpu.VMEM((data_size, 1, own), F32),
                       pltpu.VMEM((1, nq), F32)),
            in_specs=[pl.BlockSpec(memory_space=pltpu.SMEM), any_spec, any_spec, any_spec],
            out_specs=(vmem_spec, vmem_spec, vmem_spec),
            scratch_shapes=[
                pltpu.VMEM((n_pts, dim), BF16),
                pltpu.VMEM((dim, n_pts), BF16),
                pltpu.VMEM((own, n_pts), F32),
                pltpu.VMEM((own, dim), BF16),
                pltpu.VMEM((own, dim), BF16),
                pltpu.VMEM((own, 128), F32),
                pltpu.VMEM((1, own), F32),
                pltpu.VMEM((1, own), F32),
                pltpu.VMEM((own, dim), F32),
                pltpu.VMEM((own, 128), F32),
                pltpu.VMEM((own // KT, 8, n_pts), F32),
                pltpu.VMEM((own // KT, 8, n_pts), F32),
                pltpu.VMEM((1, n_pts), F32),
                pltpu.VMEM((sweeps, data_size, 8, 1, nq), F32),
                dma((4,)), dma((2,)), dma,
                dma((2, nq // IB)), dma((2, nq // IB)),
                dma((sweeps, 4, 8)), dma((sweeps, 4, 8)),
                dma((n_sb + 1,)), dma((n_sb + 1,)),
                dma((2, n_fb)), dma((2, n_fb)),
                dma((2,)), dma((2,)),
            ],
            compiler_params=pltpu.CompilerParams(
                collective_id=0, has_side_effects=True, vmem_limit_bytes=54 * 1024 * 1024),
        )(inv_temp, points, mu_init, logpi_init.reshape(data_size, 1, own))
        results = [pltpu.with_memory_space_constraint(v, pltpu.VMEM) for v in (means, logw, lse)]
        means, logw, lse = pl.pallas_call(
            flush_kernel,
            out_shape=tuple(jax.ShapeDtypeStruct(v.shape, F32) for v in results),
            in_specs=[vmem_spec] * 3,
            out_specs=(any_spec,) * 3,
            scratch_shapes=[dma((PIECES + 2,))],
            compiler_params=pltpu.CompilerParams(vmem_limit_bytes=16 * 1024 * 1024),
        )(*results)
        return means, logw.reshape(rows), lse.reshape(nq)

    row_spec = P(("fit", "data"), None)
    comp_spec = P(("fit", "comp"), None)
    weight_spec = P(("fit", "comp"))
    lse_spec = P(("fit", "data"))
    return jax.shard_map(local_fit, mesh=mesh, in_specs=(row_spec, comp_spec, weight_spec, P(None)), out_specs=(comp_spec, weight_spec, lse_spec), check_vma=False)
```

```python
import functools
import math

import jax
import jax.numpy as jnp
from jax import lax
from jax.experimental import pallas as pl
from jax.experimental.pallas import tpu as pltpu
from jax.sharding import PartitionSpec as P

EPS_COUNT = 1e-6
ALPHA = 1e-3
PIECES = 8
LOG2E = math.log2(math.e)
LN2 = math.log(2.0)
KB = 1024
IB = 256
KT = 512
MB = 1024
EARLY = 3
SB = 256
FB = 512
MESH = pl.DeviceIdType.MESH
F32 = jnp.float32
BF16 = jnp.bfloat16
NT = (((1,), (1,)), ((), ()))


def fit_kernel(cfg, temp_ref, pts_ref, mu_ref, logpi_ref, means_ref, logw_ref, lse_out_ref,
               x_ref, p_ref, mub_ref, muf_ref, c_ref, crow_ref, cfrow_ref, s_ref, n_ref,
               m_ref, sum_ref, lse_ref, g_ref,
               loc_sem, pts_send, pts_recv, st_send, st_recv, mu_send, mu_recv,
               out_send, out_recv, w_send, w_recv):
    sweeps, own, nq, dim, norm_const = cfg
    n_kb = own // KB
    n_kt = own // KT
    n_mb = own // MB
    n_fb = own // FB
    n_sb = own // SB
    n_ch = nq // IB
    fit = lax.axis_index("fit")
    comp = lax.axis_index("comp")
    data = lax.axis_index("data")
    xpos = data // 2

    def data_xor(d):
        if d == 0:
            return data
        if d == 1:
            return data + 1 - 2 * (data % 2)
        if d == 2:
            return (data + 2) % 4
        return (data + 1 - 2 * (data % 2) + 2) % 4

    def peer(r):
        return (fit, (comp + r // 4) % 2, data_xor(r % 4))

    sib, par = data_xor(1), data_xor(2)
    me = comp * 4 + data

    barrier = pltpu.get_barrier_semaphore()
    for r in range(1, 8):
        pl.semaphore_signal(barrier, inc=1, device_id=peer(r), device_id_type=MESH)

    ld_pts = pltpu.make_async_copy(pts_ref, x_ref.at[pl.ds(pl.multiple_of(data * nq, nq), nq)], loc_sem.at[0])
    ld_mu = pltpu.make_async_copy(mu_ref.at[pl.ds(pl.multiple_of(data * own, own), own)], s_ref, loc_sem.at[1])
    ld_pi = pltpu.make_async_copy(logpi_ref.at[data], crow_ref, loc_sem.at[2])
    ld_pts.start()
    ld_mu.start()
    ld_pi.start()
    pl.semaphore_wait(barrier, 7)

    def pts_copy(kind, ch):
        owner = data if kind < 2 else par
        rows = pl.ds(pl.multiple_of(owner * nq + ch * IB, IB), IB)
        src = pts_ref.at[pl.ds(ch * IB, IB)] if kind < 2 else x_ref.at[rows]
        dev = peer(2) if kind == 1 else peer(1)
        return pltpu.make_async_remote_copy(
            src_ref=src, dst_ref=x_ref.at[rows], send_sem=pts_send.at[kind, ch], recv_sem=pts_recv.at[kind, ch],
            device_id=dev, device_id_type=MESH)

    for ch in range(n_ch):
        pts_copy(1, ch).start()
    for ch in range(n_ch):
        pts_copy(0, ch).start()

    def to_col(row):
        return jnp.transpose(jnp.broadcast_to(row, (128, row.shape[1])))

    def to_row(col):
        return jnp.transpose(col)[0:1, :]

    ld_pi.wait()
    ld_mu.wait()
    beta0 = temp_ref[0]

    def init_body(kb, _):
        rows = pl.ds(pl.multiple_of(kb * KB, KB), KB)
        mu = s_ref[rows, :]
        mub_ref[rows, :] = mu.astype(BF16)
        msq = jnp.sum(mu * mu, axis=1, keepdims=True)
        lp = to_col(crow_ref[:, rows])
        c_ref[rows, :] = LOG2E * (lp - beta0 * msq)
        return 0

    lax.fori_loop(0, n_kb, init_body, 0)

    def e_tiles(starts, tb):
        def logits(i0, kb):
            xt = x_ref[pl.ds(pl.multiple_of(i0, IB), IB), :]
            a = lax.dot_general(mub_ref[pl.ds(kb * KB, KB), :], xt, NT, preferred_element_type=F32)
            for u in range(KB // KT):
                cc = c_ref[pl.ds(kb * KB + u * KT, KT), :]
                l = a[u * KT:(u + 1) * KT, :] * tb + jnp.concatenate([cc, cc], axis=1)
                yield kb * (KB // KT) + u, pl.ds(kb * KB + u * KT, KT), l.reshape(KT // 8, 8, IB)

        def maxima(i0, kb):
            cols = pl.ds(pl.multiple_of(i0, IB), IB)
            for tile, _, l3 in logits(i0, kb):
                m_ref[tile, :, cols] = jnp.max(l3, axis=0)

        def exponentials(i0, kb):
            cols = pl.ds(pl.multiple_of(i0, IB), IB)
            for tile, rows, l3 in logits(i0, kb):
                p3 = jnp.exp2(l3 - m_ref[tile, :, cols][None])
                p_ref[rows, cols] = p3.reshape(KT, IB)
                sum_ref[tile, :, cols] = jnp.sum(p3, axis=0)

        steps = [(i0, kb) for i0 in starts for kb in range(n_kb)]
        maxima(*steps[0])
        for i, step in enumerate(steps):
            if i + 1 < len(steps):
                maxima(*steps[i + 1])
            exponentials(*step)

    def e_quarter(q, tb):
        e_tiles([q * nq + it * IB for it in range(n_ch)], tb)

    def st_copy(t, q, r):
        return pltpu.make_async_remote_copy(
            src_ref=g_ref.at[t, q, me], dst_ref=g_ref.at[t, q, me], send_sem=st_send.at[t, q, r],
            recv_sem=st_recv.at[t, q, r], device_id=peer(r), device_id_type=MESH)

    def st_send_all(t, q):
        cols = pl.ds(pl.multiple_of(q * nq, nq), nq)
        top = jnp.max(jnp.max(m_ref[:, :, cols], axis=0), axis=0, keepdims=True)
        tot = jnp.sum(sum_ref[:, :, cols] * jnp.exp2(m_ref[:, :, cols] - top), axis=0)
        tot = jnp.sum(tot, axis=0, keepdims=True)
        g_ref[t, q, me] = top + LOG2E * jnp.log(tot)
        for r in range(1, 8):
            st_copy(t, q, r).start()

    def e_step(t, q, tb):
        e_quarter(q, tb)
        st_send_all(t, q)

    def st_combine(t, q):
        for r in range(1, 8):
            st_copy(t, q, r).wait_recv()
        cols = pl.ds(pl.multiple_of(q * nq, nq), nq)
        vals = g_ref[t, q]
        top = jnp.max(vals, axis=0)
        tot = jnp.sum(jnp.exp2(vals - top[None]), axis=0)
        lse = top + LOG2E * jnp.log(tot)
        lse_ref[:, cols] = lse
        m_ref[:, :, cols] = jnp.exp2(m_ref[:, :, cols] - lse)

    def m_block(kb, quarters):
        rows = pl.ds(pl.multiple_of(kb * MB, MB), MB)
        n_acc = jnp.zeros((MB, 128), F32)
        acc = jnp.zeros((MB, dim), F32)
        for q in quarters:
            for ic in range(n_ch):
                cols = pl.ds(q * nq + ic * IB, IB)
                sc = m_ref[pl.ds(kb * (MB // KT), MB // KT), :, cols]
                r = (p_ref[rows, cols].reshape(MB // KT, KT // 8, 8, IB) * sc[:, None]).reshape(MB, IB)
                n_acc = n_acc + (r[:, :128] + r[:, 128:])
                acc = acc + jnp.dot(r.astype(BF16), x_ref[cols, :], preferred_element_type=F32)
        return n_acc, acc

    def m_first(kb, _):
        rows = pl.ds(pl.multiple_of(kb * MB, MB), MB)
        n_acc, acc = m_block(kb, (0, 2))
        n_ref[rows, :] = n_acc
        s_ref[rows, :] = acc
        return 0

    def finish(n_acc, acc):
        n = jnp.sum(n_acc, axis=1, keepdims=True)
        mu = acc * (1.0 / (n + EPS_COUNT))
        return n, mu

    def mu_copy(j):
        rows = pl.ds(pl.multiple_of(j * SB, SB), SB)
        return pltpu.make_async_remote_copy(
            src_ref=mub_ref.at[rows], dst_ref=muf_ref.at[rows], send_sem=mu_send.at[j], recv_sem=mu_recv.at[j],
            device_id=peer(2), device_id_type=MESH)

    def c_copy():
        return pltpu.make_async_remote_copy(
            src_ref=crow_ref, dst_ref=cfrow_ref, send_sem=mu_send.at[n_sb], recv_sem=mu_recv.at[n_sb],
            device_id=peer(2), device_id_type=MESH)

    def m_second(kb, beta_next, share):
        rows = pl.ds(pl.multiple_of(kb * MB, MB), MB)
        n_acc, acc = m_block(kb, (1, 3))
        n, mu = finish(n_ref[rows, :] + n_acc, s_ref[rows, :] + acc)
        mub_ref[rows, :] = mu.astype(BF16)
        msq = jnp.sum(mu * mu, axis=1, keepdims=True)
        lp = jnp.log((jnp.broadcast_to(n, (MB, 128)) + ALPHA) / norm_const)
        c = LOG2E * (lp - beta_next * msq)
        c_ref[rows, :] = c
        if share:
            crow_ref[:, rows] = to_row(c)

    def out_copy(slot, kb):
        size = (MB, FB)[slot]
        owner = data if slot == 0 else par
        rows = pl.ds(pl.multiple_of(owner * own + kb * size, size), size)
        return pltpu.make_async_remote_copy(
            src_ref=means_ref.at[rows], dst_ref=means_ref.at[rows], send_sem=out_send.at[slot, kb],
            recv_sem=out_recv.at[slot, kb], device_id=peer(1), device_id_type=MESH)

    def w_copy(slot):
        owner = data if slot == 0 else par
        return pltpu.make_async_remote_copy(
            src_ref=logw_ref.at[owner], dst_ref=logw_ref.at[owner], send_sem=w_send.at[slot], recv_sem=w_recv.at[slot],
            device_id=peer(1), device_id_type=MESH)

    def emit(slot, kb, n_acc, acc):
        size = (MB, FB)[slot]
        owner = data if slot == 0 else par
        n, mu = finish(n_acc, acc)
        means_ref[pl.ds(pl.multiple_of(owner * own + kb * size, size), size), :] = mu
        nrow = to_row(jnp.broadcast_to(n, (size, 128)))
        logw_ref[owner, :, pl.ds(pl.multiple_of(kb * size, size), size)] = jnp.log((nrow + ALPHA) / norm_const)
        out_copy(slot, kb).start()

    for t in range(sweeps):
        beta = temp_ref[t]
        tb = (2.0 * LOG2E) * beta
        last = t == sweeps - 1
        if t == 0:
            ld_pts.wait()
            for ch in range(n_ch):
                pts_copy(0, ch).wait_recv()
            lax.fori_loop(0, 2, lambda s, _: (e_step(0, xpos * 2 + s, tb), 0)[1], 0)

            def far_points(ch, _):
                pts_copy(1, ch).wait_recv()
                pts_copy(2, ch).start()
                e_tiles([par * nq + ch * IB], tb)
                pts_copy(2, ch).wait_recv()
                e_tiles([data_xor(3) * nq + ch * IB], tb)
                return 0

            lax.fori_loop(0, n_ch, far_points, 0)
            st_send_all(0, par)
            st_send_all(0, data_xor(3))
        else:
            lax.fori_loop(0, 4, lambda s, _: (e_step(t, (s % 2) * 2 + s // 2, tb), 0)[1], 0)
            if last:
                for j in range(EARLY, n_sb):
                    mu_copy(j).start()
        st_combine(t, 0)
        st_combine(t, 2)
        lax.fori_loop(0, n_mb, m_first, 0)
        st_combine(t, 1)
        st_combine(t, 3)
        if not last:
            beta_next = temp_ref[t + 1]
            share = t == sweeps - 2
            lax.fori_loop(0, n_mb, lambda kb, _: (m_second(kb, beta_next, share), 0)[1], 0)
            if share:
                c_copy().start()
                for j in range(EARLY):
                    mu_copy(j).start()
        else:
            def m_last(kb, _):
                rows = pl.ds(pl.multiple_of(kb * MB, MB), MB)
                n_acc, acc = m_block(kb, (1, 3))
                emit(0, kb, n_ref[rows, :] + n_acc, s_ref[rows, :] + acc)
                return 0

            lax.fori_loop(0, n_mb, m_last, 0)
            w_copy(0).start()
            c_copy().wait_recv()

            def far_block(kb, _):
                for j in range(FB // SB):
                    mu_copy(kb * (FB // SB) + j).wait_recv()
                rows = pl.ds(pl.multiple_of(kb * FB, FB), FB)
                c = to_col(cfrow_ref[:, rows])
                c2 = jnp.concatenate([c, c], axis=1)
                n_acc = jnp.zeros((FB, 128), F32)
                acc = jnp.zeros((FB, dim), F32)
                for ic in range(4 * n_ch):
                    cols = pl.ds(ic * IB, IB)
                    xt = x_ref[cols, :]
                    a = lax.dot_general(muf_ref[rows, :], xt, NT, preferred_element_type=F32)
                    r = jnp.exp2((a * tb + c2) - lse_ref[:, cols])
                    n_acc = n_acc + (r[:, :128] + r[:, 128:])
                    acc = acc + jnp.dot(r.astype(BF16), xt, preferred_element_type=F32)
                emit(1, kb, n_acc, acc)
                return 0

            lax.fori_loop(0, n_fb, far_block, 0)
            w_copy(1).start()
            mine = pl.ds(pl.multiple_of(data * nq, nq), nq)
            xo = x_ref[mine, :].astype(F32)
            sq = xo * xo
            hi = sq.astype(BF16)
            lo = (sq - hi.astype(F32)).astype(BF16)
            ones = jnp.ones((8, dim), BF16)
            row_sq = (lax.dot_general(ones, hi, NT, preferred_element_type=F32)
                      + lax.dot_general(ones, lo, NT, preferred_element_type=F32))
            lse_out_ref[...] = LN2 * lse_ref[:, mine] - beta * row_sq[0:1, :]

    for kind in range(3):
        for ch in range(n_ch):
            pts_copy(kind, ch).wait_send()
    for t in range(sweeps):
        for q in range(4):
            for r in range(1, 8):
                st_copy(t, q, r).wait_send()
    for j in range(n_sb):
        mu_copy(j).wait_send()
    c_copy().wait_send()
    for slot in range(2):
        w_copy(slot).wait_send()
        for kb in range((n_mb, n_fb)[slot]):
            out_copy(slot, kb).wait_send()

    def sibling(dev_slot):
        owner = (sib, data_xor(3))[dev_slot]
        size = (MB, FB)[dev_slot]
        for kb in range((n_mb, n_fb)[dev_slot]):
            rows = pl.ds(pl.multiple_of(owner * own + kb * size, size), size)
            pltpu.make_async_remote_copy(
                src_ref=means_ref.at[rows], dst_ref=means_ref.at[rows], send_sem=out_send.at[dev_slot, kb],
                recv_sem=out_recv.at[dev_slot, kb], device_id=peer(1), device_id_type=MESH).wait_recv()
        pltpu.make_async_remote_copy(
            src_ref=logw_ref.at[owner], dst_ref=logw_ref.at[owner], send_sem=w_send.at[dev_slot],
            recv_sem=w_recv.at[dev_slot], device_id=peer(1), device_id_type=MESH).wait_recv()

    sibling(0)
    sibling(1)


def flush_kernel(means_ref, logw_ref, lse_ref, means_out, logw_out, lse_out, sem):
    rows = means_ref.shape[0] // PIECES
    copies = [pltpu.make_async_copy(means_ref.at[pl.ds(i * rows, rows)], means_out.at[pl.ds(i * rows, rows)], sem.at[i])
              for i in range(PIECES)]
    copies.append(pltpu.make_async_copy(logw_ref, logw_out, sem.at[PIECES]))
    copies.append(pltpu.make_async_copy(lse_ref, lse_out, sem.at[PIECES + 1]))
    for cp in copies:
        cp.start()
    for cp in copies:
        cp.wait()


def solution(mesh):
    comp_size = mesh.shape["comp"]
    data_size = mesh.shape["data"]

    def local_fit(points, mu_init, logpi_init, inv_temp):
        nq, dim = points.shape
        rows = mu_init.shape[0]
        own = rows // data_size
        sweeps = inv_temp.shape[0]
        n_pts = nq * data_size
        n_kb = own // KB
        norm_const = n_pts + rows * comp_size * ALPHA
        cfg = (sweeps, own, nq, dim, norm_const)
        any_spec = pl.BlockSpec(memory_space=pl.ANY)
        vmem_spec = pl.BlockSpec(memory_space=pltpu.VMEM)
        dma = pltpu.SemaphoreType.DMA
        n_fb, n_sb = own // FB, own // SB
        means, logw, lse = pl.pallas_call(
            functools.partial(fit_kernel, cfg),
            out_shape=(pltpu.VMEM((rows, dim), F32),
                       pltpu.VMEM((data_size, 1, own), F32),
                       pltpu.VMEM((1, nq), F32)),
            in_specs=[pl.BlockSpec(memory_space=pltpu.SMEM), any_spec, any_spec, any_spec],
            out_specs=(vmem_spec, vmem_spec, vmem_spec),
            scratch_shapes=[
                pltpu.VMEM((n_pts, dim), BF16),
                pltpu.VMEM((own, n_pts), F32),
                pltpu.VMEM((own, dim), BF16),
                pltpu.VMEM((own, dim), BF16),
                pltpu.VMEM((own, 128), F32),
                pltpu.VMEM((1, own), F32),
                pltpu.VMEM((1, own), F32),
                pltpu.VMEM((own, dim), F32),
                pltpu.VMEM((own, 128), F32),
                pltpu.VMEM((own // KT, 8, n_pts), F32),
                pltpu.VMEM((own // KT, 8, n_pts), F32),
                pltpu.VMEM((1, n_pts), F32),
                pltpu.VMEM((sweeps, data_size, 8, 1, nq), F32),
                dma((3,)),
                dma((3, nq // IB)), dma((3, nq // IB)),
                dma((sweeps, 4, 8)), dma((sweeps, 4, 8)),
                dma((n_sb + 1,)), dma((n_sb + 1,)),
                dma((2, n_fb)), dma((2, n_fb)),
                dma((2,)), dma((2,)),
            ],
            compiler_params=pltpu.CompilerParams(
                collective_id=0, has_side_effects=True, vmem_limit_bytes=54 * 1024 * 1024),
        )(inv_temp, points, mu_init, logpi_init.reshape(data_size, 1, own))
        results = [pltpu.with_memory_space_constraint(v, pltpu.VMEM) for v in (means, logw, lse)]
        means, logw, lse = pl.pallas_call(
            flush_kernel,
            out_shape=tuple(jax.ShapeDtypeStruct(v.shape, F32) for v in results),
            in_specs=[vmem_spec] * 3,
            out_specs=(any_spec,) * 3,
            scratch_shapes=[dma((PIECES + 2,))],
            compiler_params=pltpu.CompilerParams(vmem_limit_bytes=16 * 1024 * 1024),
        )(*results)
        return means, logw.reshape(rows), lse.reshape(nq)

    row_spec = P(("fit", "data"), None)
    comp_spec = P(("fit", "comp"), None)
    weight_spec = P(("fit", "comp"))
    lse_spec = P(("fit", "data"))
    return jax.shard_map(local_fit, mesh=mesh, in_specs=(row_spec, comp_spec, weight_spec, P(None)), out_specs=(comp_spec, weight_spec, lse_spec), check_vma=False)
```

```python
import functools
import math

import jax
import jax.numpy as jnp
from jax import lax
from jax.experimental import pallas as pl
from jax.experimental.pallas import tpu as pltpu
from jax.sharding import PartitionSpec as P

EPS_COUNT = 1e-6
ALPHA = 1e-3
PIECES = 8
LOG2E = math.log2(math.e)
LN2 = math.log(2.0)
KB = 1024
IB = 256
KT = 512
MB = 1024
EARLY = 3
SB = 256
FB = 512
MESH = pl.DeviceIdType.MESH
F32 = jnp.float32
BF16 = jnp.bfloat16
NT = (((1,), (1,)), ((), ()))


def fit_kernel(cfg, temp_ref, pts_ref, mu_ref, logpi_ref, means_ref, logw_ref, lse_out_ref,
               x_ref, p_ref, mub_ref, muf_ref, c_ref, crow_ref, cfrow_ref, s_ref, n_ref,
               m_ref, sum_ref, lse_ref, g_ref,
               loc_sem, pts_send, pts_recv, st_send, st_recv, mu_send, mu_recv,
               out_send, out_recv, w_send, w_recv):
    sweeps, own, nq, dim, norm_const = cfg
    n_kb = own // KB
    n_kt = own // KT
    n_mb = own // MB
    n_fb = own // FB
    n_sb = own // SB
    n_ch = nq // IB
    fit = lax.axis_index("fit")
    comp = lax.axis_index("comp")
    data = lax.axis_index("data")
    xpos = data // 2

    def data_xor(d):
        if d == 0:
            return data
        if d == 1:
            return data + 1 - 2 * (data % 2)
        if d == 2:
            return (data + 2) % 4
        return (data + 1 - 2 * (data % 2) + 2) % 4

    def peer(r):
        return (fit, (comp + r // 4) % 2, data_xor(r % 4))

    sib, par = data_xor(1), data_xor(2)
    me = comp * 4 + data

    barrier = pltpu.get_barrier_semaphore()
    for r in range(1, 8):
        pl.semaphore_signal(barrier, inc=1, device_id=peer(r), device_id_type=MESH)

    ld_pts = pltpu.make_async_copy(pts_ref, x_ref.at[pl.ds(pl.multiple_of(data * nq, nq), nq)], loc_sem.at[0])
    ld_mu = pltpu.make_async_copy(mu_ref.at[pl.ds(pl.multiple_of(data * own, own), own)], s_ref, loc_sem.at[1])
    ld_pi = pltpu.make_async_copy(logpi_ref.at[data], crow_ref, loc_sem.at[2])
    ld_pts.start()
    ld_mu.start()
    ld_pi.start()
    pl.semaphore_wait(barrier, 7)

    def pts_copy(kind, ch):
        owner = data if kind < 2 else par
        rows = pl.ds(pl.multiple_of(owner * nq + ch * IB, IB), IB)
        src = pts_ref.at[pl.ds(ch * IB, IB)] if kind < 2 else x_ref.at[rows]
        dev = peer(2) if kind == 1 else peer(1)
        return pltpu.make_async_remote_copy(
            src_ref=src, dst_ref=x_ref.at[rows], send_sem=pts_send.at[kind, ch], recv_sem=pts_recv.at[kind, ch],
            device_id=dev, device_id_type=MESH)

    for ch in range(n_ch):
        pts_copy(1, ch).start()
    for ch in range(n_ch):
        pts_copy(0, ch).start()

    def to_col(row):
        return jnp.transpose(jnp.broadcast_to(row, (128, row.shape[1])))

    def to_row(col):
        return jnp.transpose(col)[0:1, :]

    ld_pi.wait()
    ld_mu.wait()
    beta0 = temp_ref[0]

    def init_body(kb, _):
        rows = pl.ds(pl.multiple_of(kb * KB, KB), KB)
        mu = s_ref[rows, :]
        mub_ref[rows, :] = mu.astype(BF16)
        msq = jnp.sum(mu * mu, axis=1, keepdims=True)
        lp = to_col(crow_ref[:, rows])
        c_ref[rows, :] = LOG2E * (lp - beta0 * msq)
        return 0

    lax.fori_loop(0, n_kb, init_body, 0)

    def e_tiles(starts, tb):
        def logits(i0, kb):
            xt = x_ref[pl.ds(pl.multiple_of(i0, IB), IB), :]
            a = lax.dot_general(mub_ref[pl.ds(kb * KB, KB), :], xt, NT, preferred_element_type=F32)
            for u in range(KB // KT):
                cc = c_ref[pl.ds(kb * KB + u * KT, KT), :]
                l = a[u * KT:(u + 1) * KT, :] * tb + jnp.concatenate([cc, cc], axis=1)
                yield kb * (KB // KT) + u, pl.ds(kb * KB + u * KT, KT), l.reshape(KT // 8, 8, IB)

        def maxima(i0, kb):
            cols = pl.ds(pl.multiple_of(i0, IB), IB)
            for tile, _, l3 in logits(i0, kb):
                m_ref[tile, :, cols] = jnp.max(l3, axis=0)

        def exponentials(i0, kb):
            cols = pl.ds(pl.multiple_of(i0, IB), IB)
            for tile, rows, l3 in logits(i0, kb):
                p3 = jnp.exp2(l3 - m_ref[tile, :, cols][None])
                p_ref[rows, cols] = p3.reshape(KT, IB)
                sum_ref[tile, :, cols] = jnp.sum(p3, axis=0)

        steps = [(i0, kb) for i0 in starts for kb in range(n_kb)]
        maxima(*steps[0])
        for i, step in enumerate(steps):
            if i + 1 < len(steps):
                maxima(*steps[i + 1])
            exponentials(*step)

    def e_quarter(q, tb):
        e_tiles([q * nq + it * IB for it in range(n_ch)], tb)

    def st_copy(t, q, r):
        return pltpu.make_async_remote_copy(
            src_ref=g_ref.at[t, q, me], dst_ref=g_ref.at[t, q, me], send_sem=st_send.at[t, q, r],
            recv_sem=st_recv.at[t, q, r], device_id=peer(r), device_id_type=MESH)

    def st_send_all(t, q):
        cols = pl.ds(pl.multiple_of(q * nq, nq), nq)
        top = jnp.max(jnp.max(m_ref[:, :, cols], axis=0), axis=0, keepdims=True)
        tot = jnp.sum(sum_ref[:, :, cols] * jnp.exp2(m_ref[:, :, cols] - top), axis=0)
        tot = jnp.sum(tot, axis=0, keepdims=True)
        g_ref[t, q, me] = top + LOG2E * jnp.log(tot)
        for r in range(1, 8):
            st_copy(t, q, r).start()

    def e_step(t, q, tb):
        e_quarter(q, tb)
        st_send_all(t, q)

    def st_combine(t, q):
        for r in range(1, 8):
            st_copy(t, q, r).wait_recv()
        cols = pl.ds(pl.multiple_of(q * nq, nq), nq)
        vals = g_ref[t, q]
        top = jnp.max(vals, axis=0)
        tot = jnp.sum(jnp.exp2(vals - top[None]), axis=0)
        lse = top + LOG2E * jnp.log(tot)
        lse_ref[:, cols] = lse
        m_ref[:, :, cols] = jnp.exp2(m_ref[:, :, cols] - lse)

    def m_block(kb, quarters):
        rows = pl.ds(pl.multiple_of(kb * MB, MB), MB)
        n_acc = jnp.zeros((MB, 128), F32)
        acc = jnp.zeros((MB, dim), F32)
        for q in quarters:
            for ic in range(n_ch):
                cols = pl.ds(q * nq + ic * IB, IB)
                sc = m_ref[pl.ds(kb * (MB // KT), MB // KT), :, cols]
                r = (p_ref[rows, cols].reshape(MB // KT, KT // 8, 8, IB) * sc[:, None]).reshape(MB, IB)
                n_acc = n_acc + (r[:, :128] + r[:, 128:])
                acc = acc + jnp.dot(r.astype(BF16), x_ref[cols, :], preferred_element_type=F32)
        return n_acc, acc

    def m_first(kb, _):
        rows = pl.ds(pl.multiple_of(kb * MB, MB), MB)
        n_acc, acc = m_block(kb, (0, 2))
        n_ref[rows, :] = n_acc
        s_ref[rows, :] = acc
        return 0

    def finish(n_acc, acc):
        n = jnp.sum(n_acc, axis=1, keepdims=True)
        mu = acc * (1.0 / (n + EPS_COUNT))
        return n, mu

    def mu_copy(j):
        rows = pl.ds(pl.multiple_of(j * SB, SB), SB)
        return pltpu.make_async_remote_copy(
            src_ref=mub_ref.at[rows], dst_ref=muf_ref.at[rows], send_sem=mu_send.at[j], recv_sem=mu_recv.at[j],
            device_id=peer(2), device_id_type=MESH)

    def c_copy():
        return pltpu.make_async_remote_copy(
            src_ref=crow_ref, dst_ref=cfrow_ref, send_sem=mu_send.at[n_sb], recv_sem=mu_recv.at[n_sb],
            device_id=peer(2), device_id_type=MESH)

    def m_second(kb, beta_next, share):
        rows = pl.ds(pl.multiple_of(kb * MB, MB), MB)
        n_acc, acc = m_block(kb, (1, 3))
        n, mu = finish(n_ref[rows, :] + n_acc, s_ref[rows, :] + acc)
        mub_ref[rows, :] = mu.astype(BF16)
        msq = jnp.sum(mu * mu, axis=1, keepdims=True)
        lp = jnp.log((jnp.broadcast_to(n, (MB, 128)) + ALPHA) / norm_const)
        c = LOG2E * (lp - beta_next * msq)
        c_ref[rows, :] = c
        if share:
            crow_ref[:, rows] = to_row(c)

    def out_copy(slot, kb):
        size = (MB, FB)[slot]
        owner = data if slot == 0 else par
        rows = pl.ds(pl.multiple_of(owner * own + kb * size, size), size)
        return pltpu.make_async_remote_copy(
            src_ref=means_ref.at[rows], dst_ref=means_ref.at[rows], send_sem=out_send.at[slot, kb],
            recv_sem=out_recv.at[slot, kb], device_id=peer(1), device_id_type=MESH)

    def w_copy(slot):
        owner = data if slot == 0 else par
        return pltpu.make_async_remote_copy(
            src_ref=logw_ref.at[owner], dst_ref=logw_ref.at[owner], send_sem=w_send.at[slot], recv_sem=w_recv.at[slot],
            device_id=peer(1), device_id_type=MESH)

    def emit(slot, kb, n_acc, acc):
        size = (MB, FB)[slot]
        owner = data if slot == 0 else par
        n, mu = finish(n_acc, acc)
        means_ref[pl.ds(pl.multiple_of(owner * own + kb * size, size), size), :] = mu
        nrow = to_row(jnp.broadcast_to(n, (size, 128)))
        logw_ref[owner, :, pl.ds(pl.multiple_of(kb * size, size), size)] = jnp.log((nrow + ALPHA) / norm_const)
        out_copy(slot, kb).start()

    for t in range(sweeps):
        beta = temp_ref[t]
        tb = (2.0 * LOG2E) * beta
        last = t == sweeps - 1
        if t == 0:
            ld_pts.wait()
            for ch in range(n_ch):
                pts_copy(0, ch).wait_recv()
            lax.fori_loop(0, 2, lambda s, _: (e_step(0, xpos * 2 + s, tb), 0)[1], 0)

            def far_points(ch, _):
                pts_copy(1, ch).wait_recv()
                pts_copy(2, ch).start()
                e_tiles([par * nq + ch * IB], tb)
                pts_copy(2, ch).wait_recv()
                e_tiles([data_xor(3) * nq + ch * IB], tb)
                return 0

            lax.fori_loop(0, n_ch, far_points, 0)
            st_send_all(0, par)
            st_send_all(0, data_xor(3))
        else:
            lax.fori_loop(0, 4, lambda s, _: (e_step(t, (s % 2) * 2 + s // 2, tb), 0)[1], 0)
            if last:
                for j in range(EARLY, n_sb):
                    mu_copy(j).start()
        st_combine(t, 0)
        st_combine(t, 2)
        lax.fori_loop(0, n_mb, m_first, 0)
        st_combine(t, 1)
        st_combine(t, 3)
        if not last:
            beta_next = temp_ref[t + 1]
            share = t == sweeps - 2
            lax.fori_loop(0, n_mb, lambda kb, _: (m_second(kb, beta_next, share), 0)[1], 0)
            if share:
                c_copy().start()
                for j in range(EARLY):
                    mu_copy(j).start()
        else:
            def m_last(kb, _):
                rows = pl.ds(pl.multiple_of(kb * MB, MB), MB)
                n_acc, acc = m_block(kb, (1, 3))
                emit(0, kb, n_ref[rows, :] + n_acc, s_ref[rows, :] + acc)
                return 0

            lax.fori_loop(0, n_mb, m_last, 0)
            w_copy(0).start()
            c_copy().wait_recv()

            def far_block(kb, _):
                for j in range(FB // SB):
                    mu_copy(kb * (FB // SB) + j).wait_recv()
                rows = pl.ds(pl.multiple_of(kb * FB, FB), FB)
                c = to_col(cfrow_ref[:, rows])
                c2 = jnp.concatenate([c, c], axis=1)
                n_acc = jnp.zeros((FB, 128), F32)
                acc = jnp.zeros((FB, dim), F32)
                for ic in range(4 * n_ch):
                    cols = pl.ds(ic * IB, IB)
                    xt = x_ref[cols, :]
                    a = lax.dot_general(muf_ref[rows, :], xt, NT, preferred_element_type=F32)
                    r = jnp.exp2((a * tb + c2) - lse_ref[:, cols])
                    n_acc = n_acc + (r[:, :128] + r[:, 128:])
                    acc = acc + jnp.dot(r.astype(BF16), xt, preferred_element_type=F32)
                emit(1, kb, n_acc, acc)
                return 0

            lax.fori_loop(0, n_fb, far_block, 0)
            w_copy(1).start()
            mine = pl.ds(pl.multiple_of(data * nq, nq), nq)
            xo = x_ref[mine, :].astype(F32)
            sq = xo * xo
            hi = sq.astype(BF16)
            lo = (sq - hi.astype(F32)).astype(BF16)
            ones = jnp.ones((8, dim), BF16)
            row_sq = (lax.dot_general(ones, hi, NT, preferred_element_type=F32)
                      + lax.dot_general(ones, lo, NT, preferred_element_type=F32))
            lse_out_ref[...] = LN2 * lse_ref[:, mine] - beta * row_sq[0:1, :]

    for kind in range(3):
        for ch in range(n_ch):
            pts_copy(kind, ch).wait_send()
    for t in range(sweeps):
        for q in range(4):
            for r in range(1, 8):
                st_copy(t, q, r).wait_send()
    for j in range(n_sb):
        mu_copy(j).wait_send()
    c_copy().wait_send()
    for slot in range(2):
        w_copy(slot).wait_send()
        for kb in range((n_mb, n_fb)[slot]):
            out_copy(slot, kb).wait_send()

    def sibling(dev_slot):
        owner = (sib, data_xor(3))[dev_slot]
        size = (MB, FB)[dev_slot]
        for kb in range((n_mb, n_fb)[dev_slot]):
            rows = pl.ds(pl.multiple_of(owner * own + kb * size, size), size)
            pltpu.make_async_remote_copy(
                src_ref=means_ref.at[rows], dst_ref=means_ref.at[rows], send_sem=out_send.at[dev_slot, kb],
                recv_sem=out_recv.at[dev_slot, kb], device_id=peer(1), device_id_type=MESH).wait_recv()
        pltpu.make_async_remote_copy(
            src_ref=logw_ref.at[owner], dst_ref=logw_ref.at[owner], send_sem=w_send.at[dev_slot],
            recv_sem=w_recv.at[dev_slot], device_id=peer(1), device_id_type=MESH).wait_recv()

    sibling(0)
    sibling(1)


def flush_kernel(means_ref, logw_ref, lse_ref, means_out, logw_out, lse_out, sem):
    rows = means_ref.shape[0] // PIECES
    copies = [pltpu.make_async_copy(means_ref.at[pl.ds(i * rows, rows)], means_out.at[pl.ds(i * rows, rows)], sem.at[i])
              for i in range(PIECES)]
    copies.append(pltpu.make_async_copy(logw_ref, logw_out, sem.at[PIECES]))
    copies.append(pltpu.make_async_copy(lse_ref, lse_out, sem.at[PIECES + 1]))
    for cp in copies:
        cp.start()
    for cp in copies:
        cp.wait()


def solution(mesh):
    comp_size = mesh.shape["comp"]
    data_size = mesh.shape["data"]

    def local_fit(points, mu_init, logpi_init, inv_temp):
        nq, dim = points.shape
        rows = mu_init.shape[0]
        own = rows // data_size
        sweeps = inv_temp.shape[0]
        n_pts = nq * data_size
        n_kb = own // KB
        norm_const = n_pts + rows * comp_size * ALPHA
        cfg = (sweeps, own, nq, dim, norm_const)
        any_spec = pl.BlockSpec(memory_space=pl.ANY)
        vmem_spec = pl.BlockSpec(memory_space=pltpu.VMEM)
        dma = pltpu.SemaphoreType.DMA
        n_fb, n_sb = own // FB, own // SB
        means, logw, lse = pl.pallas_call(
            functools.partial(fit_kernel, cfg),
            out_shape=(pltpu.VMEM((rows, dim), F32),
                       pltpu.VMEM((data_size, 1, own), F32),
                       pltpu.VMEM((1, nq), F32)),
            in_specs=[pl.BlockSpec(memory_space=pltpu.SMEM), any_spec, any_spec, any_spec],
            out_specs=(vmem_spec, vmem_spec, vmem_spec),
            scratch_shapes=[
                pltpu.VMEM((n_pts, dim), BF16),
                pltpu.VMEM((own, n_pts + 128), F32),
                pltpu.VMEM((own, dim), BF16),
                pltpu.VMEM((own, dim), BF16),
                pltpu.VMEM((own, 128), F32),
                pltpu.VMEM((1, own), F32),
                pltpu.VMEM((1, own), F32),
                pltpu.VMEM((own, dim), F32),
                pltpu.VMEM((own, 128), F32),
                pltpu.VMEM((own // KT, 8, n_pts), F32),
                pltpu.VMEM((own // KT, 8, n_pts), F32),
                pltpu.VMEM((1, n_pts), F32),
                pltpu.VMEM((sweeps, data_size, 8, 1, nq), F32),
                dma((3,)),
                dma((3, nq // IB)), dma((3, nq // IB)),
                dma((sweeps, 4, 8)), dma((sweeps, 4, 8)),
                dma((n_sb + 1,)), dma((n_sb + 1,)),
                dma((2, n_fb)), dma((2, n_fb)),
                dma((2,)), dma((2,)),
            ],
            compiler_params=pltpu.CompilerParams(
                collective_id=0, has_side_effects=True, vmem_limit_bytes=54 * 1024 * 1024),
        )(inv_temp, points, mu_init, logpi_init.reshape(data_size, 1, own))
        results = [pltpu.with_memory_space_constraint(v, pltpu.VMEM) for v in (means, logw, lse)]
        means, logw, lse = pl.pallas_call(
            flush_kernel,
            out_shape=tuple(jax.ShapeDtypeStruct(v.shape, F32) for v in results),
            in_specs=[vmem_spec] * 3,
            out_specs=(any_spec,) * 3,
            scratch_shapes=[dma((PIECES + 2,))],
            compiler_params=pltpu.CompilerParams(vmem_limit_bytes=16 * 1024 * 1024),
        )(*results)
        return means, logw.reshape(rows), lse.reshape(nq)

    row_spec = P(("fit", "data"), None)
    comp_spec = P(("fit", "comp"), None)
    weight_spec = P(("fit", "comp"))
    lse_spec = P(("fit", "data"))
    return jax.shard_map(local_fit, mesh=mesh, in_specs=(row_spec, comp_spec, weight_spec, P(None)), out_specs=(comp_spec, weight_spec, lse_spec), check_vma=False)
```

```python
import functools
import math

import jax
import jax.numpy as jnp
from jax import lax
from jax.experimental import pallas as pl
from jax.experimental.pallas import tpu as pltpu
from jax.sharding import PartitionSpec as P

EPS_COUNT = 1e-6
ALPHA = 1e-3
PIECES = 8
LOG2E = math.log2(math.e)
LN2 = math.log(2.0)
KB = 1024
IB = 256
KT = 512
MB = 1024
EARLY = 4
SB = 256
FB = 512
MESH = pl.DeviceIdType.MESH
F32 = jnp.float32
BF16 = jnp.bfloat16
NN = (((1,), (0,)), ((), ()))


def fit_kernel(cfg, temp_ref, pts_ref, mu_ref, logpi_ref, means_ref, logw_ref, lse_out_ref,
               x_ref, xt_ref, p_ref, mub_ref, muf_ref, c_ref, crow_ref, cfrow_ref, s_ref, n_ref,
               m_ref, sum_ref, lse_ref, g_ref,
               loc_sem, pts_send, pts_recv, st_send, st_recv, mu_send, mu_recv,
               out_send, out_recv, w_send, w_recv):
    sweeps, own, nq, dim, norm_const = cfg
    n_kb = own // KB
    n_kt = own // KT
    n_mb = own // MB
    n_fb = own // FB
    n_sb = own // SB
    n_ch = nq // IB
    fit = lax.axis_index("fit")
    comp = lax.axis_index("comp")
    data = lax.axis_index("data")
    xpos = data // 2

    def data_xor(d):
        if d == 0:
            return data
        if d == 1:
            return data + 1 - 2 * (data % 2)
        if d == 2:
            return (data + 2) % 4
        return (data + 1 - 2 * (data % 2) + 2) % 4

    def peer(r):
        return (fit, (comp + r // 4) % 2, data_xor(r % 4))

    sib, par = data_xor(1), data_xor(2)
    me = comp * 4 + data

    barrier = pltpu.get_barrier_semaphore()
    for r in range(1, 8):
        pl.semaphore_signal(barrier, inc=1, device_id=peer(r), device_id_type=MESH)

    ld_pts = pltpu.make_async_copy(pts_ref, x_ref.at[pl.ds(pl.multiple_of(data * nq, nq), nq)], loc_sem.at[0])
    ld_mu = pltpu.make_async_copy(mu_ref.at[pl.ds(pl.multiple_of(data * own, own), own)], s_ref, loc_sem.at[1])
    ld_pi = pltpu.make_async_copy(logpi_ref.at[data], crow_ref, loc_sem.at[2])
    ld_pts.start()
    ld_mu.start()
    ld_pi.start()
    pl.semaphore_wait(barrier, 7)

    def pts_copy(kind, ch):
        owner = data if kind < 2 else par
        rows = pl.ds(pl.multiple_of(owner * nq + ch * IB, IB), IB)
        src = pts_ref.at[pl.ds(ch * IB, IB)] if kind < 2 else x_ref.at[rows]
        dev = peer(2) if kind == 1 else peer(1)
        return pltpu.make_async_remote_copy(
            src_ref=src, dst_ref=x_ref.at[rows], send_sem=pts_send.at[kind, ch], recv_sem=pts_recv.at[kind, ch],
            device_id=dev, device_id_type=MESH)

    for ch in range(n_ch):
        pts_copy(1, ch).start()
    for ch in range(n_ch):
        pts_copy(0, ch).start()

    def to_col(row):
        return jnp.transpose(jnp.broadcast_to(row, (128, row.shape[1])))

    def to_row(col):
        return jnp.transpose(col)[0:1, :]

    ld_pi.wait()
    ld_mu.wait()
    beta0 = temp_ref[0]

    def init_body(kb, _):
        rows = pl.ds(pl.multiple_of(kb * KB, KB), KB)
        mu = s_ref[rows, :]
        mub_ref[rows, :] = mu.astype(BF16)
        msq = jnp.sum(mu * mu, axis=1, keepdims=True)
        lp = to_col(crow_ref[:, rows])
        c_ref[rows, :] = LOG2E * (lp - beta0 * msq)
        return 0

    lax.fori_loop(0, n_kb, init_body, 0)

    def e_tiles(starts, tb, first=False):
        def logits(i0, kb):
            xt = xt_ref[:, pl.ds(pl.multiple_of(i0, IB), IB)]
            a = lax.dot_general(mub_ref[pl.ds(kb * KB, KB), :], xt, NN, preferred_element_type=F32)
            for u in range(KB // KT):
                cc = c_ref[pl.ds(kb * KB + u * KT, KT), :]
                l = a[u * KT:(u + 1) * KT, :] * tb + jnp.concatenate([cc, cc], axis=1)
                yield kb * (KB // KT) + u, pl.ds(kb * KB + u * KT, KT), l.reshape(KT // 8, 8, IB)

        def maxima(i0, kb):
            cols = pl.ds(pl.multiple_of(i0, IB), IB)
            for tile, _, l3 in logits(i0, kb):
                m_ref[tile, :, cols] = jnp.max(l3, axis=0)

        def exponentials(i0, kb):
            cols = pl.ds(pl.multiple_of(i0, IB), IB)
            for tile, rows, l3 in logits(i0, kb):
                p3 = jnp.exp2(l3 - m_ref[tile, :, cols][None])
                p_ref[rows, cols] = p3.reshape(KT, IB)
                sum_ref[tile, :, cols] = jnp.sum(p3, axis=0)

        if first:
            for i0 in starts:
                cols = pl.ds(pl.multiple_of(i0, IB), IB)
                xt_ref[:, cols] = jnp.transpose(x_ref[cols, :])
        steps = [(i0, kb) for i0 in starts for kb in range(n_kb)]
        maxima(*steps[0])
        for i, step in enumerate(steps):
            if i + 1 < len(steps):
                maxima(*steps[i + 1])
            exponentials(*step)

    def e_quarter(q, tb, first):
        e_tiles([q * nq + it * IB for it in range(n_ch)], tb, first)

    def st_copy(t, q, r):
        return pltpu.make_async_remote_copy(
            src_ref=g_ref.at[t, q, me], dst_ref=g_ref.at[t, q, me], send_sem=st_send.at[t, q, r],
            recv_sem=st_recv.at[t, q, r], device_id=peer(r), device_id_type=MESH)

    def st_send_all(t, q):
        cols = pl.ds(pl.multiple_of(q * nq, nq), nq)
        top = jnp.max(jnp.max(m_ref[:, :, cols], axis=0), axis=0, keepdims=True)
        tot = jnp.sum(sum_ref[:, :, cols] * jnp.exp2(m_ref[:, :, cols] - top), axis=0)
        tot = jnp.sum(tot, axis=0, keepdims=True)
        g_ref[t, q, me] = top + LOG2E * jnp.log(tot)
        for r in range(1, 8):
            st_copy(t, q, r).start()

    def e_step(t, q, tb):
        e_quarter(q, tb, t == 0)
        st_send_all(t, q)

    def st_combine(t, q):
        for r in range(1, 8):
            st_copy(t, q, r).wait_recv()
        cols = pl.ds(pl.multiple_of(q * nq, nq), nq)
        vals = g_ref[t, q]
        top = jnp.max(vals, axis=0)
        tot = jnp.sum(jnp.exp2(vals - top[None]), axis=0)
        lse = top + LOG2E * jnp.log(tot)
        lse_ref[:, cols] = lse
        m_ref[:, :, cols] = jnp.exp2(m_ref[:, :, cols] - lse)

    def m_block(kb, quarters):
        rows = pl.ds(pl.multiple_of(kb * MB, MB), MB)
        n_acc = jnp.zeros((MB, 128), F32)
        acc = jnp.zeros((MB, dim), F32)
        for q in quarters:
            for ic in range(n_ch):
                cols = pl.ds(q * nq + ic * IB, IB)
                sc = m_ref[pl.ds(kb * (MB // KT), MB // KT), :, cols]
                r = (p_ref[rows, cols].reshape(MB // KT, KT // 8, 8, IB) * sc[:, None]).reshape(MB, IB)
                n_acc = n_acc + (r[:, :128] + r[:, 128:])
                acc = acc + jnp.dot(r.astype(BF16), x_ref[cols, :], preferred_element_type=F32)
        return n_acc, acc

    def m_first(kb, _):
        rows = pl.ds(pl.multiple_of(kb * MB, MB), MB)
        n_acc, acc = m_block(kb, (0, 2))
        n_ref[rows, :] = n_acc
        s_ref[rows, :] = acc
        return 0

    def finish(n_acc, acc):
        n = jnp.sum(n_acc, axis=1, keepdims=True)
        mu = acc * (1.0 / (n + EPS_COUNT))
        return n, mu

    def mu_copy(j):
        rows = pl.ds(pl.multiple_of(j * SB, SB), SB)
        return pltpu.make_async_remote_copy(
            src_ref=mub_ref.at[rows], dst_ref=muf_ref.at[rows], send_sem=mu_send.at[j], recv_sem=mu_recv.at[j],
            device_id=peer(2), device_id_type=MESH)

    def c_copy():
        return pltpu.make_async_remote_copy(
            src_ref=crow_ref, dst_ref=cfrow_ref, send_sem=mu_send.at[n_sb], recv_sem=mu_recv.at[n_sb],
            device_id=peer(2), device_id_type=MESH)

    def m_second(kb, beta_next, share):
        rows = pl.ds(pl.multiple_of(kb * MB, MB), MB)
        n_acc, acc = m_block(kb, (1, 3))
        n, mu = finish(n_ref[rows, :] + n_acc, s_ref[rows, :] + acc)
        mub_ref[rows, :] = mu.astype(BF16)
        msq = jnp.sum(mu * mu, axis=1, keepdims=True)
        lp = jnp.log((jnp.broadcast_to(n, (MB, 128)) + ALPHA) / norm_const)
        c = LOG2E * (lp - beta_next * msq)
        c_ref[rows, :] = c
        if share:
            crow_ref[:, rows] = to_row(c)

    def out_copy(slot, kb):
        size = (MB, FB)[slot]
        owner = data if slot == 0 else par
        rows = pl.ds(pl.multiple_of(owner * own + kb * size, size), size)
        return pltpu.make_async_remote_copy(
            src_ref=means_ref.at[rows], dst_ref=means_ref.at[rows], send_sem=out_send.at[slot, kb],
            recv_sem=out_recv.at[slot, kb], device_id=peer(1), device_id_type=MESH)

    def w_copy(slot):
        owner = data if slot == 0 else par
        return pltpu.make_async_remote_copy(
            src_ref=logw_ref.at[owner], dst_ref=logw_ref.at[owner], send_sem=w_send.at[slot], recv_sem=w_recv.at[slot],
            device_id=peer(1), device_id_type=MESH)

    def emit(slot, kb, n_acc, acc):
        size = (MB, FB)[slot]
        owner = data if slot == 0 else par
        n, mu = finish(n_acc, acc)
        means_ref[pl.ds(pl.multiple_of(owner * own + kb * size, size), size), :] = mu
        nrow = to_row(jnp.broadcast_to(n, (size, 128)))
        logw_ref[owner, :, pl.ds(pl.multiple_of(kb * size, size), size)] = jnp.log((nrow + ALPHA) / norm_const)
        out_copy(slot, kb).start()

    for t in range(sweeps):
        beta = temp_ref[t]
        tb = (2.0 * LOG2E) * beta
        last = t == sweeps - 1
        if t == 0:
            ld_pts.wait()
            for ch in range(n_ch):
                pts_copy(0, ch).wait_recv()
            lax.fori_loop(0, 2, lambda s, _: (e_step(0, xpos * 2 + s, tb), 0)[1], 0)

            def far_points(ch, _):
                pts_copy(1, ch).wait_recv()
                pts_copy(2, ch).start()
                e_tiles([par * nq + ch * IB], tb, True)
                pts_copy(2, ch).wait_recv()
                e_tiles([data_xor(3) * nq + ch * IB], tb, True)
                return 0

            lax.fori_loop(0, n_ch, far_points, 0)
            st_send_all(0, par)
            st_send_all(0, data_xor(3))
        else:
            lax.fori_loop(0, 4, lambda s, _: (e_step(t, (s % 2) * 2 + s // 2, tb), 0)[1], 0)
            if last:
                for j in range(EARLY, n_sb):
                    mu_copy(j).start()
        st_combine(t, 0)
        st_combine(t, 2)
        lax.fori_loop(0, n_mb, m_first, 0)
        st_combine(t, 1)
        st_combine(t, 3)
        if not last:
            beta_next = temp_ref[t + 1]
            share = t == sweeps - 2
            lax.fori_loop(0, n_mb, lambda kb, _: (m_second(kb, beta_next, share), 0)[1], 0)
            if share:
                c_copy().start()
                for j in range(EARLY):
                    mu_copy(j).start()
        else:
            def m_last(kb, _):
                rows = pl.ds(pl.multiple_of(kb * MB, MB), MB)
                n_acc, acc = m_block(kb, (1, 3))
                emit(0, kb, n_ref[rows, :] + n_acc, s_ref[rows, :] + acc)
                return 0

            lax.fori_loop(0, n_mb, m_last, 0)
            w_copy(0).start()
            c_copy().wait_recv()

            def far_block(kb, _):
                for j in range(FB // SB):
                    mu_copy(kb * (FB // SB) + j).wait_recv()
                rows = pl.ds(pl.multiple_of(kb * FB, FB), FB)
                c = to_col(cfrow_ref[:, rows])
                c2 = jnp.concatenate([c, c], axis=1)
                n_acc = jnp.zeros((FB, 128), F32)
                acc = jnp.zeros((FB, dim), F32)
                for ic in range(4 * n_ch):
                    cols = pl.ds(ic * IB, IB)
                    a = lax.dot_general(muf_ref[rows, :], xt_ref[:, cols], NN, preferred_element_type=F32)
                    r = jnp.exp2((a * tb + c2) - lse_ref[:, cols])
                    n_acc = n_acc + (r[:, :128] + r[:, 128:])
                    acc = acc + jnp.dot(r.astype(BF16), x_ref[cols, :], preferred_element_type=F32)
                emit(1, kb, n_acc, acc)
                return 0

            lax.fori_loop(0, n_fb, far_block, 0)
            w_copy(1).start()
            mine = pl.ds(pl.multiple_of(data * nq, nq), nq)
            xo = xt_ref[:, mine].astype(F32)
            row_sq = jnp.sum(xo * xo, axis=0, keepdims=True)
            lse_out_ref[...] = LN2 * lse_ref[:, mine] - beta * row_sq

    for kind in range(3):
        for ch in range(n_ch):
            pts_copy(kind, ch).wait_send()
    for t in range(sweeps):
        for q in range(4):
            for r in range(1, 8):
                st_copy(t, q, r).wait_send()
    for j in range(n_sb):
        mu_copy(j).wait_send()
    c_copy().wait_send()
    for slot in range(2):
        w_copy(slot).wait_send()
        for kb in range((n_mb, n_fb)[slot]):
            out_copy(slot, kb).wait_send()

    def sibling(dev_slot):
        owner = (sib, data_xor(3))[dev_slot]
        size = (MB, FB)[dev_slot]
        for kb in range((n_mb, n_fb)[dev_slot]):
            rows = pl.ds(pl.multiple_of(owner * own + kb * size, size), size)
            pltpu.make_async_remote_copy(
                src_ref=means_ref.at[rows], dst_ref=means_ref.at[rows], send_sem=out_send.at[dev_slot, kb],
                recv_sem=out_recv.at[dev_slot, kb], device_id=peer(1), device_id_type=MESH).wait_recv()
        pltpu.make_async_remote_copy(
            src_ref=logw_ref.at[owner], dst_ref=logw_ref.at[owner], send_sem=w_send.at[dev_slot],
            recv_sem=w_recv.at[dev_slot], device_id=peer(1), device_id_type=MESH).wait_recv()

    sibling(0)
    sibling(1)


def flush_kernel(means_ref, logw_ref, lse_ref, means_out, logw_out, lse_out, sem):
    rows = means_ref.shape[0] // PIECES
    copies = [pltpu.make_async_copy(means_ref.at[pl.ds(i * rows, rows)], means_out.at[pl.ds(i * rows, rows)], sem.at[i])
              for i in range(PIECES)]
    copies.append(pltpu.make_async_copy(logw_ref, logw_out, sem.at[PIECES]))
    copies.append(pltpu.make_async_copy(lse_ref, lse_out, sem.at[PIECES + 1]))
    for cp in copies:
        cp.start()
    for cp in copies:
        cp.wait()


def solution(mesh):
    comp_size = mesh.shape["comp"]
    data_size = mesh.shape["data"]

    def local_fit(points, mu_init, logpi_init, inv_temp):
        nq, dim = points.shape
        rows = mu_init.shape[0]
        own = rows // data_size
        sweeps = inv_temp.shape[0]
        n_pts = nq * data_size
        n_kb = own // KB
        norm_const = n_pts + rows * comp_size * ALPHA
        cfg = (sweeps, own, nq, dim, norm_const)
        any_spec = pl.BlockSpec(memory_space=pl.ANY)
        vmem_spec = pl.BlockSpec(memory_space=pltpu.VMEM)
        dma = pltpu.SemaphoreType.DMA
        n_fb, n_sb = own // FB, own // SB
        means, logw, lse = pl.pallas_call(
            functools.partial(fit_kernel, cfg),
            out_shape=(pltpu.VMEM((rows, dim), F32),
                       pltpu.VMEM((data_size, 1, own), F32),
                       pltpu.VMEM((1, nq), F32)),
            in_specs=[pl.BlockSpec(memory_space=pltpu.SMEM), any_spec, any_spec, any_spec],
            out_specs=(vmem_spec, vmem_spec, vmem_spec),
            scratch_shapes=[
                pltpu.VMEM((n_pts, dim), BF16),
                pltpu.VMEM((dim, n_pts), BF16),
                pltpu.VMEM((own, n_pts + 128), F32),
                pltpu.VMEM((own, dim), BF16),
                pltpu.VMEM((own, dim), BF16),
                pltpu.VMEM((own, 128), F32),
                pltpu.VMEM((1, own), F32),
                pltpu.VMEM((1, own), F32),
                pltpu.VMEM((own, dim), F32),
                pltpu.VMEM((own, 128), F32),
                pltpu.VMEM((own // KT, 8, n_pts), F32),
                pltpu.VMEM((own // KT, 8, n_pts), F32),
                pltpu.VMEM((1, n_pts), F32),
                pltpu.VMEM((sweeps, data_size, 8, 1, nq), F32),
                dma((3,)),
                dma((3, nq // IB)), dma((3, nq // IB)),
                dma((sweeps, 4, 8)), dma((sweeps, 4, 8)),
                dma((n_sb + 1,)), dma((n_sb + 1,)),
                dma((2, n_fb)), dma((2, n_fb)),
                dma((2,)), dma((2,)),
            ],
            compiler_params=pltpu.CompilerParams(
                collective_id=0, has_side_effects=True, vmem_limit_bytes=54 * 1024 * 1024),
        )(inv_temp, points, mu_init, logpi_init.reshape(data_size, 1, own))
        results = [pltpu.with_memory_space_constraint(v, pltpu.VMEM) for v in (means, logw, lse)]
        means, logw, lse = pl.pallas_call(
            flush_kernel,
            out_shape=tuple(jax.ShapeDtypeStruct(v.shape, F32) for v in results),
            in_specs=[vmem_spec] * 3,
            out_specs=(any_spec,) * 3,
            scratch_shapes=[dma((PIECES + 2,))],
            compiler_params=pltpu.CompilerParams(vmem_limit_bytes=16 * 1024 * 1024),
        )(*results)
        return means, logw.reshape(rows), lse.reshape(nq)

    row_spec = P(("fit", "data"), None)
    comp_spec = P(("fit", "comp"), None)
    weight_spec = P(("fit", "comp"))
    lse_spec = P(("fit", "data"))
    return jax.shard_map(local_fit, mesh=mesh, in_specs=(row_spec, comp_spec, weight_spec, P(None)), out_specs=(comp_spec, weight_spec, lse_spec), check_vma=False)
```

```python
import functools
import math

import jax
import jax.numpy as jnp
from jax import lax
from jax.experimental import pallas as pl
from jax.experimental.pallas import tpu as pltpu
from jax.sharding import PartitionSpec as P

EPS_COUNT = 1e-6
ALPHA = 1e-3
PIECES = 8
LOG2E = math.log2(math.e)
LN2 = math.log(2.0)
KB = 1024
IB = 256
KT = 512
MB = 1024
EARLY = 3
SB = 256
FB = 512
MESH = pl.DeviceIdType.MESH
F32 = jnp.float32
BF16 = jnp.bfloat16
NT = (((1,), (1,)), ((), ()))


def fit_kernel(cfg, temp_ref, pts_ref, mu_ref, logpi_ref, means_ref, logw_ref, lse_out_ref,
               x_ref, p_ref, mub_ref, muf_ref, c_ref, crow_ref, cfrow_ref, s_ref, n_ref,
               m_ref, sum_ref, lse_ref, g_ref,
               loc_sem, pts_send, pts_recv, st_send, st_recv, mu_send, mu_recv,
               out_send, out_recv, w_send, w_recv):
    sweeps, own, nq, dim, norm_const = cfg
    n_kb = own // KB
    n_kt = own // KT
    n_mb = own // MB
    n_fb = own // FB
    n_sb = own // SB
    n_ch = nq // IB
    fit = lax.axis_index("fit")
    comp = lax.axis_index("comp")
    data = lax.axis_index("data")
    xpos = data // 2

    def data_xor(d):
        if d == 0:
            return data
        if d == 1:
            return data + 1 - 2 * (data % 2)
        if d == 2:
            return (data + 2) % 4
        return (data + 1 - 2 * (data % 2) + 2) % 4

    def peer(r):
        return (fit, (comp + r // 4) % 2, data_xor(r % 4))

    sib, par = data_xor(1), data_xor(2)
    me = comp * 4 + data

    barrier = pltpu.get_barrier_semaphore()
    for r in range(1, 8):
        pl.semaphore_signal(barrier, inc=1, device_id=peer(r), device_id_type=MESH)

    ld_pts = pltpu.make_async_copy(pts_ref, x_ref.at[pl.ds(pl.multiple_of(data * nq, nq), nq)], loc_sem.at[0])
    ld_mu = pltpu.make_async_copy(mu_ref.at[pl.ds(pl.multiple_of(data * own, own), own)], s_ref, loc_sem.at[1])
    ld_pi = pltpu.make_async_copy(logpi_ref.at[data], crow_ref, loc_sem.at[2])
    ld_pts.start()
    ld_mu.start()
    ld_pi.start()
    pl.semaphore_wait(barrier, 7)

    def pts_copy(kind, ch):
        owner = data if kind < 2 else par
        rows = pl.ds(pl.multiple_of(owner * nq + ch * IB, IB), IB)
        src = pts_ref.at[pl.ds(ch * IB, IB)] if kind < 2 else x_ref.at[rows]
        dev = peer(2) if kind == 1 else peer(1)
        return pltpu.make_async_remote_copy(
            src_ref=src, dst_ref=x_ref.at[rows], send_sem=pts_send.at[kind, ch], recv_sem=pts_recv.at[kind, ch],
            device_id=dev, device_id_type=MESH)

    for ch in range(n_ch):
        pts_copy(1, ch).start()
    for ch in range(n_ch):
        pts_copy(0, ch).start()

    def to_col(row):
        return jnp.transpose(jnp.broadcast_to(row, (128, row.shape[1])))

    def to_row(col):
        return jnp.transpose(col)[0:1, :]

    ld_pi.wait()
    ld_mu.wait()
    beta0 = temp_ref[0]

    def init_body(kb, _):
        rows = pl.ds(pl.multiple_of(kb * KB, KB), KB)
        mu = s_ref[rows, :]
        mub_ref[rows, :] = mu.astype(BF16)
        msq = jnp.sum(mu * mu, axis=1, keepdims=True)
        lp = to_col(crow_ref[:, rows])
        c_ref[rows, :] = LOG2E * (lp - beta0 * msq)
        return 0

    lax.fori_loop(0, n_kb, init_body, 0)

    def e_tiles(starts, tb):
        def logits(i0, kb):
            xt = x_ref[pl.ds(pl.multiple_of(i0, IB), IB), :]
            a = lax.dot_general(mub_ref[pl.ds(kb * KB, KB), :], xt, NT, preferred_element_type=F32)
            for u in range(KB // KT):
                cc = c_ref[pl.ds(kb * KB + u * KT, KT), :]
                l = a[u * KT:(u + 1) * KT, :] * tb + jnp.concatenate([cc, cc], axis=1)
                yield kb * (KB // KT) + u, pl.ds(kb * KB + u * KT, KT), l.reshape(KT // 8, 8, IB)

        def maxima(i0, kb):
            cols = pl.ds(pl.multiple_of(i0, IB), IB)
            for tile, _, l3 in logits(i0, kb):
                m_ref[tile, :, cols] = jnp.max(l3, axis=0)

        def exponentials(i0, kb):
            cols = pl.ds(pl.multiple_of(i0, IB), IB)
            for tile, rows, l3 in logits(i0, kb):
                p3 = jnp.exp2(l3 - m_ref[tile, :, cols][None])
                p_ref[rows, cols] = p3.reshape(KT, IB)
                sum_ref[tile, :, cols] = jnp.sum(p3, axis=0)

        steps = [(i0, kb) for i0 in starts for kb in range(n_kb)]
        maxima(*steps[0])
        for i, step in enumerate(steps):
            if i + 1 < len(steps):
                maxima(*steps[i + 1])
            exponentials(*step)

    def e_quarter(q, tb):
        e_tiles([q * nq + it * IB for it in range(n_ch)], tb)

    def st_copy(t, q, r):
        return pltpu.make_async_remote_copy(
            src_ref=g_ref.at[t, q, me], dst_ref=g_ref.at[t, q, me], send_sem=st_send.at[t, q, r],
            recv_sem=st_recv.at[t, q, r], device_id=peer(r), device_id_type=MESH)

    def st_send_all(t, q):
        cols = pl.ds(pl.multiple_of(q * nq, nq), nq)
        top = jnp.max(jnp.max(m_ref[:, :, cols], axis=0), axis=0, keepdims=True)
        tot = jnp.sum(sum_ref[:, :, cols] * jnp.exp2(m_ref[:, :, cols] - top), axis=0)
        tot = jnp.sum(tot, axis=0, keepdims=True)
        g_ref[t, q, me] = top + LOG2E * jnp.log(tot)
        for r in range(1, 8):
            st_copy(t, q, r).start()

    def e_step(t, q, tb):
        e_quarter(q, tb)
        st_send_all(t, q)

    def st_combine(t, q):
        for r in range(1, 8):
            st_copy(t, q, r).wait_recv()
        cols = pl.ds(pl.multiple_of(q * nq, nq), nq)
        vals = g_ref[t, q]
        top = jnp.max(vals, axis=0)
        tot = jnp.sum(jnp.exp2(vals - top[None]), axis=0)
        lse = top + LOG2E * jnp.log(tot)
        lse_ref[:, cols] = lse
        m_ref[:, :, cols] = jnp.exp2(m_ref[:, :, cols] - lse)

    def m_block(kb, quarters):
        rows = pl.ds(pl.multiple_of(kb * MB, MB), MB)
        n_acc = jnp.zeros((MB, 128), F32)
        acc = jnp.zeros((MB, dim), F32)
        for q in quarters:
            for ic in range(n_ch):
                cols = pl.ds(q * nq + ic * IB, IB)
                sc = m_ref[pl.ds(kb * (MB // KT), MB // KT), :, cols]
                r = (p_ref[rows, cols].reshape(MB // KT, KT // 8, 8, IB) * sc[:, None]).reshape(MB, IB)
                n_acc = n_acc + (r[:, :128] + r[:, 128:])
                acc = acc + jnp.dot(r.astype(BF16), x_ref[cols, :], preferred_element_type=F32)
        return n_acc, acc

    def m_first(kb, _):
        rows = pl.ds(pl.multiple_of(kb * MB, MB), MB)
        n_acc, acc = m_block(kb, (0, 2))
        n_ref[rows, :] = n_acc
        s_ref[rows, :] = acc
        return 0

    def finish(n_acc, acc):
        n = jnp.sum(n_acc, axis=1, keepdims=True)
        mu = acc * (1.0 / (n + EPS_COUNT))
        return n, mu

    def mu_copy(j):
        rows = pl.ds(pl.multiple_of(j * SB, SB), SB)
        return pltpu.make_async_remote_copy(
            src_ref=mub_ref.at[rows], dst_ref=muf_ref.at[rows], send_sem=mu_send.at[j], recv_sem=mu_recv.at[j],
            device_id=peer(2), device_id_type=MESH)

    def c_copy():
        return pltpu.make_async_remote_copy(
            src_ref=crow_ref, dst_ref=cfrow_ref, send_sem=mu_send.at[n_sb], recv_sem=mu_recv.at[n_sb],
            device_id=peer(2), device_id_type=MESH)

    def m_second(kb, beta_next, share):
        rows = pl.ds(pl.multiple_of(kb * MB, MB), MB)
        n_acc, acc = m_block(kb, (1, 3))
        n, mu = finish(n_ref[rows, :] + n_acc, s_ref[rows, :] + acc)
        mub_ref[rows, :] = mu.astype(BF16)
        msq = jnp.sum(mu * mu, axis=1, keepdims=True)
        lp = jnp.log((jnp.broadcast_to(n, (MB, 128)) + ALPHA) / norm_const)
        c = LOG2E * (lp - beta_next * msq)
        c_ref[rows, :] = c
        if share:
            crow_ref[:, rows] = to_row(c)

    def out_copy(slot, kb):
        size = (MB, FB)[slot]
        owner = data if slot == 0 else par
        rows = pl.ds(pl.multiple_of(owner * own + kb * size, size), size)
        return pltpu.make_async_remote_copy(
            src_ref=means_ref.at[rows], dst_ref=means_ref.at[rows], send_sem=out_send.at[slot, kb],
            recv_sem=out_recv.at[slot, kb], device_id=peer(1), device_id_type=MESH)

    def w_copy(slot):
        owner = data if slot == 0 else par
        return pltpu.make_async_remote_copy(
            src_ref=logw_ref.at[owner], dst_ref=logw_ref.at[owner], send_sem=w_send.at[slot], recv_sem=w_recv.at[slot],
            device_id=peer(1), device_id_type=MESH)

    def emit(slot, kb, n_acc, acc):
        size = (MB, FB)[slot]
        owner = data if slot == 0 else par
        n, mu = finish(n_acc, acc)
        means_ref[pl.ds(pl.multiple_of(owner * own + kb * size, size), size), :] = mu
        nrow = to_row(jnp.broadcast_to(n, (size, 128)))
        logw_ref[owner, :, pl.ds(pl.multiple_of(kb * size, size), size)] = jnp.log((nrow + ALPHA) / norm_const)
        out_copy(slot, kb).start()

    for t in range(sweeps):
        beta = temp_ref[t]
        tb = (2.0 * LOG2E) * beta
        last = t == sweeps - 1
        if t == 0:
            ld_pts.wait()
            for ch in range(n_ch):
                pts_copy(0, ch).wait_recv()
            lax.fori_loop(0, 2, lambda s, _: (e_step(0, xpos * 2 + s, tb), 0)[1], 0)

            away = (1 - xpos) * 2

            def far_points(ch, _):
                pts_copy(1, ch).wait_recv()
                pts_copy(2, ch).start()
                pts_copy(2, ch).wait_recv()
                e_tiles([away * nq + ch * IB], tb)
                return 0

            lax.fori_loop(0, n_ch, far_points, 0)
            st_send_all(0, away)
            e_step(0, away + 1, tb)
        else:
            lax.fori_loop(0, 4, lambda s, _: (e_step(t, (s % 2) * 2 + s // 2, tb), 0)[1], 0)
            if last:
                for j in range(EARLY, n_sb):
                    mu_copy(j).start()
        st_combine(t, 0)
        st_combine(t, 2)
        lax.fori_loop(0, n_mb, m_first, 0)
        st_combine(t, 1)
        st_combine(t, 3)
        if not last:
            beta_next = temp_ref[t + 1]
            share = t == sweeps - 2
            lax.fori_loop(0, n_mb, lambda kb, _: (m_second(kb, beta_next, share), 0)[1], 0)
            if share:
                c_copy().start()
                for j in range(EARLY):
                    mu_copy(j).start()
        else:
            def m_last(kb, _):
                rows = pl.ds(pl.multiple_of(kb * MB, MB), MB)
                n_acc, acc = m_block(kb, (1, 3))
                emit(0, kb, n_ref[rows, :] + n_acc, s_ref[rows, :] + acc)
                return 0

            lax.fori_loop(0, n_mb, m_last, 0)
            w_copy(0).start()
            c_copy().wait_recv()

            def far_block(kb, _):
                for j in range(FB // SB):
                    mu_copy(kb * (FB // SB) + j).wait_recv()
                rows = pl.ds(pl.multiple_of(kb * FB, FB), FB)
                c = to_col(cfrow_ref[:, rows])
                c2 = jnp.concatenate([c, c], axis=1)
                n_acc = jnp.zeros((FB, 128), F32)
                acc = jnp.zeros((FB, dim), F32)
                for ic in range(4 * n_ch):
                    cols = pl.ds(ic * IB, IB)
                    xt = x_ref[cols, :]
                    a = lax.dot_general(muf_ref[rows, :], xt, NT, preferred_element_type=F32)
                    r = jnp.exp2((a * tb + c2) - lse_ref[:, cols])
                    n_acc = n_acc + (r[:, :128] + r[:, 128:])
                    acc = acc + jnp.dot(r.astype(BF16), xt, preferred_element_type=F32)
                emit(1, kb, n_acc, acc)
                return 0

            lax.fori_loop(0, n_fb, far_block, 0)
            w_copy(1).start()
            mine = pl.ds(pl.multiple_of(data * nq, nq), nq)
            xo = x_ref[mine, :].astype(F32)
            sq = xo * xo
            hi = sq.astype(BF16)
            lo = (sq - hi.astype(F32)).astype(BF16)
            ones = jnp.ones((8, dim), BF16)
            row_sq = (lax.dot_general(ones, hi, NT, preferred_element_type=F32)
                      + lax.dot_general(ones, lo, NT, preferred_element_type=F32))
            lse_out_ref[...] = LN2 * lse_ref[:, mine] - beta * row_sq[0:1, :]

    for kind in range(3):
        for ch in range(n_ch):
            pts_copy(kind, ch).wait_send()
    for t in range(sweeps):
        for q in range(4):
            for r in range(1, 8):
                st_copy(t, q, r).wait_send()
    for j in range(n_sb):
        mu_copy(j).wait_send()
    c_copy().wait_send()
    for slot in range(2):
        w_copy(slot).wait_send()
        for kb in range((n_mb, n_fb)[slot]):
            out_copy(slot, kb).wait_send()

    def sibling(dev_slot):
        owner = (sib, data_xor(3))[dev_slot]
        size = (MB, FB)[dev_slot]
        for kb in range((n_mb, n_fb)[dev_slot]):
            rows = pl.ds(pl.multiple_of(owner * own + kb * size, size), size)
            pltpu.make_async_remote_copy(
                src_ref=means_ref.at[rows], dst_ref=means_ref.at[rows], send_sem=out_send.at[dev_slot, kb],
                recv_sem=out_recv.at[dev_slot, kb], device_id=peer(1), device_id_type=MESH).wait_recv()
        pltpu.make_async_remote_copy(
            src_ref=logw_ref.at[owner], dst_ref=logw_ref.at[owner], send_sem=w_send.at[dev_slot],
            recv_sem=w_recv.at[dev_slot], device_id=peer(1), device_id_type=MESH).wait_recv()

    sibling(0)
    sibling(1)


def flush_kernel(means_ref, logw_ref, lse_ref, means_out, logw_out, lse_out, sem):
    rows = means_ref.shape[0] // PIECES
    copies = [pltpu.make_async_copy(means_ref.at[pl.ds(i * rows, rows)], means_out.at[pl.ds(i * rows, rows)], sem.at[i])
              for i in range(PIECES)]
    copies.append(pltpu.make_async_copy(logw_ref, logw_out, sem.at[PIECES]))
    copies.append(pltpu.make_async_copy(lse_ref, lse_out, sem.at[PIECES + 1]))
    for cp in copies:
        cp.start()
    for cp in copies:
        cp.wait()


def solution(mesh):
    comp_size = mesh.shape["comp"]
    data_size = mesh.shape["data"]

    def local_fit(points, mu_init, logpi_init, inv_temp):
        nq, dim = points.shape
        rows = mu_init.shape[0]
        own = rows // data_size
        sweeps = inv_temp.shape[0]
        n_pts = nq * data_size
        n_kb = own // KB
        norm_const = n_pts + rows * comp_size * ALPHA
        cfg = (sweeps, own, nq, dim, norm_const)
        any_spec = pl.BlockSpec(memory_space=pl.ANY)
        vmem_spec = pl.BlockSpec(memory_space=pltpu.VMEM)
        dma = pltpu.SemaphoreType.DMA
        n_fb, n_sb = own // FB, own // SB
        means, logw, lse = pl.pallas_call(
            functools.partial(fit_kernel, cfg),
            out_shape=(pltpu.VMEM((rows, dim), F32),
                       pltpu.VMEM((data_size, 1, own), F32),
                       pltpu.VMEM((1, nq), F32)),
            in_specs=[pl.BlockSpec(memory_space=pltpu.SMEM), any_spec, any_spec, any_spec],
            out_specs=(vmem_spec, vmem_spec, vmem_spec),
            scratch_shapes=[
                pltpu.VMEM((n_pts, dim), BF16),
                pltpu.VMEM((own, n_pts + 128), F32),
                pltpu.VMEM((own, dim), BF16),
                pltpu.VMEM((own, dim), BF16),
                pltpu.VMEM((own, 128), F32),
                pltpu.VMEM((1, own), F32),
                pltpu.VMEM((1, own), F32),
                pltpu.VMEM((own, dim), F32),
                pltpu.VMEM((own, 128), F32),
                pltpu.VMEM((own // KT, 8, n_pts), F32),
                pltpu.VMEM((own // KT, 8, n_pts), F32),
                pltpu.VMEM((1, n_pts), F32),
                pltpu.VMEM((sweeps, data_size, 8, 1, nq), F32),
                dma((3,)),
                dma((3, nq // IB)), dma((3, nq // IB)),
                dma((sweeps, 4, 8)), dma((sweeps, 4, 8)),
                dma((n_sb + 1,)), dma((n_sb + 1,)),
                dma((2, n_fb)), dma((2, n_fb)),
                dma((2,)), dma((2,)),
            ],
            compiler_params=pltpu.CompilerParams(
                collective_id=0, has_side_effects=True, vmem_limit_bytes=54 * 1024 * 1024),
        )(inv_temp, points, mu_init, logpi_init.reshape(data_size, 1, own))
        results = [pltpu.with_memory_space_constraint(v, pltpu.VMEM) for v in (means, logw, lse)]
        means, logw, lse = pl.pallas_call(
            flush_kernel,
            out_shape=tuple(jax.ShapeDtypeStruct(v.shape, F32) for v in results),
            in_specs=[vmem_spec] * 3,
            out_specs=(any_spec,) * 3,
            scratch_shapes=[dma((PIECES + 2,))],
            compiler_params=pltpu.CompilerParams(vmem_limit_bytes=16 * 1024 * 1024),
        )(*results)
        return means, logw.reshape(rows), lse.reshape(nq)

    row_spec = P(("fit", "data"), None)
    comp_spec = P(("fit", "comp"), None)
    weight_spec = P(("fit", "comp"))
    lse_spec = P(("fit", "data"))
    return jax.shard_map(local_fit, mesh=mesh, in_specs=(row_spec, comp_spec, weight_spec, P(None)), out_specs=(comp_spec, weight_spec, lse_spec), check_vma=False)
```

```python
import functools
import math

import jax
import jax.numpy as jnp
from jax import lax
from jax.experimental import pallas as pl
from jax.experimental.pallas import tpu as pltpu
from jax.sharding import PartitionSpec as P

EPS_COUNT = 1e-6
ALPHA = 1e-3
PIECES = 8
LOG2E = math.log2(math.e)
LN2 = math.log(2.0)
KB = 1024
IB = 256
KT = 512
MB = 1024
EARLY = 3
SB = 256
FB = 512
MESH = pl.DeviceIdType.MESH
F32 = jnp.float32
BF16 = jnp.bfloat16
NT = (((1,), (1,)), ((), ()))


def fit_kernel(cfg, temp_ref, pts_ref, mu_ref, logpi_ref, means_ref, logw_ref, lse_out_ref,
               x_ref, p_ref, mub_ref, muf_ref, c_ref, crow_ref, cfrow_ref, s_ref, n_ref,
               m_ref, sum_ref, lse_ref, g_ref,
               loc_sem, pts_send, pts_recv, st_send, st_recv, mu_send, mu_recv,
               out_send, out_recv, w_send, w_recv):
    sweeps, own, nq, dim, norm_const = cfg
    n_kb = own // KB
    n_kt = own // KT
    n_mb = own // MB
    n_fb = own // FB
    n_sb = own // SB
    n_ch = nq // IB
    fit = lax.axis_index("fit")
    comp = lax.axis_index("comp")
    data = lax.axis_index("data")
    xpos = data // 2

    def data_xor(d):
        if d == 0:
            return data
        if d == 1:
            return data + 1 - 2 * (data % 2)
        if d == 2:
            return (data + 2) % 4
        return (data + 1 - 2 * (data % 2) + 2) % 4

    def peer(r):
        return (fit, (comp + r // 4) % 2, data_xor(r % 4))

    sib, par = data_xor(1), data_xor(2)
    me = comp * 4 + data

    barrier = pltpu.get_barrier_semaphore()
    for r in range(1, 8):
        pl.semaphore_signal(barrier, inc=1, device_id=peer(r), device_id_type=MESH)

    ld_pts = pltpu.make_async_copy(pts_ref, x_ref.at[pl.ds(pl.multiple_of(data * nq, nq), nq)], loc_sem.at[0])
    ld_mu = pltpu.make_async_copy(mu_ref.at[pl.ds(pl.multiple_of(data * own, own), own)], s_ref, loc_sem.at[1])
    ld_pi = pltpu.make_async_copy(logpi_ref.at[data], crow_ref, loc_sem.at[2])
    ld_pts.start()
    ld_mu.start()
    ld_pi.start()
    pl.semaphore_wait(barrier, 7)

    def pts_copy(kind, ch):
        owner = data if kind < 2 else par
        rows = pl.ds(pl.multiple_of(owner * nq + ch * IB, IB), IB)
        src = pts_ref.at[pl.ds(ch * IB, IB)] if kind < 2 else x_ref.at[rows]
        dev = peer(2) if kind == 1 else peer(1)
        return pltpu.make_async_remote_copy(
            src_ref=src, dst_ref=x_ref.at[rows], send_sem=pts_send.at[kind, ch], recv_sem=pts_recv.at[kind, ch],
            device_id=dev, device_id_type=MESH)

    for ch in range(n_ch):
        pts_copy(1, ch).start()
    for ch in range(n_ch):
        pts_copy(0, ch).start()

    def to_col(row):
        return jnp.transpose(jnp.broadcast_to(row, (128, row.shape[1])))

    def to_row(col):
        return jnp.transpose(col)[0:1, :]

    ld_pi.wait()
    ld_mu.wait()
    beta0 = temp_ref[0]

    def init_body(kb, _):
        rows = pl.ds(pl.multiple_of(kb * KB, KB), KB)
        mu = s_ref[rows, :]
        mub_ref[rows, :] = mu.astype(BF16)
        msq = jnp.sum(mu * mu, axis=1, keepdims=True)
        lp = to_col(crow_ref[:, rows])
        c_ref[rows, :] = LOG2E * (lp - beta0 * msq)
        return 0

    lax.fori_loop(0, n_kb, init_body, 0)

    def e_tiles(starts, tb):
        def logits(i0, kb):
            xt = x_ref[pl.ds(pl.multiple_of(i0, IB), IB), :]
            a = lax.dot_general(mub_ref[pl.ds(kb * KB, KB), :], xt, NT, preferred_element_type=F32)
            for u in range(KB // KT):
                cc = c_ref[pl.ds(kb * KB + u * KT, KT), :]
                l = a[u * KT:(u + 1) * KT, :] * tb + jnp.concatenate([cc, cc], axis=1)
                yield kb * (KB // KT) + u, pl.ds(kb * KB + u * KT, KT), l.reshape(KT // 8, 8, IB)

        def maxima(i0, kb):
            cols = pl.ds(pl.multiple_of(i0, IB), IB)
            for tile, _, l3 in logits(i0, kb):
                m_ref[tile, :, cols] = jnp.max(l3, axis=0)

        def exponentials(i0, kb):
            cols = pl.ds(pl.multiple_of(i0, IB), IB)
            for tile, rows, l3 in logits(i0, kb):
                p3 = jnp.exp2(l3 - m_ref[tile, :, cols][None])
                p_ref[rows, cols] = p3.reshape(KT, IB)
                sum_ref[tile, :, cols] = jnp.sum(p3, axis=0)

        steps = [(i0, kb) for i0 in starts for kb in range(n_kb)]
        maxima(*steps[0])
        for i, step in enumerate(steps):
            if i + 1 < len(steps):
                maxima(*steps[i + 1])
            exponentials(*step)

    def e_quarter(q, tb):
        e_tiles([q * nq + it * IB for it in range(n_ch)], tb)

    def st_copy(t, q, r):
        return pltpu.make_async_remote_copy(
            src_ref=g_ref.at[t, q, me], dst_ref=g_ref.at[t, q, me], send_sem=st_send.at[t, q, r],
            recv_sem=st_recv.at[t, q, r], device_id=peer(r), device_id_type=MESH)

    def st_send_all(t, q):
        cols = pl.ds(pl.multiple_of(q * nq, nq), nq)
        top = jnp.max(jnp.max(m_ref[:, :, cols], axis=0), axis=0, keepdims=True)
        tot = jnp.sum(sum_ref[:, :, cols] * jnp.exp2(m_ref[:, :, cols] - top), axis=0)
        tot = jnp.sum(tot, axis=0, keepdims=True)
        g_ref[t, q, me] = top + LOG2E * jnp.log(tot)
        for r in range(1, 8):
            st_copy(t, q, r).start()

    def e_step(t, q, tb):
        e_quarter(q, tb)
        st_send_all(t, q)

    def st_combine(t, q):
        for r in range(1, 8):
            st_copy(t, q, r).wait_recv()
        cols = pl.ds(pl.multiple_of(q * nq, nq), nq)
        vals = g_ref[t, q]
        top = jnp.max(vals, axis=0)
        tot = jnp.sum(jnp.exp2(vals - top[None]), axis=0)
        lse = top + LOG2E * jnp.log(tot)
        lse_ref[:, cols] = lse
        m_ref[:, :, cols] = jnp.exp2(m_ref[:, :, cols] - lse)

    def m_block(kb, quarters):
        rows = pl.ds(pl.multiple_of(kb * MB, MB), MB)
        n_acc = jnp.zeros((MB, 128), F32)
        acc = jnp.zeros((MB, dim), F32)
        for q in quarters:
            for ic in range(n_ch):
                cols = pl.ds(q * nq + ic * IB, IB)
                sc = m_ref[pl.ds(kb * (MB // KT), MB // KT), :, cols]
                r = (p_ref[rows, cols].reshape(MB // KT, KT // 8, 8, IB) * sc[:, None]).reshape(MB, IB)
                n_acc = n_acc + (r[:, :128] + r[:, 128:])
                acc = acc + jnp.dot(r.astype(BF16), x_ref[cols, :], preferred_element_type=F32)
        return n_acc, acc

    def m_first(kb, _):
        rows = pl.ds(pl.multiple_of(kb * MB, MB), MB)
        n_acc, acc = m_block(kb, (0, 2))
        n_ref[rows, :] = n_acc
        s_ref[rows, :] = acc
        return 0

    def finish(n_acc, acc):
        n = jnp.sum(n_acc, axis=1, keepdims=True)
        mu = acc * (1.0 / (n + EPS_COUNT))
        return n, mu

    def mu_copy(j):
        rows = pl.ds(pl.multiple_of(j * SB, SB), SB)
        return pltpu.make_async_remote_copy(
            src_ref=mub_ref.at[rows], dst_ref=muf_ref.at[rows], send_sem=mu_send.at[j], recv_sem=mu_recv.at[j],
            device_id=peer(2), device_id_type=MESH)

    def c_copy():
        return pltpu.make_async_remote_copy(
            src_ref=crow_ref, dst_ref=cfrow_ref, send_sem=mu_send.at[n_sb], recv_sem=mu_recv.at[n_sb],
            device_id=peer(2), device_id_type=MESH)

    def m_second(kb, beta_next, share):
        rows = pl.ds(pl.multiple_of(kb * MB, MB), MB)
        n_acc, acc = m_block(kb, (1, 3))
        n, mu = finish(n_ref[rows, :] + n_acc, s_ref[rows, :] + acc)
        mub_ref[rows, :] = mu.astype(BF16)
        msq = jnp.sum(mu * mu, axis=1, keepdims=True)
        lp = jnp.log((jnp.broadcast_to(n, (MB, 128)) + ALPHA) / norm_const)
        c = LOG2E * (lp - beta_next * msq)
        c_ref[rows, :] = c
        if share:
            crow_ref[:, rows] = to_row(c)

    def out_copy(slot, kb):
        size = (MB, FB)[slot]
        owner = data if slot == 0 else par
        rows = pl.ds(pl.multiple_of(owner * own + kb * size, size), size)
        return pltpu.make_async_remote_copy(
            src_ref=means_ref.at[rows], dst_ref=means_ref.at[rows], send_sem=out_send.at[slot, kb],
            recv_sem=out_recv.at[slot, kb], device_id=peer(1), device_id_type=MESH)

    def w_copy(slot):
        owner = data if slot == 0 else par
        return pltpu.make_async_remote_copy(
            src_ref=logw_ref.at[owner], dst_ref=logw_ref.at[owner], send_sem=w_send.at[slot], recv_sem=w_recv.at[slot],
            device_id=peer(1), device_id_type=MESH)

    def emit(slot, kb, n_acc, acc):
        size = (MB, FB)[slot]
        owner = data if slot == 0 else par
        n, mu = finish(n_acc, acc)
        means_ref[pl.ds(pl.multiple_of(owner * own + kb * size, size), size), :] = mu
        nrow = to_row(jnp.broadcast_to(n, (size, 128)))
        logw_ref[owner, :, pl.ds(pl.multiple_of(kb * size, size), size)] = jnp.log((nrow + ALPHA) / norm_const)
        out_copy(slot, kb).start()

    for t in range(sweeps):
        beta = temp_ref[t]
        tb = (2.0 * LOG2E) * beta
        last = t == sweeps - 1
        if t == 0:
            ld_pts.wait()
            for ch in range(n_ch):
                pts_copy(0, ch).wait_recv()
            lax.fori_loop(0, 2, lambda s, _: (e_step(0, xpos * 2 + s, tb), 0)[1], 0)

            away = (1 - xpos) * 2

            def pass_on(ch):
                pts_copy(1, ch).wait_recv()
                pts_copy(2, ch).start()

            def take(ch):
                pts_copy(2, ch).wait_recv()
                e_tiles([away * nq + ch * IB], tb)

            def far_points(ch, _):
                pass_on(ch + 1)
                take(ch)
                return 0

            pass_on(0)
            lax.fori_loop(0, n_ch - 1, far_points, 0)
            take(n_ch - 1)
            st_send_all(0, away)
            e_step(0, away + 1, tb)
        else:
            lax.fori_loop(0, 4, lambda s, _: (e_step(t, (s % 2) * 2 + s // 2, tb), 0)[1], 0)
            if last:
                for j in range(EARLY, n_sb):
                    mu_copy(j).start()
        st_combine(t, 0)
        st_combine(t, 2)
        lax.fori_loop(0, n_mb, m_first, 0)
        st_combine(t, 1)
        st_combine(t, 3)
        if not last:
            beta_next = temp_ref[t + 1]
            share = t == sweeps - 2
            lax.fori_loop(0, n_mb, lambda kb, _: (m_second(kb, beta_next, share), 0)[1], 0)
            if share:
                c_copy().start()
                for j in range(EARLY):
                    mu_copy(j).start()
        else:
            def m_last(kb, _):
                rows = pl.ds(pl.multiple_of(kb * MB, MB), MB)
                n_acc, acc = m_block(kb, (1, 3))
                emit(0, kb, n_ref[rows, :] + n_acc, s_ref[rows, :] + acc)
                return 0

            lax.fori_loop(0, n_mb, m_last, 0)
            w_copy(0).start()
            c_copy().wait_recv()

            def far_block(kb, _):
                for j in range(FB // SB):
                    mu_copy(kb * (FB // SB) + j).wait_recv()
                rows = pl.ds(pl.multiple_of(kb * FB, FB), FB)
                c = to_col(cfrow_ref[:, rows])
                c2 = jnp.concatenate([c, c], axis=1)
                n_acc = jnp.zeros((FB, 128), F32)
                acc = jnp.zeros((FB, dim), F32)
                for ic in range(4 * n_ch):
                    cols = pl.ds(ic * IB, IB)
                    xt = x_ref[cols, :]
                    a = lax.dot_general(muf_ref[rows, :], xt, NT, preferred_element_type=F32)
                    r = jnp.exp2((a * tb + c2) - lse_ref[:, cols])
                    n_acc = n_acc + (r[:, :128] + r[:, 128:])
                    acc = acc + jnp.dot(r.astype(BF16), xt, preferred_element_type=F32)
                emit(1, kb, n_acc, acc)
                return 0

            lax.fori_loop(0, n_fb, far_block, 0)
            w_copy(1).start()
            mine = pl.ds(pl.multiple_of(data * nq, nq), nq)
            xo = x_ref[mine, :].astype(F32)
            sq = xo * xo
            hi = sq.astype(BF16)
            lo = (sq - hi.astype(F32)).astype(BF16)
            ones = jnp.ones((8, dim), BF16)
            row_sq = (lax.dot_general(ones, hi, NT, preferred_element_type=F32)
                      + lax.dot_general(ones, lo, NT, preferred_element_type=F32))
            lse_out_ref[...] = LN2 * lse_ref[:, mine] - beta * row_sq[0:1, :]

    for kind in range(3):
        for ch in range(n_ch):
            pts_copy(kind, ch).wait_send()
    for t in range(sweeps):
        for q in range(4):
            for r in range(1, 8):
                st_copy(t, q, r).wait_send()
    for j in range(n_sb):
        mu_copy(j).wait_send()
    c_copy().wait_send()
    for slot in range(2):
        w_copy(slot).wait_send()
        for kb in range((n_mb, n_fb)[slot]):
            out_copy(slot, kb).wait_send()

    def sibling(dev_slot):
        owner = (sib, data_xor(3))[dev_slot]
        size = (MB, FB)[dev_slot]
        for kb in range((n_mb, n_fb)[dev_slot]):
            rows = pl.ds(pl.multiple_of(owner * own + kb * size, size), size)
            pltpu.make_async_remote_copy(
                src_ref=means_ref.at[rows], dst_ref=means_ref.at[rows], send_sem=out_send.at[dev_slot, kb],
                recv_sem=out_recv.at[dev_slot, kb], device_id=peer(1), device_id_type=MESH).wait_recv()
        pltpu.make_async_remote_copy(
            src_ref=logw_ref.at[owner], dst_ref=logw_ref.at[owner], send_sem=w_send.at[dev_slot],
            recv_sem=w_recv.at[dev_slot], device_id=peer(1), device_id_type=MESH).wait_recv()

    sibling(0)
    sibling(1)


def flush_kernel(means_ref, logw_ref, lse_ref, means_out, logw_out, lse_out, sem):
    rows = means_ref.shape[0] // PIECES
    copies = [pltpu.make_async_copy(means_ref.at[pl.ds(i * rows, rows)], means_out.at[pl.ds(i * rows, rows)], sem.at[i])
              for i in range(PIECES)]
    copies.append(pltpu.make_async_copy(logw_ref, logw_out, sem.at[PIECES]))
    copies.append(pltpu.make_async_copy(lse_ref, lse_out, sem.at[PIECES + 1]))
    for cp in copies:
        cp.start()
    for cp in copies:
        cp.wait()


def solution(mesh):
    comp_size = mesh.shape["comp"]
    data_size = mesh.shape["data"]

    def local_fit(points, mu_init, logpi_init, inv_temp):
        nq, dim = points.shape
        rows = mu_init.shape[0]
        own = rows // data_size
        sweeps = inv_temp.shape[0]
        n_pts = nq * data_size
        n_kb = own // KB
        norm_const = n_pts + rows * comp_size * ALPHA
        cfg = (sweeps, own, nq, dim, norm_const)
        any_spec = pl.BlockSpec(memory_space=pl.ANY)
        vmem_spec = pl.BlockSpec(memory_space=pltpu.VMEM)
        dma = pltpu.SemaphoreType.DMA
        n_fb, n_sb = own // FB, own // SB
        means, logw, lse = pl.pallas_call(
            functools.partial(fit_kernel, cfg),
            out_shape=(pltpu.VMEM((rows, dim), F32),
                       pltpu.VMEM((data_size, 1, own), F32),
                       pltpu.VMEM((1, nq), F32)),
            in_specs=[pl.BlockSpec(memory_space=pltpu.SMEM), any_spec, any_spec, any_spec],
            out_specs=(vmem_spec, vmem_spec, vmem_spec),
            scratch_shapes=[
                pltpu.VMEM((n_pts, dim), BF16),
                pltpu.VMEM((own, n_pts + 128), F32),
                pltpu.VMEM((own, dim), BF16),
                pltpu.VMEM((own, dim), BF16),
                pltpu.VMEM((own, 128), F32),
                pltpu.VMEM((1, own), F32),
                pltpu.VMEM((1, own), F32),
                pltpu.VMEM((own, dim), F32),
                pltpu.VMEM((own, 128), F32),
                pltpu.VMEM((own // KT, 8, n_pts), F32),
                pltpu.VMEM((own // KT, 8, n_pts), F32),
                pltpu.VMEM((1, n_pts), F32),
                pltpu.VMEM((sweeps, data_size, 8, 1, nq), F32),
                dma((3,)),
                dma((3, nq // IB)), dma((3, nq // IB)),
                dma((sweeps, 4, 8)), dma((sweeps, 4, 8)),
                dma((n_sb + 1,)), dma((n_sb + 1,)),
                dma((2, n_fb)), dma((2, n_fb)),
                dma((2,)), dma((2,)),
            ],
            compiler_params=pltpu.CompilerParams(
                collective_id=0, has_side_effects=True, vmem_limit_bytes=54 * 1024 * 1024),
        )(inv_temp, points, mu_init, logpi_init.reshape(data_size, 1, own))
        results = [pltpu.with_memory_space_constraint(v, pltpu.VMEM) for v in (means, logw, lse)]
        means, logw, lse = pl.pallas_call(
            flush_kernel,
            out_shape=tuple(jax.ShapeDtypeStruct(v.shape, F32) for v in results),
            in_specs=[vmem_spec] * 3,
            out_specs=(any_spec,) * 3,
            scratch_shapes=[dma((PIECES + 2,))],
            compiler_params=pltpu.CompilerParams(vmem_limit_bytes=16 * 1024 * 1024),
        )(*results)
        return means, logw.reshape(rows), lse.reshape(nq)

    row_spec = P(("fit", "data"), None)
    comp_spec = P(("fit", "comp"), None)
    weight_spec = P(("fit", "comp"))
    lse_spec = P(("fit", "data"))
    return jax.shard_map(local_fit, mesh=mesh, in_specs=(row_spec, comp_spec, weight_spec, P(None)), out_specs=(comp_spec, weight_spec, lse_spec), check_vma=False)
```
